32 devices in a mesh: gx: 8 (over z, x), gy: 4 (over y, core).
Axes of the slice: x: 2, y: 2, z: 4, core: 2. Of those that a mesh axis runs over, the one named last changes fastest.
Arguments:
- displacement_old: float32 [3, 64, 64, 256], P(None, 'gx', 'gy'), may hold values from -6 to 6
- pressure_old: float32 [64, 64, 256], P('gx', 'gy'), may hold values from -6 to 6
- body_force: float32 [3, 64, 64, 256], P(None, 'gx', 'gy'), may hold values from -400 to 400
- fluid_source: float32 [64, 64, 256], P('gx', 'gy'), may hold values from -400 to 400
- material_ids: int32 [64, 64, 256], P('gx', 'gy'), may hold values from 0 to 7
- materials: float32 [5, 8], replicated, may hold values from 0.5 to 4
Outputs:
- displacement: float32 [3, 64, 64, 256], P(None, 'gx', 'gy')
- pressure: float32 [64, 64, 256], P('gx', 'gy')
The draws below stay inside these ranges and needn't reach their ends.
All inputs are finite; a program needn't handle non-finite values.
Results may differ from the reference program's by a relative error of at most 0.00017.
Values sent between devices are 32-bit elements; how exact they have to be, the bound alone decides.
A program may use at most 64 MiB of HBM per device.

```python
import math
import jax
import jax.numpy as jnp
from jax import lax

NZ = 256
NMAT = 8
OUTER = 2
INNER = 3
NX = 64
NY = 64


def field_scale(key):
    key_rise, key_across = jax.random.split(key)
    planes = jnp.arange(NX, dtype=jnp.float32) / NX
    rising = 10.0 ** planes * jnp.exp(jax.random.uniform(key_rise, (NX,), minval=-0.35, maxval=0.35))
    across = jnp.exp(jax.random.uniform(key_across, (NY,), minval=-1.2, maxval=1.2))
    return rising[:, None, None] * across[None, :, None]


def rough_field(key, shape):
    key_scale, key_values = jax.random.split(jax.random.fold_in(key, 17))
    scale = field_scale(key_scale)
    values = jnp.clip(jax.random.normal(key_values, shape, jnp.float32), -6.0, 6.0)
    return (values * scale).astype(jnp.float32)


def draw_body_force(key, part):
    return rough_field(jax.random.fold_in(key, 101), (3, NX, NY, NZ))


def draw_fluid_source(key, part):
    return rough_field(jax.random.fold_in(key, 202), (NX, NY, NZ))


def plant(values, stream_key, low, top_value):
    spot = [jax.random.randint(jax.random.fold_in(stream_key, axis), (), 0, length) for axis, length in enumerate(values.shape)]
    main_axis = values.shape.index(max(values.shape))
    beside = spot[:main_axis] + [(spot[main_axis] + 1) % values.shape[main_axis]] + spot[main_axis + 1:]
    return values.at[tuple(spot)].set(low).at[tuple(beside)].set(top_value)


def block_levels(rng, extent, pieces, least, largest):
    factor_of, own = 1.0, jax.random.fold_in(rng, 6)
    for axis_at, shards_of in pieces:
        draws = jnp.exp(jax.random.uniform(jax.random.fold_in(own, axis_at), (shards_of,), jnp.float32, least / len(pieces), largest / len(pieces)))
        factor_of = factor_of * jnp.repeat(draws, extent[axis_at] // shards_of).reshape([-1 if axis == axis_at else 1 for axis in range(len(extent))])
    return factor_of


def normal_values(own_key, dims, spread, limit, pieces=(), kind=jnp.bfloat16):
    gain = block_levels(own_key, dims, pieces, -0.22, 0.18) if pieces else 1.0
    result = jax.random.normal(own_key, dims, jnp.float32) * spread * gain
    return jnp.minimum(jnp.maximum(result, -limit), limit).astype(kind)


def setup_inputs(seed: int = 0) -> dict:
    keys = jax.random.split(jax.random.key(seed), 7)
    return {
        "displacement_old": normal_values(keys[0], (3, NX, NY, NZ), 1.0, 6.0, ((1, 8), (2, 4)), jnp.float32),
        "pressure_old": normal_values(keys[1], (NX, NY, NZ), 1.0, 6.0, ((0, 8), (1, 4)), jnp.float32),
        "body_force": draw_body_force(jax.random.fold_in(keys[6], 71), 0),
        "fluid_source": draw_fluid_source(jax.random.fold_in(keys[6], 71), 0),
        "material_ids": plant(jax.random.randint(keys[4], (NX, NY, NZ), 0, NMAT), jax.random.fold_in(keys[4], 1), 0, NMAT - 1).astype(jnp.int32),
        "materials": jnp.clip(jnp.exp(jax.random.uniform(keys[5], (5, NMAT), jnp.float32, math.log(0.5), math.log(4.0))), 0.5, 4.0),
    }


step_time = 4.0


def shift_up(values, spatial):
    length = values.shape[spatial]
    widths = [(0, 0)] * values.ndim
    widths[spatial] = (0, 1)
    return lax.slice_in_dim(jnp.pad(values, widths), 1, length + 1, axis=spatial)


def shift_down(values, spatial):
    length = values.shape[spatial]
    widths = [(0, 0)] * values.ndim
    widths[spatial] = (1, 0)
    return lax.slice_in_dim(jnp.pad(values, widths), 0, length, axis=spatial)


def harmonic(first_value, second_value):
    return 2.0 * first_value * second_value / (first_value + second_value)


def divergence(field):
    return (shift_up(field[0], 0) - field[0] + shift_up(field[1], 1) - field[1]
            + shift_up(field[2], 2) - field[2])


def solve(operate, precond, rhs_vec, initial):
    solution = initial
    residual = rhs_vec - operate(initial)
    smoothed = precond(residual)
    direction = smoothed
    current = jnp.sum(residual * smoothed)
    for inner_step in range(INNER):
        image_vec = operate(direction)
        step_length = current / jnp.sum(direction * image_vec)
        solution = solution + step_length * direction
        if inner_step + 1 < INNER:
            residual = residual - step_length * image_vec
            smoothed = precond(residual)
            following = jnp.sum(residual * smoothed)
            direction = smoothed + (following / current) * direction
            current = following
    return solution


def reference(displacement_old, pressure_old, body_force, fluid_source, material_ids, materials):
    lame_first = materials[0][material_ids]
    shear_mod = materials[1][material_ids]
    permeability = materials[2][material_ids]
    storage = materials[3][material_ids]
    biot_coef = 0.25 * materials[4][material_ids]
    stiff_up = [0.5 * (shear_mod + shift_up(shear_mod, spatial)) for spatial in range(3)]
    stiff_down = [0.5 * (shear_mod + shift_down(shear_mod, spatial)) for spatial in range(3)]
    flow_up = [harmonic(permeability, shift_up(permeability, spatial)) for spatial in range(3)]
    flow_down = [harmonic(permeability, shift_down(permeability, spatial)) for spatial in range(3)]
    stab = biot_coef * biot_coef / (lame_first + (2.0 / 3.0) * shear_mod)
    storage_total = storage + stab
    flow_sum = flow_up[0] + flow_down[0] + flow_up[1] + flow_down[1] + flow_up[2] + flow_down[2]
    inv_pressure = 1.0 / (storage_total + step_time * flow_sum)
    stiff_sum = stiff_up[0] + stiff_down[0] + stiff_up[1] + stiff_down[1] + stiff_up[2] + stiff_down[2]
    inv_blocks = 1.0 / jnp.stack([stiff_sum + shift_down(lame_first, spatial) for spatial in range(3)])
    factor = lame_first / (1.0 + lame_first * (inv_blocks[0] + inv_blocks[1] + inv_blocks[2]))

    def apply_pressure(field):
        flux = jnp.zeros_like(field)
        for spatial in range(3):
            flux = (flux + flow_up[spatial] * (field - shift_up(field, spatial))
                    + flow_down[spatial] * (field - shift_down(field, spatial)))
        return storage_total * field + step_time * flux

    def apply_mech(field):
        summed = jnp.zeros_like(field)
        for spatial in range(3):
            summed = (summed + stiff_up[spatial] * (field - shift_up(field, spatial + 1))
                      + stiff_down[spatial] * (field - shift_down(field, spatial + 1)))
        weighted = lame_first * divergence(field)
        lame_pull = jnp.stack([shift_down(weighted, spatial) - weighted for spatial in range(3)])
        return summed + lame_pull

    def solve_pressure(residual):
        return residual * inv_pressure

    def solve_blocks(residual):
        scaled = residual * inv_blocks
        summed = scaled[0] + scaled[1] + scaled[2]
        return scaled - inv_blocks * (factor * summed)

    pressure = pressure_old
    displacement = displacement_old
    for repeat in range(OUTER):
        change = displacement - displacement_old
        rhs_pressure = (storage * pressure_old + step_time * fluid_source
                        - biot_coef * divergence(change) + stab * pressure)
        pressure = solve(apply_pressure, solve_pressure, rhs_pressure, pressure)
        loaded = biot_coef * pressure
        pressure_push = jnp.stack([shift_down(loaded, spatial) - loaded for spatial in range(3)])
        rhs_mech = body_force + pressure_push
        displacement = solve(apply_mech, solve_blocks, rhs_mech, displacement)
    return displacement, pressure
```

```python
import functools
import jax
import jax.numpy as jnp
from jax import lax
from jax.experimental import pallas as pl
from jax.experimental.pallas import tpu as pltpu
from jax.sharding import PartitionSpec as P

OUTER = 2
INNER = 3
step_time = 4.0
MESH = pl.DeviceIdType.MESH
F32 = jnp.float32


def kernel(dims, *refs):
    ngx, ngy, nx, ny, nz, nmat = dims
    (mat, d_hbm, p_hbm, bf_hbm, fs_hbm, ids_hbm, d_out, p_out,
     p_old, bforce, fsource, ids, lsem,
     XI, YIS, YIH, LAM, SHR, PRM, BIO, LAMY, SHRY, PRMY, BIOY, STO, STAB,
     SX, SY, SZ, SSUM, FX, FY, FZ, DIAG, PINV, HB, KF,
     PX, PYS, PYH, MX, MYS, MYH, MCS, MCH,
     WP, WM, AP, AD, DC, LY, LW, RB,
     isend, irecv, psend, precv, msend, mrecv, rsend, rrecv) = refs
    gx, gy = lax.axis_index("gx"), lax.axis_index("gy")
    local = [pltpu.make_async_copy(src, dst, lsem.at[n]) for n, (src, dst) in enumerate((
        (ids_hbm, ids), (p_hbm, PX.at[0, pl.ds(1, nx)]), (d_hbm, MX.at[0, :, pl.ds(1, nx)]),
        (p_hbm, p_old), (fs_hbm, fsource), (bf_hbm, bforce)))]
    for copy in local:
        copy.start()
    barrier = pltpu.get_barrier_semaphore()
    me, ndev = gx * ngy + gy, ngx * ngy

    def peer(d):
        t = lax.rem(me + d, ndev)
        return lax.div(t, ngy), lax.rem(t, ngy)
    has = {(-1, 0): gx > 0, (1, 0): gx < ngx - 1, (0, -1): gy > 0, (0, 1): gy < ngy - 1}
    has[(1, -1)] = jnp.logical_and(has[(1, 0)], has[(0, -1)])
    has[(-1, 1)] = jnp.logical_and(has[(-1, 0)], has[(0, 1)])

    rows = lax.broadcasted_iota(jnp.int32, (ny, nz), 0)
    lanes = lax.broadcasted_iota(jnp.int32, (ny, nz), 1)
    lanes8 = lax.broadcasted_iota(jnp.int32, (nx, nz), 1)
    rows8 = lax.broadcasted_iota(jnp.int32, (nx, nz), 0)
    lane1 = lax.broadcasted_iota(jnp.int32, (1, 128), 1)
    first_row, last_row = rows == 0, rows == ny - 1
    first_lane, last_lane = lanes == 0, lanes == nz - 1
    zero = jnp.zeros((ny, nz), F32)
    zero8 = jnp.zeros((nx, nz), F32)

    def upz(v):
        return pltpu.roll(v, nz - 1, 1)

    def dnz(v):
        return pltpu.roll(v, 1, 1)

    def upy(v, halo):
        return jnp.where(last_row, halo, pltpu.roll(v, ny - 1, 0))

    def dny(v, halo):
        return jnp.where(first_row, halo, pltpu.roll(v, 1, 0))

    def fold(v):
        out = None
        for i in range(0, ny, 8):
            for j in range(0, nz, 128):
                part = v[i:i + 8, j:j + 128]
                out = part if out is None else out + part
        return out

    def loop(body, init, low=0, high=nx, half=None):
        order = [low, high - 1] + list(range(low + 1, high - 1))
        for n, i in enumerate(order):
            init = body(i, init)
            if n == 1 and half is not None:
                half()
        return init

    def copies_of(pairs, send, recv):
        made = []
        for n, (src, dst, off) in enumerate(pairs):
            copy = pltpu.make_async_remote_copy(
                src_ref=src, dst_ref=dst, send_sem=send.at[n], recv_sem=recv.at[n],
                device_id=(gx + off[0], gy + off[1]), device_id_type=MESH)
            made.append((copy, off))
        return made

    def start(made, along=None):
        for copy, off in made:
            if along is not None and (off[0] != 0) != along:
                continue
            @pl.when(has[off])
            def _(copy=copy):
                copy.start()

    def wait_recv(made):
        for copy, off in made:
            @pl.when(has[(-off[0], -off[1])])
            def _(copy=copy):
                copy.wait_recv()

    def wait_send(made):
        for copy, off in made:
            @pl.when(has[off])
            def _(copy=copy):
                copy.wait_send()

    def scalar_field(f):
        return copies_of(
            [(PX.at[f, 1], PX.at[f, nx + 1], (-1, 0)), (PX.at[f, nx], PX.at[f, 0], (1, 0)),
             (PYS.at[f, 0], PYH.at[f, 1], (0, -1)), (PYS.at[f, 1], PYH.at[f, 0], (0, 1))],
            psend.at[f % 2], precv.at[f % 2])

    def vector_field(f):
        return copies_of(
            [(MX.at[f, :, 1], MX.at[f, :, nx + 1], (-1, 0)), (MX.at[f, :, nx], MX.at[f, :, 0], (1, 0)),
             (MYS.at[f, 0], MYH.at[f, 1], (0, -1)), (MYS.at[f, 1], MYH.at[f, 0], (0, 1)),
             (MCS.at[f, 0], MCH.at[f, 0], (1, -1)), (MCS.at[f, 1], MCH.at[f, 1], (-1, 1))],
            msend.at[f % 2], mrecv.at[f % 2])

    def put_scalar(f, i, v):
        PX[f, i + 1] = v
        PYS[f, 0, slice(i, i + 1), :] = v[0:1]
        PYS[f, 1, slice(i, i + 1), :] = v[ny - 1:ny]

    def put_vector(f, i, vs):
        for a in range(3):
            MX[f, a, i + 1] = vs[a]
            MYS[f, 0, a, slice(i, i + 1), :] = vs[a][0:1]
            MYS[f, 1, a, slice(i, i + 1), :] = vs[a][ny - 1:ny]

    def put_corners(f):
        MCS[f, 0] = MX[f, 1, nx, 0:1, :]
        MCS[f, 1] = MX[f, 0, 1, ny - 1:ny, :]

    nf = 1 + OUTER * INNER
    XI[0] = jnp.zeros((ny, nz), jnp.int32)
    XI[nx + 1] = jnp.zeros((ny, nz), jnp.int32)
    for s in range(2):
        YIH[s] = jnp.zeros((nx, nz), jnp.int32)

    def clear(f, c):
        PX[f, 0] = zero
        PX[f, nx + 1] = zero
        for s in range(2):
            PYH[f, s] = zero8
            MCH[f, s] = jnp.zeros((1, nz), F32)
            for a in range(3):
                MX[f, a, s * (nx + 1)] = zero
                MYH[f, s, a] = zero8
        return c
    lax.fori_loop(0, nf, clear, 0)
    for d in range(1, ndev):
        pl.semaphore_signal(barrier, inc=1, device_id=peer(d), device_id_type=MESH)


    def stage(i, c):
        code = ids[i] + 1
        XI[i + 1] = code
        YIS[0, slice(i, i + 1), :] = code[0:1]
        YIS[1, slice(i, i + 1), :] = code[ny - 1:ny]
        return c

    def stage_values(i, c):
        for side, y in ((0, 0), (1, ny - 1)):
            PYS[0, side, i:i + 1, :] = PX[0, i + 1, y:y + 1, :]
            for a in range(3):
                MYS[0, side, a, i:i + 1, :] = MX[0, a, i + 1, y:y + 1, :]
        return c
    local[0].wait()
    loop(stage, 0)
    local[1].wait()
    local[2].wait()
    loop(stage_values, 0)
    put_corners(0)
    pl.semaphore_wait(barrier, ndev - 1)

    codes_copy = copies_of(
        [(XI.at[1], XI.at[nx + 1], (-1, 0)), (XI.at[nx], XI.at[0], (1, 0)),
         (YIS.at[0], YIH.at[1], (0, -1)), (YIS.at[1], YIH.at[0], (0, 1))], isend, irecv)
    p_copy, d_copy = scalar_field(0), vector_field(0)
    start(codes_copy)
    start(p_copy)
    start(d_copy)

    def lookup(code, table_rows):
        out = [jnp.zeros(code.shape, F32) for _ in table_rows]
        for m in range(nmat):
            hit = code == m + 1
            out = [jnp.where(hit, mat[t, m], v) for t, v in zip(table_rows, out)]
        return out

    def look_plane(i, c):
        lam, shr, prm, sto, bio = lookup(XI[i + 1], (0, 1, 2, 3, 4))
        bio = 0.25 * bio
        LAM[i + 1] = lam
        SHR[i + 1] = shr
        PRM[i + 1] = prm
        BIO[i + 1] = bio
        STO[i] = sto
        STAB[i] = bio * bio / (lam + 2.0 / 3.0 * shr)
        return c
    loop(look_plane, 0)
    wait_recv(codes_copy)

    for j in (0, nx + 1):
        lam, shr, prm, bio = lookup(XI[j], (0, 1, 2, 4))
        LAM[j] = lam
        SHR[j] = shr
        PRM[j] = prm
        BIO[j] = 0.25 * bio
    for s in range(2):
        lam, shr, prm, bio = lookup(YIH[s], (0, 1, 2, 4))
        SHRY[s] = shr
        PRMY[s] = prm
        if s == 0:
            LAMY[...] = lam
            BIOY[...] = 0.25 * bio

    def harmonic(one, two):
        return (2.0 * step_time) * one * two / (one + two)

    def harmonic_plane(j, c):
        FX[j] = harmonic(PRM[j], PRM[j + 1])
        SX[j] = 0.5 * (SHR[j] + SHR[j + 1])
        return c
    loop(harmonic_plane, 0, 0, nx + 1)

    def coefs(i, c):
        shr, prm, lam = SHR[i + 1], PRM[i + 1], LAM[i + 1]
        row = slice(i, i + 1)
        fyu = harmonic(prm, upy(prm, PRMY[1, row, :]))
        fyd = harmonic(prm, dny(prm, PRMY[0, row, :]))
        fzu = jnp.where(last_lane, 0.0, harmonic(prm, upz(prm)))
        fzd = jnp.where(first_lane, 0.0, dnz(fzu))
        FY[1, i], FY[0, i], FZ[1, i], FZ[0, i] = fyu, fyd, fzu, fzd
        diag = STO[i] + STAB[i] + (FX[i] + FX[i + 1] + fyu + fyd + fzu + fzd)
        DIAG[i] = diag
        PINV[i] = 1.0 / diag
        half = 0.5 * shr
        syu = 0.5 * (shr + upy(shr, SHRY[1, row, :]))
        syd = 0.5 * (shr + dny(shr, SHRY[0, row, :]))
        szu = half + jnp.where(last_lane, 0.0, 0.5 * upz(shr))
        szd = half + jnp.where(first_lane, 0.0, 0.5 * dnz(shr))
        total = SX[i] + SX[i + 1] + syu + syd + szu + szd
        SY[1, i], SY[0, i] = syu, syd
        SZ[1, i] = jnp.where(last_lane, 0.0, szu)
        SZ[0, i] = jnp.where(first_lane, 0.0, szd)
        SSUM[i] = total
        h0 = 1.0 / (total + LAM[i])
        h1 = 1.0 / (total + dny(lam, LAMY[row, :]))
        h2 = 1.0 / (total + jnp.where(first_lane, 0.0, dnz(lam)))
        HB[0, i], HB[1, i], HB[2, i] = h0, h1, h2
        KF[i] = lam / (1.0 + lam * (h0 + h1 + h2))
        return c
    loop(coefs, 0)

    def apply_pressure(f, emit, init, half=None):
        def body(i, c):
            row = slice(i, i + 1)
            v = PX[f, i + 1]
            out = (DIAG[i] * v - FX[i + 1] * PX[f, i + 2] - FX[i] * PX[f, i]
                   - FY[1, i] * upy(v, PYH[f, 1, row, :]) - FY[0, i] * dny(v, PYH[f, 0, row, :])
                   - FZ[1, i] * upz(v) - FZ[0, i] * dnz(v))
            return emit(i, v, out, c)
        return loop(body, init, half=half)

    def apply_mech(f, emit, init, half=None):
        m = [MYH[f, 0, a] for a in range(3)]
        ahead = jnp.where(rows8 == nx - 1, MCH[f, 1], pltpu.roll(m[0], nx - 1, 0))
        z8 = jnp.where(lanes8 == nz - 1, 0.0, pltpu.roll(m[2], nz - 1, 1))
        LY[...] = LAMY[...] * (ahead - m[0] + MYS[f, 0, 1] - m[1] + z8 - m[2])
        m = [MX[f, a, 0] for a in range(3)]
        below_first = LAM[0] * (MX[f, 0, 1] - m[0] + upy(m[1], MCH[f, 0]) - m[1]
                          + jnp.where(last_lane, 0.0, upz(m[2])) - m[2])

        def weigh(i):
            w = [MX[f, a, i + 1] for a in range(3)]
            return LAM[i + 1] * (MX[f, 0, i + 2] - w[0] + upy(w[1], MYH[f, 1, 1, i:i + 1, :]) - w[1]
                                 + jnp.where(last_lane, 0.0, upz(w[2])) - w[2])

        def body(i, c):
            row = slice(i, i + 1)
            ws, outs, div = [], [], None
            for a in range(3):
                w, wx = MX[f, a, i + 1], MX[f, a, i + 2]
                wy, wz = upy(w, MYH[f, 1, a, row, :]), upz(w)
                out = (SSUM[i] * w - SX[i + 1] * wx - SX[i] * MX[f, a, i]
                       - SY[1, i] * wy - SY[0, i] * dny(w, MYH[f, 0, a, row, :])
                       - SZ[1, i] * wz - SZ[0, i] * dnz(w))
                part = (wx, wy, jnp.where(last_lane, 0.0, wz))[a] - w
                div = part if div is None else div + part
                ws.append(w)
                outs.append(out)
            weighted = LAM[i + 1] * div
            LW[i] = weighted
            before = below_first if i == 0 else weigh(i - 1) if i == nx - 1 else LW[i - 1]
            below = (before, dny(weighted, LY[row, :]), jnp.where(first_lane, 0.0, dnz(weighted)))
            outs = [outs[a] + (below[a] - weighted) for a in range(3)]
            return emit(i, ws, outs, c)
        return loop(body, init, half=half)

    def block_solve(i, r):
        scaled = [r[a] * HB[a, i] for a in range(3)]
        tail = KF[i] * (scaled[0] + scaled[1] + scaled[2])
        return [scaled[a] - HB[a, i] * tail for a in range(3)]

    def dot3(a, b):
        return fold(a[0] * b[0] + a[1] * b[1] + a[2] * b[2])

    summed = []

    def all_sum(q, sums):
        row = jnp.zeros((1, 128), F32)
        for k, s in enumerate(sums):
            row = jnp.where(lane1 == k, jnp.sum(s, keepdims=True), row)
        RB[q, me] = row
        for d in sorted(range(1, ndev), key=lambda d: -min(d, ndev - d)):
            copy = pltpu.make_async_remote_copy(
                src_ref=RB.at[q, me], dst_ref=RB.at[q, me], send_sem=rsend.at[q],
                recv_sem=rrecv.at[q], device_id=peer(d), device_id_type=MESH)
            copy.start()
        every = RB.at[q, pl.ds(0, ndev - 1)]
        whole = pltpu.make_async_remote_copy(
            src_ref=every, dst_ref=every, send_sem=rsend.at[q], recv_sem=rrecv.at[q],
            device_id=peer(1), device_id_type=MESH)
        whole.wait_recv()
        summed.append(whole)
        parts = [RB[q, d] for d in range(ndev)]
        while len(parts) > 1:
            parts = [sum(parts[d + 1:d + 2], parts[d]) for d in range(0, len(parts), 2)]
        row = parts[0]
        return [row[:, k:k + 1] for k in range(len(sums))]

    def combine(t):
        n0, m0, m1, m2, m3, m4 = t
        n1 = m0 - n0
        n2 = m1 - n1
        l1, l2 = m1 / m0, m2 / m0
        d1 = m2 - l1 * m1
        e = m3 - l1 * m2
        l3 = jnp.where(d1 > 0, e / d1, 0.0)
        d2 = m4 - l2 * m2 - l3 * e
        y1 = n1 - l1 * n0
        y2 = n2 - l2 * n0 - l3 * y1
        c2 = jnp.where(d2 > 0, y2 / d2, 0.0)
        c1 = jnp.where(d1 > 0, y1 / d1, 0.0) - l3 * c2
        c0 = n0 / m0 - l1 * c1 - l2 * c2
        return c0, c1, c2

    zacc = jnp.zeros((8, 128), F32)
    wait_recv(p_copy)
    wait_send(p_copy)
    wait_send(codes_copy)

    def keep_ap(i, v, out, c):
        AP[i] = out
        return c
    apply_pressure(0, keep_ap, 0)

    def clear_change(i, c):
        DC[i] = zero
        return c
    loop(clear_change, 0)
    local[3].wait()
    local[4].wait()

    psent, msent = [], []

    def retire(queue):
        if len(queue) == 2:
            wait_send(queue.pop(0))
    for outer in range(OUTER):
        base = 1 + INNER * outer

        def p_start(i, acc):
            if outer > 0:
                m_change(i, 0)
            rhs = (STO[i] * p_old[i] + step_time * fsource[i] - BIO[i + 1] * DC[i]
                   + STAB[i] * PX[0, i + 1])
            r = rhs - AP[i]
            u = r * PINV[i]
            put_scalar(base, i, u)
            return acc + fold(r * u)
        retire(psent)
        made = scalar_field(base)
        n0 = loop(p_start, zacc, half=functools.partial(start, made, True))
        start(made, False)
        psent.append(made)
        if outer > 0:
            loop(m_after, 0)
        if outer == 0:
            wait_recv(d_copy)
            wait_send(d_copy)

            def keep_ad(i, ws, outs, c):
                for a in range(3):
                    AD[a, i] = outs[a]
                return c
            apply_mech(0, keep_ad, 0)
            local[5].wait()
        sums = [n0]
        for k in range(INNER):
            sums = [jnp.sum(v, keepdims=True) for v in sums]
            wait_recv(made)

            def p_step(i, v, w, c):
                WP[k, i] = w
                even = c[0] + fold(v * w)
                if k == INNER - 1:
                    return (even,)
                u = w * PINV[i] - v
                put_scalar(base + k + 1, i, u)
                return even, c[1] + fold(u * w)
            half = None
            if k < INNER - 1:
                retire(psent)
                made = scalar_field(base + k + 1)
                half = functools.partial(start, made, True)
            sums += apply_pressure(base + k, p_step, (zacc,) * (1 if k == INNER - 1 else 2), half)
            if k < INNER - 1:
                start(made, False)
                psent.append(made)
        cs = combine(all_sum(2 * outer, sums))

        def p_update(j, c):
            v = PX[0, j]
            for k in range(INNER):
                v = v + cs[k] * PX[base + k, j]
            PX[0, j] = v
            return c
        loop(p_update, 0, 0, nx + 1)
        ph = PYH[0, 0]
        for k in range(INNER):
            ph = ph + cs[k] * PYH[base + k, 0]
        PYH[0, 0] = ph
        LY[...] = BIOY[...] * ph

        def m_start(i, acc):
            row = slice(i, i + 1)
            load = BIO[i + 1] * PX[0, i + 1]
            below = (BIO[i] * PX[0, i], dny(load, LY[row, :]), jnp.where(first_lane, 0.0, dnz(load)))
            r = [bforce[a, i] + (below[a] - load) - AD[a, i] for a in range(3)]
            u = block_solve(i, r)
            put_vector(base, i, u)
            return acc + dot3(r, u)
        retire(msent)
        made = vector_field(base)

        def send_planes(f, made):
            put_corners(f)
            start(made, True)
        n0 = loop(m_start, zacc, half=functools.partial(send_planes, base, made))
        start(made, False)
        msent.append(made)

        def p_after(i, c):
            if outer == OUTER - 1:
                p_out[i] = PX[0, i + 1]
            else:
                v = AP[i]
                for k in range(INNER):
                    v = v + cs[k] * WP[k, i]
                AP[i] = v
            return c
        loop(p_after, 0)
        sums = [n0]
        for k in range(INNER):
            sums = [jnp.sum(v, keepdims=True) for v in sums]
            wait_recv(made)

            def m_step(i, v, w, c):
                if outer < OUTER - 1:
                    for a in range(3):
                        WM[k, a, i] = w[a]
                even = c[0] + dot3(v, w)
                if k == INNER - 1:
                    return (even,)
                z = block_solve(i, w)
                u = [z[a] - v[a] for a in range(3)]
                put_vector(base + k + 1, i, u)
                return even, c[1] + dot3(u, w)
            half = None
            if k < INNER - 1:
                retire(msent)
                made = vector_field(base + k + 1)
                half = functools.partial(send_planes, base + k + 1, made)
            sums += apply_mech(base + k, m_step, (zacc,) * (1 if k == INNER - 1 else 2), half)
            if k < INNER - 1:
                start(made, False)
                msent.append(made)
        cs = combine(all_sum(2 * outer + 1, sums))

        def mixed(get, cs=cs, base=base):
            v = cs[0] * get(base)
            for k in range(1, INNER):
                v = v + cs[k] * get(base + k)
            return v

        def m_change(i, c):
            row = slice(i, i + 1)
            change = [mixed(lambda f, a=a: MX[f, a, i + 1]) for a in range(3)]
            cx = mixed(lambda f: MX[f, 0, i + 2])
            cy = upy(change[1], mixed(lambda f: MYH[f, 1, 1, row, :]))
            cz = jnp.where(last_lane, 0.0, upz(change[2]))
            DC[i] = DC[i] + (cx - change[0] + cy - change[1] + cz - change[2])
            return c

        def m_after(i, c, cs=cs, mixed=mixed, outer=outer):
            for a in range(3):
                before = MX[0, a, i + 1] if outer == 0 else d_out[a, i]
                d_out[a, i] = before + mixed(lambda f, a=a: MX[f, a, i + 1])
            if outer < OUTER - 1:
                for a in range(3):
                    v = AD[a, i]
                    for k in range(INNER):
                        v = v + cs[k] * WM[k, a, i]
                    AD[a, i] = v
            return c
        if outer == OUTER - 1:
            loop(m_after, 0)

    for made in psent + msent:
        wait_send(made)
    for copy in summed:
        copy.wait_send()


def on_device(dims, d_old, p_old, bforce, fsource, ids, materials):
    ngx, ngy, nx, ny, nz, nmat = dims
    nf = 1 + OUTER * INNER
    nq = 2 * OUTER

    def vm(*shape, dtype=F32):
        return pltpu.VMEM(shape, dtype)
    plane, strip = (ny, nz), (nx, nz)
    cell = (nx, ny, nz)
    ext = (nx + 2, ny, nz)
    dma = pltpu.SemaphoreType.DMA
    scratch = [
        vm(*cell), vm(3, *cell), vm(*cell), vm(*cell, dtype=jnp.int32), dma((6,)),
        vm(*ext, dtype=jnp.int32), vm(2, *strip, dtype=jnp.int32), vm(2, *strip, dtype=jnp.int32),
        vm(*ext), vm(*ext), vm(*ext), vm(*ext), vm(*strip), vm(2, *strip), vm(2, *strip), vm(*strip),
        vm(*cell), vm(*cell),
        vm(nx + 1, *plane), vm(2, *cell), vm(2, *cell), vm(*cell),
        vm(nx + 1, *plane), vm(2, *cell), vm(2, *cell), vm(*cell), vm(*cell),
        vm(3, *cell), vm(*cell),
        vm(nf, *ext), vm(nf, 2, *strip), vm(nf, 2, *strip),
        vm(nf, 3, *ext), vm(nf, 2, 3, *strip), vm(nf, 2, 3, *strip), vm(nf, 2, 1, nz), vm(nf, 2, 1, nz),
        vm(INNER, *cell), vm(INNER, 3, *cell), vm(*cell), vm(3, *cell), vm(*cell),
        vm(*strip), vm(*cell), vm(nq, ngx * ngy, 1, 128),
        dma((4,)), dma((4,)), dma((2, 4)), dma((2, 4)), dma((2, 6)), dma((2, 6)),
        dma((nq,)), dma((nq,)),
    ]
    block = pl.BlockSpec(memory_space=pltpu.VMEM)
    return pl.pallas_call(
        functools.partial(kernel, dims),
        out_shape=(jax.ShapeDtypeStruct(d_old.shape, F32), jax.ShapeDtypeStruct(p_old.shape, F32)),
        in_specs=[pl.BlockSpec(memory_space=pltpu.SMEM)] + [pl.BlockSpec(memory_space=pl.ANY)] * 5,
        out_specs=(block, block),
        scratch_shapes=scratch,
        compiler_params=pltpu.CompilerParams(
            collective_id=0, has_side_effects=True, vmem_limit_bytes=63 * 1024 * 1024),
        name="poro",
    )(materials, d_old, p_old, bforce, fsource, ids)


def solution(mesh):
    ngx, ngy = mesh.shape["gx"], mesh.shape["gy"]

    def body(d_old, p_old, bforce, fsource, ids, materials):
        dims = (ngx, ngy, *p_old.shape, materials.shape[1])
        return on_device(dims, d_old, p_old, bforce, fsource, ids, materials)

    return jax.shard_map(
        body,
        mesh=mesh,
        in_specs=(P(None, "gx", "gy", None), P("gx", "gy", None), P(None, "gx", "gy", None),
                  P("gx", "gy", None), P("gx", "gy", None), P()),
        out_specs=(P(None, "gx", "gy", None), P("gx", "gy", None)),
        check_vma=False,
    )
```

```python
import functools
import jax
import jax.numpy as jnp
from jax import lax
from jax.experimental import pallas as pl
from jax.experimental.pallas import tpu as pltpu
from jax.sharding import PartitionSpec as P

OUTER = 2
INNER = 3
step_time = 4.0
D = INNER
TINY = 1e-30
VMEM_BYTES = 67043328
DIAGONALS = ((1, -1), (-1, 1), (1, 1), (-1, -1))
MESH = pl.DeviceIdType.MESH
F32 = jnp.float32


def kernel(dims, *refs):
    ngx, ngy, nx, ny, nz, nmat = dims
    (mat, d_hbm, p_hbm, bf_hbm, fs_hbm, ids_hbm, d_out, p_out,
     p_old, bforce, fsource, ids, lsem,
     XI, XIY, XIS, XIR, LAM, SHR, PRM, BIO, STO, STAB, LAMY,
     SX, SY, SZ, SSUM, FX, FY, FZ, DIAG, PINV, HB, KF,
     P0, P0Y, U, UY, UCS, UCR, MX, MYS, MYH, MCS, MCH,
     WP, WM, AP, AD, DC, LY, LW, RB,
     isend, irecv, zsend, zrecv, psend, precv, msend, mrecv, rsend, rrecv) = refs
    gx, gy = lax.axis_index("gx"), lax.axis_index("gy")
    local = [pltpu.make_async_copy(src, dst, lsem.at[n]) for n, (src, dst) in enumerate((
        (ids_hbm, ids), (p_hbm, P0.at[pl.ds(D, nx), pl.ds(0, ny)]), (d_hbm, MX.at[0, :, pl.ds(1, nx)]),
        (p_hbm, p_old), (fs_hbm, fsource), (bf_hbm, bforce)))]
    for copy in local:
        copy.start()
    barrier = pltpu.get_barrier_semaphore()
    me, ndev = gx * ngy + gy, ngx * ngy

    def peer(d):
        t = lax.rem(me + d, ndev)
        return lax.div(t, ngy), lax.rem(t, ngy)
    has = {(-1, 0): gx > 0, (1, 0): gx < ngx - 1, (0, -1): gy > 0, (0, 1): gy < ngy - 1}
    for c in DIAGONALS:
        has[c] = jnp.logical_and(has[(c[0], 0)], has[(0, c[1])])

    rows = lax.broadcasted_iota(jnp.int32, (ny, nz), 0)
    lanes = lax.broadcasted_iota(jnp.int32, (ny, nz), 1)
    lanes8 = lax.broadcasted_iota(jnp.int32, (nx, nz), 1)
    rows8 = lax.broadcasted_iota(jnp.int32, (nx, nz), 0)
    lane1 = lax.broadcasted_iota(jnp.int32, (1, 128), 1)
    first_row, last_row = rows == 0, rows == ny - 1
    first_lane, last_lane = lanes == 0, lanes == nz - 1
    zero = jnp.zeros((ny, nz), F32)
    near = lax.broadcasted_iota(jnp.int32, (8, nz), 0) < 4
    wide = ny + 8
    first_wide = lax.broadcasted_iota(jnp.int32, (wide, nz), 1) == 0
    last_wide = lax.broadcasted_iota(jnp.int32, (wide, nz), 1) == nz - 1
    zero8 = jnp.zeros((nx, nz), F32)

    def upz(v):
        return pltpu.roll(v, nz - 1, 1)

    def dnz(v):
        return pltpu.roll(v, 1, 1)

    def upy(v, halo):
        return jnp.where(last_row, halo, pltpu.roll(v, ny - 1, 0))

    def dny(v, halo):
        return jnp.where(first_row, halo, pltpu.roll(v, 1, 0))

    def upw(v):
        return pltpu.roll(v, wide - 1, 0)

    def dnw(v):
        return pltpu.roll(v, 1, 0)

    def fold(v):
        out = None
        for i in range(0, ny, 8):
            for j in range(0, nz, 128):
                part = v[i:i + 8, j:j + 128]
                out = part if out is None else out + part
        return out

    def loop(body, init, low=0, high=nx, half=None):
        order = [low, high - 1] + list(range(low + 1, high - 1))
        for n, i in enumerate(order):
            init = body(i, init)
            if n == 1 and half is not None:
                half()
        return init

    def copies_of(pairs, send, recv):
        made = []
        for n, (src, dst, off) in enumerate(pairs):
            copy = pltpu.make_async_remote_copy(
                src_ref=src, dst_ref=dst, send_sem=send.at[n], recv_sem=recv.at[n],
                device_id=(gx + off[0], gy + off[1]), device_id_type=MESH)
            made.append((copy, off))
        return made

    def start(made, along=None):
        for copy, off in made:
            if along is not None and (off[0] != 0) != along:
                continue
            @pl.when(has[off])
            def _(copy=copy):
                copy.start()

    def wait_recv(made):
        for copy, off in made:
            @pl.when(has[(-off[0], -off[1])])
            def _(copy=copy):
                copy.wait_recv()

    def wait_send(made):
        for copy, off in made:
            @pl.when(has[off])
            def _(copy=copy):
                copy.wait_send()

    def wide_field(F, Y, CS, CR, depth, send, recv):
        pairs = [(F.at[pl.ds(D, depth), pl.ds(0, ny)], F.at[pl.ds(D + nx, depth), pl.ds(0, ny)], (-1, 0)),
                 (F.at[pl.ds(D + nx - depth, depth), pl.ds(0, ny)], F.at[pl.ds(D - depth, depth), pl.ds(0, ny)], (1, 0)),
                 (F.at[pl.ds(D, nx), pl.ds(0, 8)], Y.at[1], (0, -1)),
                 (F.at[pl.ds(D, nx), pl.ds(ny - 8, 8)], Y.at[0], (0, 1))]
        if CS is not None:
            pairs += [(CS.at[c], CR.at[c], off) for c, off in enumerate(DIAGONALS)]
        return copies_of(pairs, send, recv)

    def stage_corners(F, CS):
        n, m = CS.shape[1:3]
        for c, (sx, sy) in enumerate(DIAGONALS):
            for t in range(n):
                CS[c, t] = F[D + (t if sx < 0 else nx - n + t), (0 if sy < 0 else ny - m):(m if sy < 0 else ny), :]

    def clear_missing(F, Y, CR, depth):
        none = jnp.zeros((wide, nz), F.dtype)
        for side, low in ((-1, D - depth), (1, D + nx)):
            @pl.when(jnp.logical_not(has[(side, 0)]))
            def _(low=low):
                for t in range(depth):
                    F[low + t] = none
        for side, s in ((-1, 0), (1, 1)):
            @pl.when(jnp.logical_not(has[(0, side)]))
            def _(s=s):
                for i in range(nx):
                    Y[s, i] = none[:8]
        if CR is not None:
            for c, off in enumerate(DIAGONALS):
                @pl.when(jnp.logical_not(has[(-off[0], -off[1])]))
                def _(c=c):
                    CR[c] = jnp.zeros(CR.shape[1:], F.dtype)

    def merge(F, Y, CR):
        for i in range(nx):
            F[D + i, ny:, :] = jnp.where(near, Y[1, i], Y[0, i])
        if CR is not None:
            n, m = CR.shape[1:3]
            for c, (sx, sy) in enumerate(DIAGONALS):
                for t in range(n):
                    low = ny if sy < 0 else wide - m
                    F[(D + nx + t) if sx < 0 else (D - n + t), low:low + m, :] = CR[c, t]

    def vector_field(f):
        return copies_of(
            [(MX.at[f, :, 1], MX.at[f, :, nx + 1], (-1, 0)), (MX.at[f, :, nx], MX.at[f, :, 0], (1, 0)),
             (MYS.at[f, 0], MYH.at[f, 1], (0, -1)), (MYS.at[f, 1], MYH.at[f, 0], (0, 1)),
             (MCS.at[f, 0], MCH.at[f, 0], (1, -1)), (MCS.at[f, 1], MCH.at[f, 1], (-1, 1))],
            msend.at[f % 2], mrecv.at[f % 2])

    def put_vector(f, i, vs):
        for a in range(3):
            MX[f, a, i + 1] = vs[a]
            MYS[f, 0, a, slice(i, i + 1), :] = vs[a][0:1]
            MYS[f, 1, a, slice(i, i + 1), :] = vs[a][ny - 1:ny]

    def put_corners(f):
        MCS[f, 0] = MX[f, 1, nx, 0:1, :]
        MCS[f, 1] = MX[f, 0, 1, ny - 1:ny, :]

    nf = 1 + OUTER * INNER
    def clear(f, c):
        for s in range(2):
            MCH[f, s] = jnp.zeros((1, nz), F32)
            for a in range(3):
                MX[f, a, s * (nx + 1)] = zero
                MYH[f, s, a] = zero8
        return c
    lax.fori_loop(0, nf, clear, 0)
    for d in range(1, ndev):
        pl.semaphore_signal(barrier, inc=1, device_id=peer(d), device_id_type=MESH)


    def stage_values(i, c):
        for side, y in ((0, 0), (1, ny - 1)):
            for a in range(3):
                MYS[0, side, a, i:i + 1, :] = MX[0, a, i + 1, y:y + 1, :]
        return c
    local[0].wait()
    for i in range(nx):
        XI[D + i, 0:ny, :] = ids[i] + 1
    stage_corners(XI, XIS)
    local[1].wait()
    pl.semaphore_wait(barrier, ndev - 1)
    p_copy = wide_field(P0, P0Y, None, None, 1, zsend, zrecv)
    codes_copy = wide_field(XI, XIY, XIS, XIR, D, isend, irecv)
    d_copy = vector_field(0)
    start(p_copy)
    start(codes_copy)
    local[2].wait()
    loop(stage_values, 0)
    put_corners(0)
    start(d_copy)
    clear_missing(XI, XIY, XIR, D)
    clear_missing(P0, P0Y, None, 1)
    for outer in range(OUTER):
        clear_missing(U.at[INNER * outer], UY.at[outer], UCR.at[outer], D)

    def lookup(code, table_rows):
        out = [jnp.zeros(code.shape, F32) for _ in table_rows]
        for m in range(nmat):
            hit = code == m + 1
            out = [jnp.where(hit, mat[t, m], v) for t, v in zip(table_rows, out)]
        return out

    def look(j, part):
        code = XI[j, part, :]
        lam, shr, prm, sto, bio = lookup(code, (0, 1, 2, 3, 4))
        bio = 0.25 * bio
        LAM[j, part, :] = lam
        SHR[j, part, :] = shr
        PRM[j, part, :] = prm
        BIO[j, part, :] = bio
        STO[j, part, :] = sto
        STAB[j, part, :] = bio * bio / jnp.maximum(lam + 2.0 / 3.0 * shr, TINY)
    for i in range(nx):
        look(D + i, slice(0, ny))
    wait_recv(codes_copy)
    merge(XI, XIY, XIR)
    for i in range(nx):
        look(D + i, slice(ny, wide))
    for j in (D - 1, D + nx):
        look(j, slice(0, wide))

    def harmonic(one, two):
        return (2.0 * step_time) * one * two / jnp.maximum(one + two, TINY)

    def flow(j):
        prm = PRM[j]
        fzu = jnp.where(last_wide, 0.0, harmonic(prm, upz(prm)))
        fyu = harmonic(prm, upw(prm))
        FY[j], FZ[j] = fyu, fzu
        diag = STO[j] + STAB[j] + (FX[j] + FX[j + 1] + fyu + dnw(fyu) + fzu + dnz(fzu))
        DIAG[j] = diag
        PINV[j] = jnp.where(XI[j] > 0, 1.0 / jnp.maximum(diag, TINY), 0.0)

    def face(j):
        FX[j] = harmonic(PRM[j - 1], PRM[j])
    for j in range(D, D + nx + 1):
        face(j)
    for j in range(D, D + nx):
        flow(j)

    def rim():
        outer_planes = [j for j in range(nx + 2 * D) if j < D - 1 or j > D + nx]
        for j in outer_planes:
            look(j, slice(0, wide))
        for j in list(range(1, D)) + list(range(D + nx + 1, nx + 2 * D)):
            face(j)
        for j in list(range(1, D)) + list(range(D + nx, nx + 2 * D - 1)):
            flow(j)

    def stiff_face(j, c):
        SX[j] = 0.5 * (SHR[D + j - 1, 0:ny, :] + SHR[D + j, 0:ny, :])
        return c

    def coefs(i, c):
        shrw, lamw = SHR[D + i], LAM[D + i]
        shr, lam = shrw[:ny], lamw[:ny]
        LAMY[slice(i, i + 1), :] = LAM[D + i, wide - 1:wide, :]
        half = 0.5 * shr
        syw = 0.5 * (shrw + upw(shrw))
        syu, syd = syw[:ny], dnw(syw)[:ny]
        szu = half + jnp.where(last_lane, 0.0, 0.5 * upz(shr))
        szd = half + jnp.where(first_lane, 0.0, 0.5 * dnz(shr))
        total = SX[i] + SX[i + 1] + syu + syd + szu + szd
        SY[1, i], SY[0, i] = syu, syd
        SZ[1, i] = jnp.where(last_lane, 0.0, szu)
        SZ[0, i] = jnp.where(first_lane, 0.0, szd)
        SSUM[i] = total
        h0 = 1.0 / (total + LAM[D + i - 1, 0:ny, :])
        h1 = 1.0 / (total + dnw(lamw)[:ny])
        h2 = 1.0 / (total + jnp.where(first_lane, 0.0, dnz(lam)))
        HB[0, i], HB[1, i], HB[2, i] = h0, h1, h2
        KF[i] = lam / (1.0 + lam * (h0 + h1 + h2))
        return c

    def apply_pressure(F, j, rows):
        v = F[j]
        out = (DIAG[j] * v - FX[j + 1] * F[j + 1] - FX[j] * F[j - 1]
               - FY[j] * upw(v) - dnw(FY[j] * v)
               - FZ[j] * upz(v) - dnz(FZ[j] * v))
        return v[:rows], out[:rows]

    def apply_mech(f, emit, init, half=None):
        m = [MYH[f, 0, a] for a in range(3)]
        ahead = jnp.where(rows8 == nx - 1, MCH[f, 1], pltpu.roll(m[0], nx - 1, 0))
        z8 = jnp.where(lanes8 == nz - 1, 0.0, pltpu.roll(m[2], nz - 1, 1))
        LY[...] = LAMY[...] * (ahead - m[0] + MYS[f, 0, 1] - m[1] + z8 - m[2])
        m = [MX[f, a, 0] for a in range(3)]
        below_first = LAM[D - 1, 0:ny, :] * (MX[f, 0, 1] - m[0] + upy(m[1], MCH[f, 0]) - m[1]
                          + jnp.where(last_lane, 0.0, upz(m[2])) - m[2])

        def weigh(i):
            w = [MX[f, a, i + 1] for a in range(3)]
            return LAM[D + i, 0:ny, :] * (MX[f, 0, i + 2] - w[0] + upy(w[1], MYH[f, 1, 1, i:i + 1, :]) - w[1]
                                 + jnp.where(last_lane, 0.0, upz(w[2])) - w[2])

        def body(i, c):
            row = slice(i, i + 1)
            ws, outs, div = [], [], None
            for a in range(3):
                w, wx = MX[f, a, i + 1], MX[f, a, i + 2]
                wy, wz = upy(w, MYH[f, 1, a, row, :]), upz(w)
                out = (SSUM[i] * w - SX[i + 1] * wx - SX[i] * MX[f, a, i]
                       - SY[1, i] * wy - SY[0, i] * dny(w, MYH[f, 0, a, row, :])
                       - SZ[1, i] * wz - SZ[0, i] * dnz(w))
                part = (wx, wy, jnp.where(last_lane, 0.0, wz))[a] - w
                div = part if div is None else div + part
                ws.append(w)
                outs.append(out)
            weighted = LAM[D + i, 0:ny, :] * div
            LW[i] = weighted
            before = below_first if i == 0 else weigh(i - 1) if i == nx - 1 else LW[i - 1]
            below = (before, dny(weighted, LY[row, :]), jnp.where(first_lane, 0.0, dnz(weighted)))
            outs = [outs[a] + (below[a] - weighted) for a in range(3)]
            return emit(i, ws, outs, c)
        return loop(body, init, half=half)

    def block_solve(i, r):
        scaled = [r[a] * HB[a, i] for a in range(3)]
        tail = KF[i] * (scaled[0] + scaled[1] + scaled[2])
        return [scaled[a] - HB[a, i] * tail for a in range(3)]

    def dot3(a, b):
        return fold(a[0] * b[0] + a[1] * b[1] + a[2] * b[2])

    summed = []

    def all_sum(q, sums):
        row = jnp.zeros((1, 128), F32)
        for k, s in enumerate(sums):
            row = jnp.where(lane1 == k, jnp.sum(s, keepdims=True), row)
        RB[q, me] = row
        for d in sorted(range(1, ndev), key=lambda d: -min(d, ndev - d)):
            copy = pltpu.make_async_remote_copy(
                src_ref=RB.at[q, me], dst_ref=RB.at[q, me], send_sem=rsend.at[q],
                recv_sem=rrecv.at[q], device_id=peer(d), device_id_type=MESH)
            copy.start()
        every = RB.at[q, pl.ds(0, ndev - 1)]
        whole = pltpu.make_async_remote_copy(
            src_ref=every, dst_ref=every, send_sem=rsend.at[q], recv_sem=rrecv.at[q],
            device_id=peer(1), device_id_type=MESH)
        whole.wait_recv()
        summed.append(whole)
        parts = [RB[q, d] for d in range(ndev)]
        while len(parts) > 1:
            parts = [sum(parts[d + 1:d + 2], parts[d]) for d in range(0, len(parts), 2)]
        row = parts[0]
        return [row[:, k:k + 1] for k in range(len(sums))]

    def combine(t):
        n0, m0, m1, m2, m3, m4 = t
        n1 = m0 - n0
        n2 = m1 - n1
        l1, l2 = m1 / m0, m2 / m0
        d1 = m2 - l1 * m1
        e = m3 - l1 * m2
        l3 = jnp.where(d1 > 0, e / d1, 0.0)
        d2 = m4 - l2 * m2 - l3 * e
        y1 = n1 - l1 * n0
        y2 = n2 - l2 * n0 - l3 * y1
        c2 = jnp.where(d2 > 0, y2 / d2, 0.0)
        c1 = jnp.where(d1 > 0, y1 / d1, 0.0) - l3 * c2
        c0 = n0 / m0 - l1 * c1 - l2 * c2
        return c0, c1, c2

    zacc = jnp.zeros((8, 128), F32)
    wait_recv(p_copy)
    merge(P0, P0Y, None)
    for i in range(nx):
        AP[i] = apply_pressure(P0, D + i, ny)[1]
    wait_send(p_copy)

    def clear_change(i, c):
        DC[i] = zero
        return c
    loop(clear_change, 0)
    local[3].wait()
    local[4].wait()

    msent = []

    def retire(queue):
        if len(queue) == 2:
            wait_send(queue.pop(0))
    for outer in range(OUTER):
        base = 1 + INNER * outer

        u0 = U.at[INNER * outer]

        def p_start(i, acc):
            if outer > 0:
                m_change(i, 0)
            own = slice(0, ny)
            rhs = (STO[D + i, own, :] * p_old[i] + step_time * fsource[i] - BIO[D + i, own, :] * DC[i]
                   + STAB[D + i, own, :] * P0[D + i, own, :])
            r = rhs - AP[i]
            u = r * PINV[D + i, own, :]
            u0[D + i, own, :] = u
            return acc + fold(r * u)
        if outer > 0:
            wait_send(made_p)
        n0 = loop(p_start, zacc)
        stage_corners(u0, UCS.at[outer])
        made_p = wide_field(u0, UY.at[outer], UCS.at[outer], UCR.at[outer], D, psend, precv)
        start(made_p)
        if outer > 0:
            loop(m_after, 0)
        if outer == 0:
            rim()
            loop(stiff_face, 0, 0, nx + 1)
            loop(coefs, 0)
            wait_recv(d_copy)
            wait_send(d_copy)

            def keep_ad(i, ws, outs, c):
                for a in range(3):
                    AD[a, i] = outs[a]
                return c
            apply_mech(0, keep_ad, 0)
            local[5].wait()
        sums = [n0]
        wait_recv(made_p)
        merge(u0, UY.at[outer], UCR.at[outer])
        for k in range(INNER):
            sums = [jnp.sum(v, keepdims=True) for v in sums]
            F = U.at[INNER * outer + k]
            reach = 0 if k == INNER - 1 else D - 1 - k
            even, odd = zacc, zacc
            for j in range(D - reach, D + nx + reach):
                own = D <= j < D + nx
                v, w = apply_pressure(F, j, wide if k < INNER - 1 else ny)
                if own:
                    WP[k, j - D] = w[:ny]
                    even = even + fold(v[:ny] * w[:ny])
                if k < INNER - 1:
                    u = w * PINV[j] - v
                    U[INNER * outer + k + 1, j] = u
                    if own:
                        odd = odd + fold(u[:ny] * w[:ny])
            sums += [even] if k == INNER - 1 else [even, odd]
        cs = combine(all_sum(2 * outer, sums))

        for j in range(D - 1, D + nx):
            v = P0[j]
            for k in range(INNER):
                v = v + cs[k] * U[INNER * outer + k, j]
            P0[j] = v

        def m_start(i, acc):
            loadw = BIO[D + i] * P0[D + i]
            load = loadw[:ny]
            below = (BIO[D + i - 1, 0:ny, :] * P0[D + i - 1, 0:ny, :], dnw(loadw)[:ny],
                     jnp.where(first_lane, 0.0, dnz(load)))
            r = [bforce[a, i] + (below[a] - load) - AD[a, i] for a in range(3)]
            u = block_solve(i, r)
            put_vector(base, i, u)
            return acc + dot3(r, u)
        retire(msent)
        made = vector_field(base)

        def send_planes(f, made):
            put_corners(f)
            start(made, True)
        n0 = loop(m_start, zacc, half=functools.partial(send_planes, base, made))
        start(made, False)
        msent.append(made)

        def p_after(i, c):
            if outer == OUTER - 1:
                p_out[i] = P0[D + i, 0:ny, :]
            else:
                v = AP[i]
                for k in range(INNER):
                    v = v + cs[k] * WP[k, i]
                AP[i] = v
            return c
        loop(p_after, 0)
        sums = [n0]
        for k in range(INNER):
            sums = [jnp.sum(v, keepdims=True) for v in sums]
            wait_recv(made)

            def m_step(i, v, w, c):
                if outer < OUTER - 1:
                    for a in range(3):
                        WM[k, a, i] = w[a]
                even = c[0] + dot3(v, w)
                if k == INNER - 1:
                    return (even,)
                z = block_solve(i, w)
                u = [z[a] - v[a] for a in range(3)]
                put_vector(base + k + 1, i, u)
                return even, c[1] + dot3(u, w)
            half = None
            if k < INNER - 1:
                retire(msent)
                made = vector_field(base + k + 1)
                half = functools.partial(send_planes, base + k + 1, made)
            sums += apply_mech(base + k, m_step, (zacc,) * (1 if k == INNER - 1 else 2), half)
            if k < INNER - 1:
                start(made, False)
                msent.append(made)
        cs = combine(all_sum(2 * outer + 1, sums))

        def mixed(get, cs=cs, base=base):
            v = cs[0] * get(base)
            for k in range(1, INNER):
                v = v + cs[k] * get(base + k)
            return v

        def m_change(i, c):
            row = slice(i, i + 1)
            change = [mixed(lambda f, a=a: MX[f, a, i + 1]) for a in range(3)]
            cx = mixed(lambda f: MX[f, 0, i + 2])
            cy = upy(change[1], mixed(lambda f: MYH[f, 1, 1, row, :]))
            cz = jnp.where(last_lane, 0.0, upz(change[2]))
            DC[i] = DC[i] + (cx - change[0] + cy - change[1] + cz - change[2])
            return c

        def m_after(i, c, cs=cs, mixed=mixed, outer=outer):
            for a in range(3):
                before = MX[0, a, i + 1] if outer == 0 else d_out[a, i]
                d_out[a, i] = before + mixed(lambda f, a=a: MX[f, a, i + 1])
            if outer < OUTER - 1:
                for a in range(3):
                    v = AD[a, i]
                    for k in range(INNER):
                        v = v + cs[k] * WM[k, a, i]
                    AD[a, i] = v
            return c
        if outer == OUTER - 1:
            loop(m_after, 0)

    for made in msent + [codes_copy, made_p]:
        wait_send(made)
    for copy in summed:
        copy.wait_send()


def on_device(dims, d_old, p_old, bforce, fsource, ids, materials):
    ngx, ngy, nx, ny, nz, nmat = dims
    nf = 1 + OUTER * INNER
    nq = 2 * OUTER

    def vm(*shape, dtype=F32):
        return pltpu.VMEM(shape, dtype)
    plane, strip = (ny, nz), (nx, nz)
    cell = (nx, ny, nz)
    ext = (nx + 2, ny, nz)
    big = (nx + 2 * D, ny + 8, nz)
    edge = (2, nx, 8, nz)
    corner = (4, D - 1, 2 if D == 3 else 4, nz)
    dma = pltpu.SemaphoreType.DMA
    scratch = [
        vm(*cell), vm(3, *cell), vm(*cell), vm(*cell, dtype=jnp.int32), dma((6,)),
        vm(*big, dtype=jnp.int32), vm(*edge, dtype=jnp.int32),
        vm(*corner, dtype=jnp.int32), vm(*corner, dtype=jnp.int32),
        vm(*big), vm(*big), vm(*big), vm(*big), vm(*big), vm(*big), vm(*strip),
        vm(nx + 1, *plane), vm(2, *cell), vm(2, *cell), vm(*cell),
        vm(*big), vm(*big), vm(*big), vm(*big), vm(*big),
        vm(3, *cell), vm(*cell),
        vm(*big), vm(*edge), vm(OUTER * INNER, *big), vm(OUTER, *edge), vm(OUTER, *corner), vm(OUTER, *corner),
        vm(nf, 3, *ext), vm(nf, 2, 3, *strip), vm(nf, 2, 3, *strip), vm(nf, 2, 1, nz), vm(nf, 2, 1, nz),
        vm(INNER, *cell), vm(INNER, 3, *cell), vm(*cell), vm(3, *cell), vm(*cell),
        vm(*strip), vm(*cell), vm(nq, ngx * ngy, 1, 128),
        dma((8,)), dma((8,)), dma((4,)), dma((4,)), dma((8,)), dma((8,)), dma((2, 6)), dma((2, 6)),
        dma((nq,)), dma((nq,)),
    ]
    block = pl.BlockSpec(memory_space=pltpu.VMEM)
    return pl.pallas_call(
        functools.partial(kernel, dims),
        out_shape=(pltpu.VMEM(d_old.shape, F32), pltpu.VMEM(p_old.shape, F32)),
        in_specs=[pl.BlockSpec(memory_space=pltpu.SMEM)] + [pl.BlockSpec(memory_space=pl.ANY)] * 5,
        out_specs=(block, block),
        scratch_shapes=scratch,
        compiler_params=pltpu.CompilerParams(
            collective_id=0, has_side_effects=True,
            vmem_limit_bytes=VMEM_BYTES - 4 * (d_old.size + p_old.size) - 131072),
        name="poro",
    )(materials, d_old, p_old, bforce, fsource, ids)


def solution(mesh):
    ngx, ngy = mesh.shape["gx"], mesh.shape["gy"]

    def body(d_old, p_old, bforce, fsource, ids, materials):
        dims = (ngx, ngy, *p_old.shape, materials.shape[1])
        return on_device(dims, d_old, p_old, bforce, fsource, ids, materials)

    return jax.shard_map(
        body,
        mesh=mesh,
        in_specs=(P(None, "gx", "gy", None), P("gx", "gy", None), P(None, "gx", "gy", None),
                  P("gx", "gy", None), P("gx", "gy", None), P()),
        out_specs=(P(None, "gx", "gy", None), P("gx", "gy", None)),
        check_vma=False,
    )
```

```python
import functools
import jax
import jax.numpy as jnp
from jax import lax
from jax.experimental import pallas as pl
from jax.experimental.pallas import tpu as pltpu
from jax.sharding import PartitionSpec as P

OUTER = 2
INNER = 3
step_time = 4.0
D = INNER
TINY = 1e-30
VMEM_BYTES = 67043328
DIAGONALS = ((1, -1), (-1, 1), (1, 1), (-1, -1))
MESH = pl.DeviceIdType.MESH
F32 = jnp.float32


def kernel(dims, *refs):
    ngx, ngy, nx, ny, nz, nmat = dims
    (mat, d_hbm, p_hbm, bf_hbm, fs_hbm, ids_hbm, d_out, p_out,
     p_old, bforce, fsource, ids, lsem,
     XI, XIY, XIS, XIR, LAM, SHR, PRM, BIO, STO, STAB, LAMY,
     SX, SY, SZ, SSUM, FX, FY, FZ, DIAG, PINV, HB, KF,
     P0, P0Y, P0S, P0R, U, UY, UCS, UCR, VY, VCS, VCR, RX, RY, RCS, RCR, MX, MYS, MYH, MCS, MCH,
     WP, WM, AP, AD, DC, LY, LW, RB,
     isend, irecv, zsend, zrecv, vsend, vrecv, wsend, wrecv, psend, precv, msend, mrecv, rsend, rrecv) = refs
    gx, gy = lax.axis_index("gx"), lax.axis_index("gy")
    local = [pltpu.make_async_copy(src, dst, lsem.at[n]) for n, (src, dst) in enumerate((
        (ids_hbm, ids), (p_hbm, P0.at[pl.ds(D, nx), pl.ds(0, ny)]), (d_hbm, MX.at[0, :, pl.ds(1, nx)]),
        (p_hbm, p_old), (fs_hbm, fsource), (bf_hbm, bforce)))]
    for copy in local:
        copy.start()
    barrier = pltpu.get_barrier_semaphore()
    me, ndev = gx * ngy + gy, ngx * ngy

    def peer(d):
        t = lax.rem(me + d, ndev)
        return lax.div(t, ngy), lax.rem(t, ngy)
    has = {(-1, 0): gx > 0, (1, 0): gx < ngx - 1, (0, -1): gy > 0, (0, 1): gy < ngy - 1}
    for c in DIAGONALS:
        has[c] = jnp.logical_and(has[(c[0], 0)], has[(0, c[1])])

    rows = lax.broadcasted_iota(jnp.int32, (ny, nz), 0)
    lanes = lax.broadcasted_iota(jnp.int32, (ny, nz), 1)
    lanes8 = lax.broadcasted_iota(jnp.int32, (nx, nz), 1)
    rows8 = lax.broadcasted_iota(jnp.int32, (nx, nz), 0)
    lane1 = lax.broadcasted_iota(jnp.int32, (1, 128), 1)
    first_row, last_row = rows == 0, rows == ny - 1
    first_lane, last_lane = lanes == 0, lanes == nz - 1
    zero = jnp.zeros((ny, nz), F32)
    near = lax.broadcasted_iota(jnp.int32, (8, nz), 0) < 4
    wide = ny + 8
    first_wide = lax.broadcasted_iota(jnp.int32, (wide, nz), 1) == 0
    last_wide = lax.broadcasted_iota(jnp.int32, (wide, nz), 1) == nz - 1
    zero8 = jnp.zeros((nx, nz), F32)

    def upz(v):
        return pltpu.roll(v, nz - 1, 1)

    def dnz(v):
        return pltpu.roll(v, 1, 1)

    def upy(v, halo):
        return jnp.where(last_row, halo, pltpu.roll(v, ny - 1, 0))

    def dny(v, halo):
        return jnp.where(first_row, halo, pltpu.roll(v, 1, 0))

    def upw(v):
        return pltpu.roll(v, wide - 1, 0)

    def dnw(v):
        return pltpu.roll(v, 1, 0)

    def fold(v):
        out = None
        for i in range(0, ny, 8):
            for j in range(0, nz, 128):
                part = v[i:i + 8, j:j + 128]
                out = part if out is None else out + part
        return out

    def loop(body, init, low=0, high=nx, half=None):
        order = [low, high - 1] + list(range(low + 1, high - 1))
        for n, i in enumerate(order):
            init = body(i, init)
            if n == 1 and half is not None:
                half()
        return init

    def copies_of(pairs, send, recv):
        made = []
        for n, (src, dst, off) in enumerate(pairs):
            copy = pltpu.make_async_remote_copy(
                src_ref=src, dst_ref=dst, send_sem=send.at[n], recv_sem=recv.at[n],
                device_id=(gx + off[0], gy + off[1]), device_id_type=MESH)
            made.append((copy, off))
        return made

    def start(made, along=None):
        for copy, off in made:
            if along is not None and (off[0] != 0) != along:
                continue
            @pl.when(has[off])
            def _(copy=copy):
                copy.start()

    def wait_recv(made):
        for copy, off in made:
            @pl.when(has[(-off[0], -off[1])])
            def _(copy=copy):
                copy.wait_recv()

    def wait_send(made):
        for copy, off in made:
            @pl.when(has[off])
            def _(copy=copy):
                copy.wait_send()

    def wide_field(F, Y, CS, CR, depth, send, recv):
        pairs = [(F.at[pl.ds(D, depth), pl.ds(0, ny)], F.at[pl.ds(D + nx, depth), pl.ds(0, ny)], (-1, 0)),
                 (F.at[pl.ds(D + nx - depth, depth), pl.ds(0, ny)], F.at[pl.ds(D - depth, depth), pl.ds(0, ny)], (1, 0)),
                 (F.at[pl.ds(D, nx), pl.ds(0, 8)], Y.at[1], (0, -1)),
                 (F.at[pl.ds(D, nx), pl.ds(ny - 8, 8)], Y.at[0], (0, 1))]
        if CS is not None:
            pairs += [(CS.at[c], CR.at[c], off) for c, off in enumerate(DIAGONALS)]
        return copies_of(pairs, send, recv)

    def stage_corners(F, CS):
        n, m = CS.shape[1:3]
        for c, (sx, sy) in enumerate(DIAGONALS):
            for t in range(n):
                CS[c, t] = F[D + (t if sx < 0 else nx - n + t), (0 if sy < 0 else ny - m):(m if sy < 0 else ny), :]

    def clear_missing(F, Y, CR, depth):
        none = jnp.zeros((wide, nz), F.dtype)
        for side, low in ((-1, D - depth), (1, D + nx)):
            @pl.when(jnp.logical_not(has[(side, 0)]))
            def _(low=low):
                for t in range(depth):
                    F[low + t] = none
        for side, s in ((-1, 0), (1, 1)):
            @pl.when(jnp.logical_not(has[(0, side)]))
            def _(s=s):
                for i in range(nx):
                    Y[s, i] = none[:8]
        if CR is not None:
            for c, off in enumerate(DIAGONALS):
                @pl.when(jnp.logical_not(has[(-off[0], -off[1])]))
                def _(c=c):
                    CR[c] = jnp.zeros(CR.shape[1:], F.dtype)

    def late_field(o):
        last = U.at[INNER * o + INNER - 1]
        pairs = [(last.at[pl.ds(D + nx - 2, 1), pl.ds(0, ny)], last.at[pl.ds(D - 2, 1), pl.ds(0, ny)], (1, 0)),
                 (last.at[pl.ds(D, nx), pl.ds(ny - 8, 8)], VY.at[o], (0, 1))]
        pairs += [(VCS.at[o, c], VCR.at[o, c], off) for c, off in enumerate(DIAGONALS[:3])]
        return copies_of(pairs, vsend, vrecv)

    def stage_late(o):
        for c, (sx, sy) in enumerate(DIAGONALS[:3]):
            for k in range(1, INNER):
                for t in range(2):
                    VCS[o, c, k - 1, t] = U[INNER * o + k, D + (t if sx < 0 else nx - 2 + t),
                                            (0 if sy < 0 else ny - 2):(2 if sy < 0 else ny), :]

    def merge_late(o):
        f = INNER * o + INNER - 1
        for i in range(nx):
            U[f, D + i, ny:, :] = jnp.where(near, U[f, D + i, ny:, :], VY[o, i])
        for c, (sx, sy) in enumerate(DIAGONALS[:3]):
            for k in range(1, INNER):
                for t in range(2):
                    low = ny if sy < 0 else wide - 2
                    U[INNER * o + k, (D + nx + t) if sx < 0 else (D - 2 + t), low:low + 2, :] = VCR[o, c, k - 1, t]

    def load_field(o):
        F = RX.at[o]
        pairs = [(F.at[:, pl.ds(1, 1), pl.ds(0, ny)], F.at[:, pl.ds(nx + 1, 1), pl.ds(0, ny)], (-1, 0)),
                 (F.at[:, pl.ds(nx, 1), pl.ds(0, ny)], F.at[:, pl.ds(0, 1), pl.ds(0, ny)], (1, 0)),
                 (F.at[:, pl.ds(1, nx), pl.ds(0, 8)], RY.at[o, 1], (0, -1)),
                 (F.at[:, pl.ds(1, nx), pl.ds(ny - 8, 8)], RY.at[o, 0], (0, 1)),
                 (RCS.at[o, 0], RCR.at[o, 0], DIAGONALS[0]), (RCS.at[o, 1], RCR.at[o, 1], DIAGONALS[1])]
        return copies_of(pairs, wsend, wrecv)

    def stage_load(o):
        for a in range(3):
            RCS[o, 0, a] = RX[o, a, nx, 0:1, :]
            RCS[o, 1, a] = RX[o, a, 1, ny - 1:ny, :]

    def merge_load(o):
        for a in range(3):
            for i in range(nx):
                RX[o, a, i + 1, ny:, :] = jnp.where(near, RY[o, 1, a, i], RY[o, 0, a, i])
            RX[o, a, 0, ny:ny + 1, :] = RCR[o, 0, a]
            RX[o, a, nx + 1, wide - 1:wide, :] = RCR[o, 1, a]

    def clear_late(o):
        none = jnp.zeros((wide, nz), F32)

        @pl.when(jnp.logical_not(has[(-1, 0)]))
        def _():
            U[INNER * o + INNER - 1, D - 2] = none
            for a in range(3):
                RX[o, a, 0] = none

        @pl.when(jnp.logical_not(has[(1, 0)]))
        def _():
            for a in range(3):
                RX[o, a, nx + 1] = none

        @pl.when(jnp.logical_not(has[(0, -1)]))
        def _():
            for i in range(nx):
                VY[o, i] = none[:8]
                for a in range(3):
                    RY[o, 0, a, i] = none[:8]

        @pl.when(jnp.logical_not(has[(0, 1)]))
        def _():
            for i in range(nx):
                for a in range(3):
                    RY[o, 1, a, i] = none[:8]
        for c, off in enumerate(DIAGONALS[:3]):
            @pl.when(jnp.logical_not(has[(-off[0], -off[1])]))
            def _(c=c):
                VCR[o, c] = jnp.zeros(VCR.shape[2:], F32)
                if c < 2:
                    RCR[o, c] = jnp.zeros(RCR.shape[2:], F32)

    def merge(F, Y, CR):
        for i in range(nx):
            F[D + i, ny:, :] = jnp.where(near, Y[1, i], Y[0, i])
        if CR is not None:
            n, m = CR.shape[1:3]
            for c, (sx, sy) in enumerate(DIAGONALS):
                for t in range(n):
                    low = ny if sy < 0 else wide - m
                    F[(D + nx + t) if sx < 0 else (D - n + t), low:low + m, :] = CR[c, t]

    def vector_field(f):
        return copies_of(
            [(MX.at[f, :, 1], MX.at[f, :, nx + 1], (-1, 0)), (MX.at[f, :, nx], MX.at[f, :, 0], (1, 0)),
             (MYS.at[f, 0], MYH.at[f, 1], (0, -1)), (MYS.at[f, 1], MYH.at[f, 0], (0, 1)),
             (MCS.at[f, 0], MCH.at[f, 0], (1, -1)), (MCS.at[f, 1], MCH.at[f, 1], (-1, 1))],
            msend.at[f % 2], mrecv.at[f % 2])

    def put_vector(f, i, vs):
        for a in range(3):
            MX[f, a, i + 1] = vs[a]
            MYS[f, 0, a, slice(i, i + 1), :] = vs[a][0:1]
            MYS[f, 1, a, slice(i, i + 1), :] = vs[a][ny - 1:ny]

    def put_corners(f):
        MCS[f, 0] = MX[f, 1, nx, 0:1, :]
        MCS[f, 1] = MX[f, 0, 1, ny - 1:ny, :]

    nf = 1 + OUTER * INNER
    def clear(f, c):
        for s in range(2):
            MCH[f, s] = jnp.zeros((1, nz), F32)
            for a in range(3):
                MX[f, a, s * (nx + 1)] = zero
                MYH[f, s, a] = zero8
        return c
    lax.fori_loop(0, nf, clear, 0)
    for d in range(1, ndev):
        pl.semaphore_signal(barrier, inc=1, device_id=peer(d), device_id_type=MESH)


    def stage_values(i, c):
        for side, y in ((0, 0), (1, ny - 1)):
            for a in range(3):
                MYS[0, side, a, i:i + 1, :] = MX[0, a, i + 1, y:y + 1, :]
        return c
    local[0].wait()
    for i in range(nx):
        XI[D + i, 0:ny, :] = ids[i] + 1
    stage_corners(XI, XIS)
    local[1].wait()
    stage_corners(P0, P0S)
    pl.semaphore_wait(barrier, ndev - 1)
    p_copy = wide_field(P0, P0Y, P0S, P0R, 2, zsend, zrecv)
    codes_copy = wide_field(XI, XIY, XIS, XIR, D, isend, irecv)
    d_copy = vector_field(0)
    start(p_copy)
    start(codes_copy)
    local[2].wait()
    loop(stage_values, 0)
    put_corners(0)
    start(d_copy)
    clear_missing(XI, XIY, XIR, D)
    clear_missing(P0, P0Y, P0R, 2)
    for outer in range(OUTER):
        clear_missing(U.at[INNER * outer], UY.at[outer], UCR.at[outer], D)
        clear_late(outer)

    def lookup(code, table_rows):
        out = [jnp.zeros(code.shape, F32) for _ in table_rows]
        for m in range(nmat):
            hit = code == m + 1
            out = [jnp.where(hit, mat[t, m], v) for t, v in zip(table_rows, out)]
        return out

    def look(j, part):
        code = XI[j, part, :]
        lam, shr, prm, sto, bio = lookup(code, (0, 1, 2, 3, 4))
        bio = 0.25 * bio
        LAM[j, part, :] = lam
        SHR[j, part, :] = shr
        PRM[j, part, :] = prm
        BIO[j, part, :] = bio
        STO[j, part, :] = sto
        STAB[j, part, :] = bio * bio / jnp.maximum(lam + 2.0 / 3.0 * shr, TINY)
    for i in range(nx):
        look(D + i, slice(0, ny))
    wait_recv(codes_copy)
    merge(XI, XIY, XIR)
    for i in range(nx):
        look(D + i, slice(ny, wide))
    for j in (D - 1, D + nx):
        look(j, slice(0, wide))

    def harmonic(one, two):
        return (2.0 * step_time) * one * two / jnp.maximum(one + two, TINY)

    def flow(j):
        prm = PRM[j]
        fzu = jnp.where(last_wide, 0.0, harmonic(prm, upz(prm)))
        fyu = harmonic(prm, upw(prm))
        FY[j], FZ[j] = fyu, fzu
        diag = STO[j] + STAB[j] + (FX[j] + FX[j + 1] + fyu + dnw(fyu) + fzu + dnz(fzu))
        DIAG[j] = diag
        PINV[j] = jnp.where(XI[j] > 0, 1.0 / jnp.maximum(diag, TINY), 0.0)

    def face(j):
        FX[j] = harmonic(PRM[j - 1], PRM[j])
    for j in range(D, D + nx + 1):
        face(j)
    for j in range(D, D + nx):
        flow(j)

    def rim():
        outer_planes = [j for j in range(nx + 2 * D) if j < D - 1 or j > D + nx]
        for j in outer_planes:
            look(j, slice(0, wide))
        for j in list(range(1, D)) + list(range(D + nx + 1, nx + 2 * D)):
            face(j)
        for j in list(range(1, D)) + list(range(D + nx, nx + 2 * D - 1)):
            flow(j)

    def stiff_face(t):
        SX[t] = 0.5 * (SHR[D + t - 2] + SHR[D + t - 1])

    def coefs(i):
        shr, lam = SHR[D + i], LAM[D + i]
        half = 0.5 * shr
        syu = 0.5 * (shr + upw(shr))
        syd = dnw(syu)
        szu = half + jnp.where(last_wide, 0.0, 0.5 * upz(shr))
        szd = half + jnp.where(first_wide, 0.0, 0.5 * dnz(shr))
        total = SX[i + 1] + SX[i + 2] + syu + syd + szu + szd
        if 0 <= i < nx:
            LAMY[slice(i, i + 1), :] = LAM[D + i, wide - 1:wide, :]
            SY[1, i], SY[0, i] = syu[:ny], syd[:ny]
            SZ[1, i] = jnp.where(last_lane, 0.0, szu[:ny])
            SZ[0, i] = jnp.where(first_lane, 0.0, szd[:ny])
            SSUM[i] = total[:ny]
        inside = XI[D + i] > 0
        hs = []
        for a, below in enumerate((LAM[D + i - 1], dnw(lam), jnp.where(first_wide, 0.0, dnz(lam)))):
            h = jnp.where(inside, 1.0 / jnp.maximum(total + below, TINY), 0.0)
            HB[a, i + 1] = h
            hs.append(h)
        KF[i + 1] = lam / (1.0 + lam * (hs[0] + hs[1] + hs[2]))

    def apply_pressure(F, j, rows):
        v = F[j]
        out = (DIAG[j] * v - FX[j + 1] * F[j + 1] - FX[j] * F[j - 1]
               - FY[j] * upw(v) - dnw(FY[j] * v)
               - FZ[j] * upz(v) - dnz(FZ[j] * v))
        return v[:rows], out[:rows]

    def apply_mech(f, emit, init, half=None):
        m = [MYH[f, 0, a] for a in range(3)]
        ahead = jnp.where(rows8 == nx - 1, MCH[f, 1], pltpu.roll(m[0], nx - 1, 0))
        z8 = jnp.where(lanes8 == nz - 1, 0.0, pltpu.roll(m[2], nz - 1, 1))
        LY[...] = LAMY[...] * (ahead - m[0] + MYS[f, 0, 1] - m[1] + z8 - m[2])
        m = [MX[f, a, 0] for a in range(3)]
        below_first = LAM[D - 1, 0:ny, :] * (MX[f, 0, 1] - m[0] + upy(m[1], MCH[f, 0]) - m[1]
                          + jnp.where(last_lane, 0.0, upz(m[2])) - m[2])

        def weigh(i):
            w = [MX[f, a, i + 1] for a in range(3)]
            return LAM[D + i, 0:ny, :] * (MX[f, 0, i + 2] - w[0] + upy(w[1], MYH[f, 1, 1, i:i + 1, :]) - w[1]
                                 + jnp.where(last_lane, 0.0, upz(w[2])) - w[2])

        def body(i, c):
            row = slice(i, i + 1)
            ws, outs, div = [], [], None
            for a in range(3):
                w, wx = MX[f, a, i + 1], MX[f, a, i + 2]
                wy, wz = upy(w, MYH[f, 1, a, row, :]), upz(w)
                out = (SSUM[i] * w - SX[i + 2, 0:ny, :] * wx - SX[i + 1, 0:ny, :] * MX[f, a, i]
                       - SY[1, i] * wy - SY[0, i] * dny(w, MYH[f, 0, a, row, :])
                       - SZ[1, i] * wz - SZ[0, i] * dnz(w))
                part = (wx, wy, jnp.where(last_lane, 0.0, wz))[a] - w
                div = part if div is None else div + part
                ws.append(w)
                outs.append(out)
            weighted = LAM[D + i, 0:ny, :] * div
            LW[i] = weighted
            before = below_first if i == 0 else weigh(i - 1) if i == nx - 1 else LW[i - 1]
            below = (before, dny(weighted, LY[row, :]), jnp.where(first_lane, 0.0, dnz(weighted)))
            outs = [outs[a] + (below[a] - weighted) for a in range(3)]
            return emit(i, ws, outs, c)
        return loop(body, init, half=half)

    def block_solve(i, r, rows):
        part = slice(0, rows)
        scaled = [r[a] * HB[a, i + 1, part, :] for a in range(3)]
        tail = KF[i + 1, part, :] * (scaled[0] + scaled[1] + scaled[2])
        return [scaled[a] - HB[a, i + 1, part, :] * tail for a in range(3)]

    def dot3(a, b):
        return fold(a[0] * b[0] + a[1] * b[1] + a[2] * b[2])

    summed = []

    def all_sum(q, sums, meanwhile=None):
        row = jnp.zeros((1, 128), F32)
        for k, s in enumerate(sums):
            row = jnp.where(lane1 == k, jnp.sum(s, keepdims=True), row)
        RB[q, me] = row
        for d in sorted(range(1, ndev), key=lambda d: -min(d, ndev - d)):
            copy = pltpu.make_async_remote_copy(
                src_ref=RB.at[q, me], dst_ref=RB.at[q, me], send_sem=rsend.at[q],
                recv_sem=rrecv.at[q], device_id=peer(d), device_id_type=MESH)
            copy.start()
        every = RB.at[q, pl.ds(0, ndev - 1)]
        whole = pltpu.make_async_remote_copy(
            src_ref=every, dst_ref=every, send_sem=rsend.at[q], recv_sem=rrecv.at[q],
            device_id=peer(1), device_id_type=MESH)
        if meanwhile is not None:
            meanwhile()
        whole.wait_recv()
        summed.append(whole)
        parts = [RB[q, d] for d in range(ndev)]
        while len(parts) > 1:
            parts = [sum(parts[d + 1:d + 2], parts[d]) for d in range(0, len(parts), 2)]
        row = parts[0]
        return [row[:, k:k + 1] for k in range(len(sums))]

    def combine(t):
        n0, m0, m1, m2, m3, m4 = t
        n1 = m0 - n0
        n2 = m1 - n1
        l1, l2 = m1 / m0, m2 / m0
        d1 = m2 - l1 * m1
        e = m3 - l1 * m2
        l3 = jnp.where(d1 > 0, e / d1, 0.0)
        d2 = m4 - l2 * m2 - l3 * e
        y1 = n1 - l1 * n0
        y2 = n2 - l2 * n0 - l3 * y1
        c2 = jnp.where(d2 > 0, y2 / d2, 0.0)
        c1 = jnp.where(d1 > 0, y1 / d1, 0.0) - l3 * c2
        c0 = n0 / m0 - l1 * c1 - l2 * c2
        return c0, c1, c2

    zacc = jnp.zeros((8, 128), F32)
    wait_recv(p_copy)
    merge(P0, P0Y, P0R)
    for i in range(nx):
        AP[i] = apply_pressure(P0, D + i, ny)[1]
    wait_send(p_copy)

    def clear_change(i, c):
        DC[i] = zero
        return c
    loop(clear_change, 0)
    local[3].wait()
    local[4].wait()

    msent = []

    def retire(queue):
        if len(queue) == 2:
            wait_send(queue.pop(0))
    for outer in range(OUTER):
        base = 1 + INNER * outer

        u0 = U.at[INNER * outer]

        def p_start(i, acc):
            if outer > 0:
                m_change(i, 0)
            own = slice(0, ny)
            rhs = (STO[D + i, own, :] * p_old[i] + step_time * fsource[i] - BIO[D + i, own, :] * DC[i]
                   + STAB[D + i, own, :] * P0[D + i, own, :])
            r = rhs - AP[i]
            u = r * PINV[D + i, own, :]
            u0[D + i, own, :] = u
            return acc + fold(r * u)
        if outer > 0:
            wait_send(made_p)
        n0 = loop(p_start, zacc)
        stage_corners(u0, UCS.at[outer])
        made_p = wide_field(u0, UY.at[outer], UCS.at[outer], UCR.at[outer], D, psend, precv)
        start(made_p)
        if outer > 0:
            loop(m_after, 0)
        if outer == 0:
            rim()
            for t in range(nx + 3):
                stiff_face(t)
            for i in range(-1, nx + 1):
                coefs(i)
            wait_recv(d_copy)
            wait_send(d_copy)

            def keep_ad(i, ws, outs, c):
                for a in range(3):
                    AD[a, i] = outs[a]
                    RX[0, a, i + 1, 0:ny, :] = bforce[a, i] - outs[a]
                return c
            local[5].wait()
            apply_mech(0, keep_ad, 0)
        else:
            wait_send(made_r)
        stage_load(outer)
        made_r = load_field(outer)
        start(made_r)
        sums = [n0]
        wait_recv(made_p)
        merge(u0, UY.at[outer], UCR.at[outer])
        for k in range(INNER):
            sums = [jnp.sum(v, keepdims=True) for v in sums]
            F = U.at[INNER * outer + k]
            reach = 0 if k == INNER - 1 else D - 1 - k
            even, odd = zacc, zacc
            for j in range(D - reach, D + nx + reach):
                own = D <= j < D + nx
                v, w = apply_pressure(F, j, wide if k < INNER - 1 else ny)
                if own:
                    WP[k, j - D] = w[:ny]
                    even = even + fold(v[:ny] * w[:ny])
                if k < INNER - 1:
                    u = w * PINV[j] - v
                    U[INNER * outer + k + 1, j] = u
                    if own:
                        odd = odd + fold(u[:ny] * w[:ny])
            sums += [even] if k == INNER - 1 else [even, odd]
            if k == INNER - 2:
                if outer > 0:
                    wait_send(made_v)
                stage_late(outer)
                made_v = late_field(outer)
                start(made_v)

        def arrivals():
            wait_recv(made_r)
            merge_load(outer)
            wait_recv(made_v)
            merge_late(outer)
        cs = combine(all_sum(2 * outer, sums, arrivals))

        for j in range(D - 2, D + nx + 1):
            v = P0[j]
            for k in range(INNER):
                v = v + cs[k] * U[INNER * outer + k, j]
            P0[j] = v

        n0 = zacc
        for i in range(-1, nx + 1):
            load = BIO[D + i] * P0[D + i]
            below = (BIO[D + i - 1] * P0[D + i - 1], dnw(load), jnp.where(first_wide, 0.0, dnz(load)))
            r = [RX[outer, a, i + 1] + (below[a] - load) for a in range(3)]
            u = block_solve(i, r, wide)
            if 0 <= i < nx:
                put_vector(base, i, [v[:ny] for v in u])
                for a in range(3):
                    MYH[base, 1, a, i:i + 1, :] = u[a][ny:ny + 1]
                    MYH[base, 0, a, i:i + 1, :] = u[a][wide - 1:wide]
                n0 = n0 + dot3([v[:ny] for v in r], [v[:ny] for v in u])
            else:
                for a in range(3):
                    MX[base, a, i + 1] = u[a][:ny]
                if i < 0:
                    MCH[base, 0] = u[1][ny:ny + 1]
                else:
                    MCH[base, 1] = u[0][wide - 1:wide]

        def send_planes(f, made):
            put_corners(f)
            start(made, True)

        def p_after(i, c):
            if outer == OUTER - 1:
                p_out[i] = P0[D + i, 0:ny, :]
            else:
                v = AP[i]
                for k in range(INNER):
                    v = v + cs[k] * WP[k, i]
                AP[i] = v
            return c
        loop(p_after, 0)
        sums = [n0]
        for k in range(INNER):
            sums = [jnp.sum(v, keepdims=True) for v in sums]
            if k > 0:
                wait_recv(made)

            def m_step(i, v, w, c):
                if outer < OUTER - 1:
                    for a in range(3):
                        WM[k, a, i] = w[a]
                even = c[0] + dot3(v, w)
                if k == INNER - 1:
                    return (even,)
                z = block_solve(i, w, ny)
                u = [z[a] - v[a] for a in range(3)]
                put_vector(base + k + 1, i, u)
                return even, c[1] + dot3(u, w)
            half = None
            if k < INNER - 1:
                retire(msent)
                made = vector_field(base + k + 1)
                half = functools.partial(send_planes, base + k + 1, made)
            sums += apply_mech(base + k, m_step, (zacc,) * (1 if k == INNER - 1 else 2), half)
            if k < INNER - 1:
                start(made, False)
                msent.append(made)
        cs = combine(all_sum(2 * outer + 1, sums))

        def mixed(get, cs=cs, base=base):
            v = cs[0] * get(base)
            for k in range(1, INNER):
                v = v + cs[k] * get(base + k)
            return v

        def m_change(i, c):
            row = slice(i, i + 1)
            change = [mixed(lambda f, a=a: MX[f, a, i + 1]) for a in range(3)]
            cx = mixed(lambda f: MX[f, 0, i + 2])
            cy = upy(change[1], mixed(lambda f: MYH[f, 1, 1, row, :]))
            cz = jnp.where(last_lane, 0.0, upz(change[2]))
            DC[i] = DC[i] + (cx - change[0] + cy - change[1] + cz - change[2])
            return c

        def m_after(i, c, cs=cs, mixed=mixed, outer=outer):
            for a in range(3):
                before = MX[0, a, i + 1] if outer == 0 else d_out[a, i]
                d_out[a, i] = before + mixed(lambda f, a=a: MX[f, a, i + 1])
            if outer < OUTER - 1:
                for a in range(3):
                    v = AD[a, i]
                    for k in range(INNER):
                        v = v + cs[k] * WM[k, a, i]
                    RX[outer + 1, a, i + 1, 0:ny, :] = bforce[a, i] - v
            return c
        if outer == OUTER - 1:
            loop(m_after, 0)

    for made in msent + [codes_copy, made_p, made_r, made_v]:
        wait_send(made)
    for copy in summed:
        copy.wait_send()


def on_device(dims, d_old, p_old, bforce, fsource, ids, materials):
    ngx, ngy, nx, ny, nz, nmat = dims
    nf = 1 + OUTER * INNER
    nq = 2 * OUTER

    def vm(*shape, dtype=F32):
        return pltpu.VMEM(shape, dtype)
    plane, strip = (ny, nz), (nx, nz)
    cell = (nx, ny, nz)
    ext = (nx + 2, ny, nz)
    broad = (ny + 8, nz)
    big = (nx + 2 * D, ny + 8, nz)
    edge = (2, nx, 8, nz)
    corner = (4, D - 1, 2 if D == 3 else 4, nz)
    dma = pltpu.SemaphoreType.DMA
    scratch = [
        vm(*cell), vm(3, *cell), vm(*cell), vm(*cell, dtype=jnp.int32), dma((6,)),
        vm(*big, dtype=jnp.int32), vm(*edge, dtype=jnp.int32),
        vm(*corner, dtype=jnp.int32), vm(*corner, dtype=jnp.int32),
        vm(*big), vm(*big), vm(*big), vm(*big), vm(*big), vm(*big), vm(*strip),
        vm(nx + 3, *broad), vm(2, *cell), vm(2, *cell), vm(*cell),
        vm(*big), vm(*big), vm(*big), vm(*big), vm(*big),
        vm(3, nx + 2, *broad), vm(nx + 2, *broad),
        vm(*big), vm(*edge), vm(*corner), vm(*corner), vm(OUTER * INNER, *big), vm(OUTER, *edge), vm(OUTER, *corner), vm(OUTER, *corner),
        vm(OUTER, nx, 8, nz), vm(OUTER, 3, INNER - 1, 2, 2, nz), vm(OUTER, 3, INNER - 1, 2, 2, nz),
        vm(OUTER, 3, nx + 2, *broad), vm(OUTER, 2, 3, nx, 8, nz), vm(OUTER, 2, 3, 1, nz), vm(OUTER, 2, 3, 1, nz),
        vm(nf, 3, *ext), vm(nf, 2, 3, *strip), vm(nf, 2, 3, *strip), vm(nf, 2, 1, nz), vm(nf, 2, 1, nz),
        vm(INNER, *cell), vm(INNER, 3, *cell), vm(*cell), vm(3, *cell), vm(*cell),
        vm(*strip), vm(*cell), vm(nq, ngx * ngy, 1, 128),
        dma((8,)), dma((8,)), dma((8,)), dma((8,)), dma((5,)), dma((5,)), dma((6,)), dma((6,)), dma((8,)), dma((8,)), dma((2, 6)), dma((2, 6)),
        dma((nq,)), dma((nq,)),
    ]
    block = pl.BlockSpec(memory_space=pltpu.VMEM)
    return pl.pallas_call(
        functools.partial(kernel, dims),
        out_shape=(pltpu.VMEM(d_old.shape, F32), pltpu.VMEM(p_old.shape, F32)),
        in_specs=[pl.BlockSpec(memory_space=pltpu.SMEM)] + [pl.BlockSpec(memory_space=pl.ANY)] * 5,
        out_specs=(block, block),
        scratch_shapes=scratch,
        compiler_params=pltpu.CompilerParams(
            collective_id=0, has_side_effects=True,
            vmem_limit_bytes=VMEM_BYTES - 4 * (d_old.size + p_old.size) - 131072),
        name="poro",
    )(materials, d_old, p_old, bforce, fsource, ids)


def solution(mesh):
    ngx, ngy = mesh.shape["gx"], mesh.shape["gy"]

    def body(d_old, p_old, bforce, fsource, ids, materials):
        dims = (ngx, ngy, *p_old.shape, materials.shape[1])
        return on_device(dims, d_old, p_old, bforce, fsource, ids, materials)

    return jax.shard_map(
        body,
        mesh=mesh,
        in_specs=(P(None, "gx", "gy", None), P("gx", "gy", None), P(None, "gx", "gy", None),
                  P("gx", "gy", None), P("gx", "gy", None), P()),
        out_specs=(P(None, "gx", "gy", None), P("gx", "gy", None)),
        check_vma=False,
    )
```

```python
import functools
import jax
import jax.numpy as jnp
from jax import lax
from jax.experimental import pallas as pl
from jax.experimental.pallas import tpu as pltpu
from jax.sharding import PartitionSpec as P

OUTER = 2
INNER = 3
step_time = 4.0
D = INNER
TINY = 1e-30
VMEM_BYTES = 67043328
DIAGONALS = ((1, -1), (-1, 1), (1, 1), (-1, -1))
MESH = pl.DeviceIdType.MESH
F32 = jnp.float32


def kernel(dims, *refs):
    ngx, ngy, nx, ny, nz, nmat = dims
    (mat, d_hbm, p_hbm, bf_hbm, fs_hbm, ids_hbm, d_out, p_out,
     p_old, bforce, fsource, ids, lsem,
     XI, XIY, XIS, XIR, LAM, SHR, PRM, BIO, STO, STAB, LAMY,
     SX, SY, SZ, SSUM, FX, FY, FZ, DIAG, PINV, HB, KF,
     P0, P0Y, P0S, P0R, U, UY, UCS, UCR, VY, VCS, VCR, RX, RY, RCS, RCR, MX, MYS, MYH, MCS, MCH,
     WP, WM, AP, AD, DC, DK, LY, LW, RB,
     isend, irecv, zsend, zrecv, vsend, vrecv, wsend, wrecv, psend, precv, msend, mrecv, rsend, rrecv) = refs
    gx, gy = lax.axis_index("gx"), lax.axis_index("gy")
    local = [pltpu.make_async_copy(src, dst, lsem.at[n]) for n, (src, dst) in enumerate((
        (ids_hbm, ids), (p_hbm, P0.at[pl.ds(D, nx), pl.ds(0, ny)]), (d_hbm, MX.at[0, :, pl.ds(1, nx)]),
        (p_hbm, p_old), (fs_hbm, fsource), (bf_hbm, bforce)))]
    for copy in local:
        copy.start()
    barrier = pltpu.get_barrier_semaphore()
    me, ndev = gx * ngy + gy, ngx * ngy

    def peer(d):
        t = lax.rem(me + d, ndev)
        return lax.div(t, ngy), lax.rem(t, ngy)
    has = {(-1, 0): gx > 0, (1, 0): gx < ngx - 1, (0, -1): gy > 0, (0, 1): gy < ngy - 1}
    for c in DIAGONALS:
        has[c] = jnp.logical_and(has[(c[0], 0)], has[(0, c[1])])

    rows = lax.broadcasted_iota(jnp.int32, (ny, nz), 0)
    lanes = lax.broadcasted_iota(jnp.int32, (ny, nz), 1)
    lanes8 = lax.broadcasted_iota(jnp.int32, (nx, nz), 1)
    rows8 = lax.broadcasted_iota(jnp.int32, (nx, nz), 0)
    lane1 = lax.broadcasted_iota(jnp.int32, (1, 128), 1)
    first_row, last_row = rows == 0, rows == ny - 1
    first_lane, last_lane = lanes == 0, lanes == nz - 1
    zero = jnp.zeros((ny, nz), F32)
    near = lax.broadcasted_iota(jnp.int32, (8, nz), 0) < 4
    wide = ny + 8
    first_wide = lax.broadcasted_iota(jnp.int32, (wide, nz), 1) == 0
    last_wide = lax.broadcasted_iota(jnp.int32, (wide, nz), 1) == nz - 1
    zero8 = jnp.zeros((nx, nz), F32)

    def upz(v):
        return pltpu.roll(v, nz - 1, 1)

    def dnz(v):
        return pltpu.roll(v, 1, 1)

    def upy(v, halo):
        return jnp.where(last_row, halo, pltpu.roll(v, ny - 1, 0))

    def dny(v, halo):
        return jnp.where(first_row, halo, pltpu.roll(v, 1, 0))

    def upw(v):
        return pltpu.roll(v, wide - 1, 0)

    def dnw(v):
        return pltpu.roll(v, 1, 0)

    def fold(v):
        out = None
        for i in range(0, ny, 8):
            for j in range(0, nz, 128):
                part = v[i:i + 8, j:j + 128]
                out = part if out is None else out + part
        return out

    def loop(body, init, low=0, high=nx, half=None):
        order = [low, high - 1] + list(range(low + 1, high - 1))
        for n, i in enumerate(order):
            init = body(i, init)
            if n == 1 and half is not None:
                half()
        return init

    def copies_of(pairs, send, recv):
        made = []
        for n, (src, dst, off) in enumerate(pairs):
            copy = pltpu.make_async_remote_copy(
                src_ref=src, dst_ref=dst, send_sem=send.at[n], recv_sem=recv.at[n],
                device_id=(gx + off[0], gy + off[1]), device_id_type=MESH)
            made.append((copy, off))
        return made

    def start(made, along=None):
        for copy, off in made:
            if along is not None and (off[0] != 0) != along:
                continue
            @pl.when(has[off])
            def _(copy=copy):
                copy.start()

    def wait_recv(made):
        for copy, off in made:
            @pl.when(has[(-off[0], -off[1])])
            def _(copy=copy):
                copy.wait_recv()

    def wait_send(made):
        for copy, off in made:
            @pl.when(has[off])
            def _(copy=copy):
                copy.wait_send()

    def wide_field(F, Y, CS, CR, depth, send, recv):
        pairs = [(F.at[pl.ds(D, depth), pl.ds(0, ny)], F.at[pl.ds(D + nx, depth), pl.ds(0, ny)], (-1, 0)),
                 (F.at[pl.ds(D + nx - depth, depth), pl.ds(0, ny)], F.at[pl.ds(D - depth, depth), pl.ds(0, ny)], (1, 0)),
                 (F.at[pl.ds(D, nx), pl.ds(0, 8)], Y.at[1], (0, -1)),
                 (F.at[pl.ds(D, nx), pl.ds(ny - 8, 8)], Y.at[0], (0, 1))]
        if CS is not None:
            pairs += [(CS.at[c], CR.at[c], off) for c, off in enumerate(DIAGONALS)]
        return copies_of(pairs, send, recv)

    def split_field(F, Y, CS, CR, depth, send, recv):
        far = depth - 1
        pairs = [(F.at[pl.ds(D, 1), pl.ds(0, ny)], F.at[pl.ds(D + nx, 1), pl.ds(0, ny)], (-1, 0)),
                 (F.at[pl.ds(D + nx - 1, 1), pl.ds(0, ny)], F.at[pl.ds(D - 1, 1), pl.ds(0, ny)], (1, 0)),
                 (F.at[pl.ds(D, nx), pl.ds(0, 8)], Y.at[1], (0, -1)),
                 (F.at[pl.ds(D, nx), pl.ds(ny - 8, 8)], Y.at[0], (0, 1)),
                 (F.at[pl.ds(D + 1, far), pl.ds(0, ny)], F.at[pl.ds(D + nx + 1, far), pl.ds(0, ny)], (-1, 0)),
                 (F.at[pl.ds(D + nx - depth, far), pl.ds(0, ny)], F.at[pl.ds(D - depth, far), pl.ds(0, ny)], (1, 0))]
        pairs += [(CS.at[c], CR.at[c], off) for c, off in enumerate(DIAGONALS)]
        made = copies_of(pairs, send, recv)
        return made[:4], made[4:]

    def stage_corners(F, CS):
        n, m = CS.shape[1:3]
        for c, (sx, sy) in enumerate(DIAGONALS):
            for t in range(n):
                CS[c, t] = F[D + (t if sx < 0 else nx - n + t), (0 if sy < 0 else ny - m):(m if sy < 0 else ny), :]

    def clear_missing(F, Y, CR, depth):
        none = jnp.zeros((wide, nz), F.dtype)
        for side, low in ((-1, D - depth), (1, D + nx)):
            @pl.when(jnp.logical_not(has[(side, 0)]))
            def _(low=low):
                for t in range(depth):
                    F[low + t] = none
        for side, s in ((-1, 0), (1, 1)):
            @pl.when(jnp.logical_not(has[(0, side)]))
            def _(s=s):
                for i in range(nx):
                    Y[s, i] = none[:8]
        if CR is not None:
            for c, off in enumerate(DIAGONALS):
                @pl.when(jnp.logical_not(has[(-off[0], -off[1])]))
                def _(c=c):
                    CR[c] = jnp.zeros(CR.shape[1:], F.dtype)

    def late_field(o):
        last = U.at[INNER * o + INNER - 1]
        pairs = [(last.at[pl.ds(D + nx - 2, 1), pl.ds(0, ny)], last.at[pl.ds(D - 2, 1), pl.ds(0, ny)], (1, 0)),
                 (last.at[pl.ds(D, nx), pl.ds(ny - 8, 8)], VY.at[o], (0, 1))]
        pairs += [(VCS.at[o, c], VCR.at[o, c], off) for c, off in enumerate(DIAGONALS[:3])]
        return copies_of(pairs, vsend, vrecv)

    def stage_late(o):
        for c, (sx, sy) in enumerate(DIAGONALS[:3]):
            for k in range(1, INNER):
                for t in range(2):
                    VCS[o, c, k - 1, t] = U[INNER * o + k, D + (t if sx < 0 else nx - 2 + t),
                                            (0 if sy < 0 else ny - 2):(2 if sy < 0 else ny), :]

    def merge_late(o):
        f = INNER * o + INNER - 1
        for i in range(nx):
            U[f, D + i, ny:, :] = jnp.where(near, U[f, D + i, ny:, :], VY[o, i])
        for c, (sx, sy) in enumerate(DIAGONALS[:3]):
            for k in range(1, INNER):
                for t in range(2):
                    low = ny if sy < 0 else wide - 2
                    U[INNER * o + k, (D + nx + t) if sx < 0 else (D - 2 + t), low:low + 2, :] = VCR[o, c, k - 1, t]

    def load_field(o):
        F = RX.at[o]
        pairs = [(F.at[:, pl.ds(1, 1), pl.ds(0, ny)], F.at[:, pl.ds(nx + 1, 1), pl.ds(0, ny)], (-1, 0)),
                 (F.at[:, pl.ds(nx, 1), pl.ds(0, ny)], F.at[:, pl.ds(0, 1), pl.ds(0, ny)], (1, 0)),
                 (F.at[:, pl.ds(1, nx), pl.ds(0, 8)], RY.at[o, 1], (0, -1)),
                 (F.at[:, pl.ds(1, nx), pl.ds(ny - 8, 8)], RY.at[o, 0], (0, 1)),
                 (RCS.at[o, 0], RCR.at[o, 0], DIAGONALS[0]), (RCS.at[o, 1], RCR.at[o, 1], DIAGONALS[1])]
        return copies_of(pairs, wsend, wrecv)

    def stage_load(o):
        for a in range(3):
            RCS[o, 0, a] = RX[o, a, nx, 0:1, :]
            RCS[o, 1, a] = RX[o, a, 1, ny - 1:ny, :]

    def merge_load(o):
        for a in range(3):
            for i in range(nx):
                RX[o, a, i + 1, ny:, :] = jnp.where(near, RY[o, 1, a, i], RY[o, 0, a, i])
            RX[o, a, 0, ny:ny + 1, :] = RCR[o, 0, a]
            RX[o, a, nx + 1, wide - 1:wide, :] = RCR[o, 1, a]

    def clear_late(o):
        none = jnp.zeros((wide, nz), F32)

        @pl.when(jnp.logical_not(has[(-1, 0)]))
        def _():
            U[INNER * o + INNER - 1, D - 2] = none
            for a in range(3):
                RX[o, a, 0] = none

        @pl.when(jnp.logical_not(has[(1, 0)]))
        def _():
            for a in range(3):
                RX[o, a, nx + 1] = none

        @pl.when(jnp.logical_not(has[(0, -1)]))
        def _():
            for i in range(nx):
                VY[o, i] = none[:8]
                for a in range(3):
                    RY[o, 0, a, i] = none[:8]

        @pl.when(jnp.logical_not(has[(0, 1)]))
        def _():
            for i in range(nx):
                for a in range(3):
                    RY[o, 1, a, i] = none[:8]
        for c, off in enumerate(DIAGONALS[:3]):
            @pl.when(jnp.logical_not(has[(-off[0], -off[1])]))
            def _(c=c):
                VCR[o, c] = jnp.zeros(VCR.shape[2:], F32)
                if c < 2:
                    RCR[o, c] = jnp.zeros(RCR.shape[2:], F32)

    def merge(F, Y, CR):
        for i in range(nx):
            F[D + i, ny:, :] = jnp.where(near, Y[1, i], Y[0, i])
        if CR is not None:
            merge_corners(F, CR)

    def merge_corners(F, CR):
        n, m = CR.shape[1:3]
        for c, (sx, sy) in enumerate(DIAGONALS):
            for t in range(n):
                low = ny if sy < 0 else wide - m
                F[(D + nx + t) if sx < 0 else (D - n + t), low:low + m, :] = CR[c, t]

    def vector_field(f):
        return copies_of(
            [(MX.at[f, :, 1], MX.at[f, :, nx + 1], (-1, 0)), (MX.at[f, :, nx], MX.at[f, :, 0], (1, 0)),
             (MYS.at[f, 0], MYH.at[f, 1], (0, -1)), (MYS.at[f, 1], MYH.at[f, 0], (0, 1)),
             (MCS.at[f, 0], MCH.at[f, 0], (1, -1)), (MCS.at[f, 1], MCH.at[f, 1], (-1, 1))],
            msend.at[f % 2], mrecv.at[f % 2])

    def put_vector(f, i, vs):
        for a in range(3):
            MX[f, a, i + 1] = vs[a]
            MYS[f, 0, a, slice(i, i + 1), :] = vs[a][0:1]
            MYS[f, 1, a, slice(i, i + 1), :] = vs[a][ny - 1:ny]

    def put_corners(f):
        MCS[f, 0] = MX[f, 1, nx, 0:1, :]
        MCS[f, 1] = MX[f, 0, 1, ny - 1:ny, :]

    nf = 1 + OUTER * INNER
    for d in range(1, ndev):
        pl.semaphore_signal(barrier, inc=1, device_id=peer(d), device_id_type=MESH)


    def stage_values(i, c):
        for side, y in ((0, 0), (1, ny - 1)):
            for a in range(3):
                MYS[0, side, a, i:i + 1, :] = MX[0, a, i + 1, y:y + 1, :]
        return c
    local[0].wait()
    for i in range(nx):
        XI[D + i, 0:ny, :] = ids[i] + 1
    stage_corners(XI, XIS)
    local[1].wait()
    stage_corners(P0, P0S)
    pl.semaphore_wait(barrier, ndev - 1)
    p_near, p_far = split_field(P0, P0Y, P0S, P0R, 2, zsend, zrecv)
    codes_near, codes_far = split_field(XI, XIY, XIS, XIR, D, isend, irecv)
    d_copy = vector_field(0)
    start(p_near)
    start(codes_near)
    start(codes_far)
    local[2].wait()
    loop(stage_values, 0)
    put_corners(0)
    start(d_copy)
    start(p_far)
    clear_missing(XI, XIY, XIR, D)
    clear_missing(P0, P0Y, P0R, 2)
    for outer in range(OUTER):
        clear_missing(U.at[INNER * outer], UY.at[outer], UCR.at[outer], D)
        clear_late(outer)

    def clear_vector(f, c):
        for side, j, s in ((-1, 0, 0), (1, nx + 1, 1)):
            @pl.when(jnp.logical_not(has[(side, 0)]))
            def _(j=j):
                for a in range(3):
                    MX[f, a, j] = zero

            @pl.when(jnp.logical_not(has[(0, side)]))
            def _(s=s):
                for a in range(3):
                    MYH[f, s, a] = zero8
        for c2, off in enumerate(DIAGONALS[:2]):
            @pl.when(jnp.logical_not(has[(-off[0], -off[1])]))
            def _(c2=c2):
                MCH[f, c2] = jnp.zeros((1, nz), F32)
        return c
    lax.fori_loop(0, nf, clear_vector, 0)

    def lookup(code, table_rows):
        out = [jnp.zeros(code.shape, F32) for _ in table_rows]
        for m in range(nmat):
            hit = code == m + 1
            out = [jnp.where(hit, mat[t, m], v) for t, v in zip(table_rows, out)]
        return out

    def look(j, part):
        code = XI[j, part, :]
        lam, shr, prm, sto, bio = lookup(code, (0, 1, 2, 3, 4))
        bio = 0.25 * bio
        LAM[j, part, :] = lam
        SHR[j, part, :] = shr
        PRM[j, part, :] = prm
        BIO[j, part, :] = bio
        STO[j, part, :] = sto
        STAB[j, part, :] = bio * bio / jnp.maximum(lam + 2.0 / 3.0 * shr, TINY)
    for i in range(nx):
        look(D + i, slice(0, ny))
    wait_recv(codes_near)
    merge(XI, XIY, None)
    for i in range(nx):
        look(D + i, slice(ny, wide))
    for j in (D - 1, D + nx):
        look(j, slice(0, ny))

    def harmonic(one, two):
        return (2.0 * step_time) * one * two / jnp.maximum(one + two, TINY)

    def flow(j):
        prm = PRM[j]
        fzu = jnp.where(last_wide, 0.0, harmonic(prm, upz(prm)))
        fyu = harmonic(prm, upw(prm))
        FY[j], FZ[j] = fyu, fzu
        diag = STO[j] + STAB[j] + (FX[j] + FX[j + 1] + fyu + dnw(fyu) + fzu + dnz(fzu))
        DIAG[j] = diag
        PINV[j] = jnp.where(XI[j] > 0, 1.0 / jnp.maximum(diag, TINY), 0.0)

    def face(j):
        FX[j] = harmonic(PRM[j - 1], PRM[j])
    for j in range(D, D + nx + 1):
        face(j)
    for j in range(D, D + nx):
        flow(j)

    def rim():
        wait_recv(codes_far)
        merge_corners(XI, XIR)
        for j in (D - 1, D + nx):
            look(j, slice(ny, wide))
        for j in range(nx + 2 * D):
            if j < D - 1 or j > D + nx:
                look(j, slice(0, wide))
        for j in list(range(1, D + 1)) + list(range(D + nx, nx + 2 * D)):
            face(j)
        for j in list(range(1, D + 1)) + list(range(D + nx - 1, nx + 2 * D - 1)):
            flow(j)

    def stiff_face(t):
        SX[t] = 0.5 * (SHR[D + t - 2] + SHR[D + t - 1])

    def coefs(i):
        shr, lam = SHR[D + i], LAM[D + i]
        half = 0.5 * shr
        syu = 0.5 * (shr + upw(shr))
        syd = dnw(syu)
        szu = half + jnp.where(last_wide, 0.0, 0.5 * upz(shr))
        szd = half + jnp.where(first_wide, 0.0, 0.5 * dnz(shr))
        total = SX[i + 1] + SX[i + 2] + syu + syd + szu + szd
        if 0 <= i < nx:
            LAMY[slice(i, i + 1), :] = LAM[D + i, wide - 1:wide, :]
            SY[1, i], SY[0, i] = syu[:ny], syd[:ny]
            SZ[1, i] = jnp.where(last_lane, 0.0, szu[:ny])
            SZ[0, i] = jnp.where(first_lane, 0.0, szd[:ny])
            SSUM[i] = total[:ny]
        inside = XI[D + i] > 0
        hs = []
        for a, below in enumerate((LAM[D + i - 1], dnw(lam), jnp.where(first_wide, 0.0, dnz(lam)))):
            h = jnp.where(inside, 1.0 / jnp.maximum(total + below, TINY), 0.0)
            HB[a, i + 1] = h
            hs.append(h)
        KF[i + 1] = lam / (1.0 + lam * (hs[0] + hs[1] + hs[2]))

    def apply_pressure(F, j, rows):
        v = F[j]
        out = (DIAG[j] * v - FX[j + 1] * F[j + 1] - FX[j] * F[j - 1]
               - FY[j] * upw(v) - dnw(FY[j] * v)
               - FZ[j] * upz(v) - dnz(FZ[j] * v))
        return v[:rows], out[:rows]

    def apply_mech(f, emit, init, half=None):
        m = [MYH[f, 0, a] for a in range(3)]
        ahead = jnp.where(rows8 == nx - 1, MCH[f, 1], pltpu.roll(m[0], nx - 1, 0))
        z8 = jnp.where(lanes8 == nz - 1, 0.0, pltpu.roll(m[2], nz - 1, 1))
        LY[...] = LAMY[...] * (ahead - m[0] + MYS[f, 0, 1] - m[1] + z8 - m[2])
        m = [MX[f, a, 0] for a in range(3)]
        below_first = LAM[D - 1, 0:ny, :] * (MX[f, 0, 1] - m[0] + upy(m[1], MCH[f, 0]) - m[1]
                          + jnp.where(last_lane, 0.0, upz(m[2])) - m[2])

        def weigh(i):
            w = [MX[f, a, i + 1] for a in range(3)]
            return LAM[D + i, 0:ny, :] * (MX[f, 0, i + 2] - w[0] + upy(w[1], MYH[f, 1, 1, i:i + 1, :]) - w[1]
                                 + jnp.where(last_lane, 0.0, upz(w[2])) - w[2])

        def body(i, c):
            row = slice(i, i + 1)
            ws, outs, div = [], [], None
            for a in range(3):
                w, wx = MX[f, a, i + 1], MX[f, a, i + 2]
                wy, wz = upy(w, MYH[f, 1, a, row, :]), upz(w)
                out = (SSUM[i] * w - SX[i + 2, 0:ny, :] * wx - SX[i + 1, 0:ny, :] * MX[f, a, i]
                       - SY[1, i] * wy - SY[0, i] * dny(w, MYH[f, 0, a, row, :])
                       - SZ[1, i] * wz - SZ[0, i] * dnz(w))
                part = (wx, wy, jnp.where(last_lane, 0.0, wz))[a] - w
                div = part if div is None else div + part
                ws.append(w)
                outs.append(out)
            weighted = LAM[D + i, 0:ny, :] * div
            LW[i] = weighted
            before = below_first if i == 0 else weigh(i - 1) if i == nx - 1 else LW[i - 1]
            below = (before, dny(weighted, LY[row, :]), jnp.where(first_lane, 0.0, dnz(weighted)))
            outs = [outs[a] + (below[a] - weighted) for a in range(3)]
            return emit(i, ws, outs, c)
        return loop(body, init, half=half)

    def block_solve(i, r, rows):
        part = slice(0, rows)
        scaled = [r[a] * HB[a, i + 1, part, :] for a in range(3)]
        tail = KF[i + 1, part, :] * (scaled[0] + scaled[1] + scaled[2])
        return [scaled[a] - HB[a, i + 1, part, :] * tail for a in range(3)]

    def dot3(a, b):
        return fold(a[0] * b[0] + a[1] * b[1] + a[2] * b[2])

    summed = []

    def all_sum(q, sums, meanwhile=None):
        row = jnp.zeros((1, 128), F32)
        for k, s in enumerate(sums):
            row = jnp.where(lane1 == k, jnp.sum(s, keepdims=True), row)
        RB[q, me] = row
        for d in sorted(range(1, ndev), key=lambda d: -min(d, ndev - d)):
            copy = pltpu.make_async_remote_copy(
                src_ref=RB.at[q, me], dst_ref=RB.at[q, me], send_sem=rsend.at[q],
                recv_sem=rrecv.at[q], device_id=peer(d), device_id_type=MESH)
            copy.start()
        every = RB.at[q, pl.ds(0, ndev - 1)]
        whole = pltpu.make_async_remote_copy(
            src_ref=every, dst_ref=every, send_sem=rsend.at[q], recv_sem=rrecv.at[q],
            device_id=peer(1), device_id_type=MESH)
        if meanwhile is not None:
            meanwhile()
        whole.wait_recv()
        summed.append(whole)
        parts = [RB[q, d] for d in range(ndev)]
        while len(parts) > 1:
            parts = [sum(parts[d + 1:d + 2], parts[d]) for d in range(0, len(parts), 2)]
        row = parts[0]
        return [row[:, k:k + 1] for k in range(len(sums))]

    def combine(t):
        n0, m0, m1, m2, m3, m4 = t
        n1 = m0 - n0
        n2 = m1 - n1
        l1, l2 = m1 / m0, m2 / m0
        d1 = m2 - l1 * m1
        e = m3 - l1 * m2
        l3 = jnp.where(d1 > 0, e / d1, 0.0)
        d2 = m4 - l2 * m2 - l3 * e
        y1 = n1 - l1 * n0
        y2 = n2 - l2 * n0 - l3 * y1
        c2 = jnp.where(d2 > 0, y2 / d2, 0.0)
        c1 = jnp.where(d1 > 0, y1 / d1, 0.0) - l3 * c2
        c0 = n0 / m0 - l1 * c1 - l2 * c2
        return c0, c1, c2

    zacc = jnp.zeros((8, 128), F32)
    wait_recv(p_near)
    merge(P0, P0Y, None)
    for i in range(nx):
        AP[i] = apply_pressure(P0, D + i, ny)[1]

    local[3].wait()
    local[4].wait()

    msent = []

    def retire(queue):
        if len(queue) == 2:
            wait_send(queue.pop(0))
    for outer in range(OUTER):
        base = 1 + INNER * outer

        u0 = U.at[INNER * outer]

        def p_start(i, acc):
            if outer > 0:
                m_change(i)
            own = slice(0, ny)
            rhs = (STO[D + i, own, :] * p_old[i] + step_time * fsource[i]
                   + STAB[D + i, own, :] * P0[D + i, own, :])
            if outer > 0:
                rhs = rhs - BIO[D + i, own, :] * DC[i]
            r = rhs - AP[i]
            u = r * PINV[D + i, own, :]
            u0[D + i, own, :] = u
            return acc + fold(r * u)
        if outer > 0:
            wait_send(made_p)
        n0 = loop(p_start, zacc)
        stage_corners(u0, UCS.at[outer])
        made_p = wide_field(u0, UY.at[outer], UCS.at[outer], UCR.at[outer], D, psend, precv)
        start(made_p)
        if outer > 0:
            loop(m_after, 0)
        if outer == 0:
            rim()
            for t in range(nx + 3):
                stiff_face(t)
            for i in range(-1, nx + 1):
                coefs(i)
            wait_recv(d_copy)
            wait_send(d_copy)

            def keep_ad(i, ws, outs, c):
                for a in range(3):
                    AD[a, i] = outs[a]
                    RX[0, a, i + 1, 0:ny, :] = bforce[a, i] - outs[a]
                return c
            local[5].wait()
            apply_mech(0, keep_ad, 0)
        else:
            wait_send(made_r)
        stage_load(outer)
        made_r = load_field(outer)
        start(made_r)
        sums = [n0]
        wait_recv(made_p)
        merge(u0, UY.at[outer], UCR.at[outer])
        for k in range(INNER):
            sums = [jnp.sum(v, keepdims=True) for v in sums]
            F = U.at[INNER * outer + k]
            reach = 0 if k == INNER - 1 else D - 1 - k
            even, odd = zacc, zacc
            for j in range(D - reach, D + nx + reach):
                own = D <= j < D + nx
                v, w = apply_pressure(F, j, wide if k < INNER - 1 else ny)
                if own:
                    WP[k, j - D] = w[:ny]
                    even = even + fold(v[:ny] * w[:ny])
                if k < INNER - 1:
                    u = w * PINV[j] - v
                    U[INNER * outer + k + 1, j] = u
                    if own:
                        odd = odd + fold(u[:ny] * w[:ny])
            sums += [even] if k == INNER - 1 else [even, odd]
            if k == INNER - 2:
                if outer > 0:
                    wait_send(made_v)
                stage_late(outer)
                made_v = late_field(outer)
                start(made_v)

        def arrivals():
            if outer == 0:
                wait_recv(p_far)
                merge_corners(P0, P0R)
                wait_send(p_near)
                wait_send(p_far)
            wait_recv(made_r)
            merge_load(outer)
            wait_recv(made_v)
            merge_late(outer)
        cs = combine(all_sum(2 * outer, sums, arrivals))

        for j in range(D - 2, D + nx + 1):
            v = P0[j]
            for k in range(INNER):
                v = v + cs[k] * U[INNER * outer + k, j]
            P0[j] = v

        n0 = zacc
        for i in range(-1, nx + 1):
            load = BIO[D + i] * P0[D + i]
            below = (BIO[D + i - 1] * P0[D + i - 1], dnw(load), jnp.where(first_wide, 0.0, dnz(load)))
            r = [RX[outer, a, i + 1] + (below[a] - load) for a in range(3)]
            u = block_solve(i, r, wide)
            if 0 <= i < nx:
                put_vector(base, i, [v[:ny] for v in u])
                for a in range(3):
                    MYH[base, 1, a, i:i + 1, :] = u[a][ny:ny + 1]
                    MYH[base, 0, a, i:i + 1, :] = u[a][wide - 1:wide]
                n0 = n0 + dot3([v[:ny] for v in r], [v[:ny] for v in u])
            else:
                for a in range(3):
                    MX[base, a, i + 1] = u[a][:ny]
                if i < 0:
                    MCH[base, 0] = u[1][ny:ny + 1]
                else:
                    MCH[base, 1] = u[0][wide - 1:wide]

        def send_planes(f, made):
            put_corners(f)
            start(made, True)

        def p_after(i, c):
            if outer == OUTER - 1:
                p_out[i] = P0[D + i, 0:ny, :]
            else:
                v = AP[i]
                for k in range(INNER):
                    v = v + cs[k] * WP[k, i]
                AP[i] = v
            return c
        loop(p_after, 0)
        sums = [n0]
        for k in range(INNER):
            sums = [jnp.sum(v, keepdims=True) for v in sums]
            if k > 0:
                wait_recv(made)

            def m_step(i, v, w, c):
                if outer < OUTER - 1:
                    for a in range(3):
                        WM[k, a, i] = w[a]
                even = c[0] + dot3(v, w)
                if k == INNER - 1:
                    return (even,)
                z = block_solve(i, w, ny)
                u = [z[a] - v[a] for a in range(3)]
                put_vector(base + k + 1, i, u)
                return even, c[1] + dot3(u, w)
            half = None
            if k < INNER - 1:
                retire(msent)
                made = vector_field(base + k + 1)
                half = functools.partial(send_planes, base + k + 1, made)
            sums += apply_mech(base + k, m_step, (zacc,) * (1 if k == INNER - 1 else 2), half)
            if k < INNER - 1:
                start(made, False)
                msent.append(made)
        def changes():
            for k in range(INNER):
                for i in range(nx):
                    w = [MX[base + k, a, i + 1] for a in range(3)]
                    DK[k, i] = (MX[base + k, 0, i + 2] - w[0] + upy(w[1], MYH[base + k, 1, 1, i:i + 1, :]) - w[1]
                                + jnp.where(last_lane, 0.0, upz(w[2])) - w[2])
        cs = combine(all_sum(2 * outer + 1, sums, changes if outer < OUTER - 1 else None))

        def mixed(get, cs=cs, base=base):
            v = cs[0] * get(base)
            for k in range(1, INNER):
                v = v + cs[k] * get(base + k)
            return v

        def m_change(i, outer=outer, cs=cs):
            v = DC[i] if outer > 0 else None
            for k in range(INNER):
                part = cs[k] * DK[k, i]
                v = part if v is None else v + part
            DC[i] = v

        def m_after(i, c, cs=cs, mixed=mixed, outer=outer):
            for a in range(3):
                before = MX[0, a, i + 1] if outer == 0 else d_out[a, i]
                d_out[a, i] = before + mixed(lambda f, a=a: MX[f, a, i + 1])
            if outer < OUTER - 1:
                for a in range(3):
                    v = AD[a, i]
                    for k in range(INNER):
                        v = v + cs[k] * WM[k, a, i]
                    RX[outer + 1, a, i + 1, 0:ny, :] = bforce[a, i] - v
            return c
        if outer == OUTER - 1:
            loop(m_after, 0)

    for made in msent + [codes_near, codes_far, made_p, made_r, made_v]:
        wait_send(made)
    for copy in summed:
        copy.wait_send()


def on_device(dims, d_old, p_old, bforce, fsource, ids, materials):
    ngx, ngy, nx, ny, nz, nmat = dims
    nf = 1 + OUTER * INNER
    nq = 2 * OUTER

    def vm(*shape, dtype=F32):
        return pltpu.VMEM(shape, dtype)
    plane, strip = (ny, nz), (nx, nz)
    cell = (nx, ny, nz)
    ext = (nx + 2, ny, nz)
    broad = (ny + 8, nz)
    big = (nx + 2 * D, ny + 8, nz)
    edge = (2, nx, 8, nz)
    corner = (4, D - 1, 2 if D == 3 else 4, nz)
    dma = pltpu.SemaphoreType.DMA
    scratch = [
        vm(*cell), vm(3, *cell), vm(*cell), vm(*cell, dtype=jnp.int32), dma((6,)),
        vm(*big, dtype=jnp.int32), vm(*edge, dtype=jnp.int32),
        vm(*corner, dtype=jnp.int32), vm(*corner, dtype=jnp.int32),
        vm(*big), vm(*big), vm(*big), vm(*big), vm(*big), vm(*big), vm(*strip),
        vm(nx + 3, *broad), vm(2, *cell), vm(2, *cell), vm(*cell),
        vm(*big), vm(*big), vm(*big), vm(*big), vm(*big),
        vm(3, nx + 2, *broad), vm(nx + 2, *broad),
        vm(*big), vm(*edge), vm(*corner), vm(*corner), vm(OUTER * INNER, *big), vm(OUTER, *edge), vm(OUTER, *corner), vm(OUTER, *corner),
        vm(OUTER, nx, 8, nz), vm(OUTER, 3, INNER - 1, 2, 2, nz), vm(OUTER, 3, INNER - 1, 2, 2, nz),
        vm(OUTER, 3, nx + 2, *broad), vm(OUTER, 2, 3, nx, 8, nz), vm(OUTER, 2, 3, 1, nz), vm(OUTER, 2, 3, 1, nz),
        vm(nf, 3, *ext), vm(nf, 2, 3, *strip), vm(nf, 2, 3, *strip), vm(nf, 2, 1, nz), vm(nf, 2, 1, nz),
        vm(INNER, *cell), vm(INNER, 3, *cell), vm(*cell), vm(3, *cell), vm(*cell), vm(INNER, *cell),
        vm(*strip), vm(*cell), vm(nq, ngx * ngy, 1, 128),
        dma((10,)), dma((10,)), dma((10,)), dma((10,)), dma((5,)), dma((5,)), dma((6,)), dma((6,)), dma((8,)), dma((8,)), dma((2, 6)), dma((2, 6)),
        dma((nq,)), dma((nq,)),
    ]
    block = pl.BlockSpec(memory_space=pltpu.VMEM)
    return pl.pallas_call(
        functools.partial(kernel, dims),
        out_shape=(pltpu.VMEM(d_old.shape, F32), pltpu.VMEM(p_old.shape, F32)),
        in_specs=[pl.BlockSpec(memory_space=pltpu.SMEM)] + [pl.BlockSpec(memory_space=pl.ANY)] * 5,
        out_specs=(block, block),
        scratch_shapes=scratch,
        compiler_params=pltpu.CompilerParams(
            collective_id=0, has_side_effects=True,
            vmem_limit_bytes=VMEM_BYTES - 4 * (d_old.size + p_old.size) - 131072),
        name="poro",
    )(materials, d_old, p_old, bforce, fsource, ids)


def solution(mesh):
    ngx, ngy = mesh.shape["gx"], mesh.shape["gy"]

    def body(d_old, p_old, bforce, fsource, ids, materials):
        dims = (ngx, ngy, *p_old.shape, materials.shape[1])
        return on_device(dims, d_old, p_old, bforce, fsource, ids, materials)

    return jax.shard_map(
        body,
        mesh=mesh,
        in_specs=(P(None, "gx", "gy", None), P("gx", "gy", None), P(None, "gx", "gy", None),
                  P("gx", "gy", None), P("gx", "gy", None), P()),
        out_specs=(P(None, "gx", "gy", None), P("gx", "gy", None)),
        check_vma=False,
    )
```

```python
import functools
import jax
import jax.numpy as jnp
from jax import lax
from jax.experimental import pallas as pl
from jax.experimental.pallas import tpu as pltpu
from jax.sharding import PartitionSpec as P

OUTER = 2
INNER = 3
step_time = 4.0
D = INNER
TINY = 1e-30
VMEM_BYTES = 67043328
DIAGONALS = ((1, -1), (-1, 1), (1, 1), (-1, -1))
MESH = pl.DeviceIdType.MESH
F32 = jnp.float32


def kernel(dims, *refs):
    ngx, ngy, nx, ny, nz, nmat = dims
    (mat_hbm, d_hbm, p_hbm, bf_hbm, fs_hbm, ids_hbm, d_out, p_out,
     mat, p_old, bforce, fsource, ids, lsem,
     XI, XIY, XIS, XIR, LAM, SHR, PRM, BIO, STO, STAB, LAMY,
     SX, SY, SZ, SSUM, FX, FY, FZ, DIAG, PINV, HB, KF,
     P0, P0Y, P0S, P0R, U, UY, UCS, UCR, VY, VCS, VCR, RX, RY, RCS, RCR, MX, MYS, MYH, MCS, MCH,
     WP, WM, AP, AD, DC, DK, LY, LW, RB,
     isend, irecv, zsend, zrecv, vsend, vrecv, wsend, wrecv, psend, precv, msend, mrecv, rsend, rrecv) = refs
    gx, gy = lax.axis_index("gx"), lax.axis_index("gy")
    local = [pltpu.make_async_copy(src, dst, lsem.at[n]) for n, (src, dst) in enumerate((
        (ids_hbm, ids), (p_hbm, P0.at[pl.ds(D, nx), pl.ds(0, ny)]), (d_hbm, MX.at[0, :, pl.ds(1, nx)]),
        (p_hbm, p_old), (fs_hbm, fsource), (bf_hbm, bforce), (mat_hbm, mat)))]
    for copy in local:
        copy.start()
    barrier = pltpu.get_barrier_semaphore()
    me, ndev = gx * ngy + gy, ngx * ngy

    def peer(d):
        t = lax.rem(me + d, ndev)
        return lax.div(t, ngy), lax.rem(t, ngy)
    has = {(-1, 0): gx > 0, (1, 0): gx < ngx - 1, (0, -1): gy > 0, (0, 1): gy < ngy - 1}
    for c in DIAGONALS:
        has[c] = jnp.logical_and(has[(c[0], 0)], has[(0, c[1])])

    rows = lax.broadcasted_iota(jnp.int32, (ny, nz), 0)
    lanes = lax.broadcasted_iota(jnp.int32, (ny, nz), 1)
    lanes8 = lax.broadcasted_iota(jnp.int32, (nx, nz), 1)
    rows8 = lax.broadcasted_iota(jnp.int32, (nx, nz), 0)
    lane1 = lax.broadcasted_iota(jnp.int32, (1, 128), 1)
    first_row, last_row = rows == 0, rows == ny - 1
    first_lane, last_lane = lanes == 0, lanes == nz - 1
    zero = jnp.zeros((ny, nz), F32)
    near = lax.broadcasted_iota(jnp.int32, (8, nz), 0) < 4
    wide = ny + 8
    first_wide = lax.broadcasted_iota(jnp.int32, (wide, nz), 1) == 0
    last_wide = lax.broadcasted_iota(jnp.int32, (wide, nz), 1) == nz - 1
    zero8 = jnp.zeros((nx, nz), F32)

    def upz(v):
        return pltpu.roll(v, nz - 1, 1)

    def dnz(v):
        return pltpu.roll(v, 1, 1)

    def upy(v, halo):
        return jnp.where(last_row, halo, pltpu.roll(v, ny - 1, 0))

    def dny(v, halo):
        return jnp.where(first_row, halo, pltpu.roll(v, 1, 0))

    def upw(v):
        return pltpu.roll(v, wide - 1, 0)

    def dnw(v):
        return pltpu.roll(v, 1, 0)

    def fold(v):
        out = None
        for i in range(0, ny, 8):
            for j in range(0, nz, 128):
                part = v[i:i + 8, j:j + 128]
                out = part if out is None else out + part
        return out

    def loop(body, init, low=0, high=nx, half=None):
        order = [low, high - 1] + list(range(low + 1, high - 1))
        for n, i in enumerate(order):
            init = body(i, init)
            if n == 1 and half is not None:
                half()
        return init

    def copies_of(pairs, send, recv):
        made = []
        for n, (src, dst, off) in enumerate(pairs):
            copy = pltpu.make_async_remote_copy(
                src_ref=src, dst_ref=dst, send_sem=send.at[n], recv_sem=recv.at[n],
                device_id=(gx + off[0], gy + off[1]), device_id_type=MESH)
            made.append((copy, off))
        return made

    def start(made, along=None):
        for copy, off in made:
            if along is not None and (off[0] != 0) != along:
                continue
            @pl.when(has[off])
            def _(copy=copy):
                copy.start()

    def wait_recv(made):
        for copy, off in made:
            @pl.when(has[(-off[0], -off[1])])
            def _(copy=copy):
                copy.wait_recv()

    def wait_send(made):
        for copy, off in made:
            @pl.when(has[off])
            def _(copy=copy):
                copy.wait_send()

    def wide_field(F, Y, CS, CR, depth, send, recv):
        pairs = [(F.at[pl.ds(D, depth), pl.ds(0, ny)], F.at[pl.ds(D + nx, depth), pl.ds(0, ny)], (-1, 0)),
                 (F.at[pl.ds(D + nx - depth, depth), pl.ds(0, ny)], F.at[pl.ds(D - depth, depth), pl.ds(0, ny)], (1, 0)),
                 (F.at[pl.ds(D, nx), pl.ds(0, 8)], Y.at[1], (0, -1)),
                 (F.at[pl.ds(D, nx), pl.ds(ny - 8, 8)], Y.at[0], (0, 1))]
        if CS is not None:
            pairs += [(CS.at[c], CR.at[c], off) for c, off in enumerate(DIAGONALS)]
        return copies_of(pairs, send, recv)

    def split_field(F, Y, CS, CR, depth, send, recv):
        far = depth - 1
        pairs = [(F.at[pl.ds(D, 1), pl.ds(0, ny)], F.at[pl.ds(D + nx, 1), pl.ds(0, ny)], (-1, 0)),
                 (F.at[pl.ds(D + nx - 1, 1), pl.ds(0, ny)], F.at[pl.ds(D - 1, 1), pl.ds(0, ny)], (1, 0)),
                 (F.at[pl.ds(D, nx), pl.ds(0, 8)], Y.at[1], (0, -1)),
                 (F.at[pl.ds(D, nx), pl.ds(ny - 8, 8)], Y.at[0], (0, 1)),
                 (F.at[pl.ds(D + 1, far), pl.ds(0, ny)], F.at[pl.ds(D + nx + 1, far), pl.ds(0, ny)], (-1, 0)),
                 (F.at[pl.ds(D + nx - depth, far), pl.ds(0, ny)], F.at[pl.ds(D - depth, far), pl.ds(0, ny)], (1, 0))]
        pairs += [(CS.at[c], CR.at[c], off) for c, off in enumerate(DIAGONALS)]
        made = copies_of(pairs, send, recv)
        return made[:4], made[4:]

    def stage_corners(F, CS):
        n, m = CS.shape[1:3]
        for c, (sx, sy) in enumerate(DIAGONALS):
            for t in range(n):
                CS[c, t] = F[D + (t if sx < 0 else nx - n + t), (0 if sy < 0 else ny - m):(m if sy < 0 else ny), :]

    def clear_missing(F, Y, CR, depth):
        none = jnp.zeros((wide, nz), F.dtype)
        for side, low in ((-1, D - depth), (1, D + nx)):
            @pl.when(jnp.logical_not(has[(side, 0)]))
            def _(low=low):
                for t in range(depth):
                    F[low + t] = none
        for side, s in ((-1, 0), (1, 1)):
            @pl.when(jnp.logical_not(has[(0, side)]))
            def _(s=s):
                for i in range(nx):
                    Y[s, i] = none[:8]
        if CR is not None:
            for c, off in enumerate(DIAGONALS):
                @pl.when(jnp.logical_not(has[(-off[0], -off[1])]))
                def _(c=c):
                    CR[c] = jnp.zeros(CR.shape[1:], F.dtype)

    def late_field(o):
        last = U.at[INNER * o + INNER - 1]
        pairs = [(last.at[pl.ds(D + nx - 2, 1), pl.ds(0, ny)], last.at[pl.ds(D - 2, 1), pl.ds(0, ny)], (1, 0)),
                 (last.at[pl.ds(D, nx), pl.ds(ny - 8, 8)], VY.at[o], (0, 1))]
        pairs += [(VCS.at[o, c], VCR.at[o, c], off) for c, off in enumerate(DIAGONALS[:3])]
        return copies_of(pairs, vsend, vrecv)

    def stage_late(o):
        for c, (sx, sy) in enumerate(DIAGONALS[:3]):
            for k in range(1, INNER):
                for t in range(2):
                    VCS[o, c, k - 1, t] = U[INNER * o + k, D + (t if sx < 0 else nx - 2 + t),
                                            (0 if sy < 0 else ny - 2):(2 if sy < 0 else ny), :]

    def merge_late(o):
        f = INNER * o + INNER - 1
        for i in range(nx):
            U[f, D + i, ny:, :] = jnp.where(near, U[f, D + i, ny:, :], VY[o, i])
        for c, (sx, sy) in enumerate(DIAGONALS[:3]):
            for k in range(1, INNER):
                for t in range(2):
                    low = ny if sy < 0 else wide - 2
                    U[INNER * o + k, (D + nx + t) if sx < 0 else (D - 2 + t), low:low + 2, :] = VCR[o, c, k - 1, t]

    def load_field(o):
        F = RX.at[o]
        pairs = [(F.at[:, pl.ds(1, 1), pl.ds(0, ny)], F.at[:, pl.ds(nx + 1, 1), pl.ds(0, ny)], (-1, 0)),
                 (F.at[:, pl.ds(nx, 1), pl.ds(0, ny)], F.at[:, pl.ds(0, 1), pl.ds(0, ny)], (1, 0)),
                 (F.at[:, pl.ds(1, nx), pl.ds(0, 8)], RY.at[o, 1], (0, -1)),
                 (F.at[:, pl.ds(1, nx), pl.ds(ny - 8, 8)], RY.at[o, 0], (0, 1)),
                 (RCS.at[o, 0], RCR.at[o, 0], DIAGONALS[0]), (RCS.at[o, 1], RCR.at[o, 1], DIAGONALS[1])]
        return copies_of(pairs, wsend, wrecv)

    def stage_load(o):
        for a in range(3):
            RCS[o, 0, a] = RX[o, a, nx, 0:1, :]
            RCS[o, 1, a] = RX[o, a, 1, ny - 1:ny, :]

    def merge_load(o):
        for a in range(3):
            for i in range(nx):
                RX[o, a, i + 1, ny:, :] = jnp.where(near, RY[o, 1, a, i], RY[o, 0, a, i])
            RX[o, a, 0, ny:ny + 1, :] = RCR[o, 0, a]
            RX[o, a, nx + 1, wide - 1:wide, :] = RCR[o, 1, a]

    def clear_late(o):
        none = jnp.zeros((wide, nz), F32)

        @pl.when(jnp.logical_not(has[(-1, 0)]))
        def _():
            U[INNER * o + INNER - 1, D - 2] = none
            for a in range(3):
                RX[o, a, 0] = none

        @pl.when(jnp.logical_not(has[(1, 0)]))
        def _():
            for a in range(3):
                RX[o, a, nx + 1] = none

        @pl.when(jnp.logical_not(has[(0, -1)]))
        def _():
            for i in range(nx):
                VY[o, i] = none[:8]
                for a in range(3):
                    RY[o, 0, a, i] = none[:8]

        @pl.when(jnp.logical_not(has[(0, 1)]))
        def _():
            for i in range(nx):
                for a in range(3):
                    RY[o, 1, a, i] = none[:8]
        for c, off in enumerate(DIAGONALS[:3]):
            @pl.when(jnp.logical_not(has[(-off[0], -off[1])]))
            def _(c=c):
                VCR[o, c] = jnp.zeros(VCR.shape[2:], F32)
                if c < 2:
                    RCR[o, c] = jnp.zeros(RCR.shape[2:], F32)

    def merge(F, Y, CR):
        for i in range(nx):
            F[D + i, ny:, :] = jnp.where(near, Y[1, i], Y[0, i])
        if CR is not None:
            merge_corners(F, CR)

    def merge_corners(F, CR):
        n, m = CR.shape[1:3]
        for c, (sx, sy) in enumerate(DIAGONALS):
            for t in range(n):
                low = ny if sy < 0 else wide - m
                F[(D + nx + t) if sx < 0 else (D - n + t), low:low + m, :] = CR[c, t]

    def vector_field(f):
        return copies_of(
            [(MX.at[f, :, 1], MX.at[f, :, nx + 1], (-1, 0)), (MX.at[f, :, nx], MX.at[f, :, 0], (1, 0)),
             (MYS.at[f, 0], MYH.at[f, 1], (0, -1)), (MYS.at[f, 1], MYH.at[f, 0], (0, 1)),
             (MCS.at[f, 0], MCH.at[f, 0], (1, -1)), (MCS.at[f, 1], MCH.at[f, 1], (-1, 1))],
            msend.at[f % 2], mrecv.at[f % 2])

    def put_vector(f, i, vs):
        for a in range(3):
            MX[f, a, i + 1] = vs[a]
            MYS[f, 0, a, slice(i, i + 1), :] = vs[a][0:1]
            MYS[f, 1, a, slice(i, i + 1), :] = vs[a][ny - 1:ny]

    def put_corners(f):
        MCS[f, 0] = MX[f, 1, nx, 0:1, :]
        MCS[f, 1] = MX[f, 0, 1, ny - 1:ny, :]

    nf = 1 + OUTER * INNER
    for d in range(1, ndev):
        pl.semaphore_signal(barrier, inc=1, device_id=peer(d), device_id_type=MESH)


    def stage_values(i, c):
        for side, y in ((0, 0), (1, ny - 1)):
            for a in range(3):
                MYS[0, side, a, i:i + 1, :] = MX[0, a, i + 1, y:y + 1, :]
        return c
    local[0].wait()
    for i in range(nx):
        XI[D + i, 0:ny, :] = ids[i] + 1
    stage_corners(XI, XIS)
    local[1].wait()
    stage_corners(P0, P0S)
    pl.semaphore_wait(barrier, ndev - 1)
    p_near, p_far = split_field(P0, P0Y, P0S, P0R, 2, zsend, zrecv)
    codes_near, codes_far = split_field(XI, XIY, XIS, XIR, D, isend, irecv)
    d_copy = vector_field(0)
    start(p_near)
    start(codes_near)
    start(codes_far)
    local[2].wait()
    loop(stage_values, 0)
    put_corners(0)
    start(d_copy)
    start(p_far)
    clear_missing(XI, XIY, XIR, D)
    clear_missing(P0, P0Y, P0R, 2)
    for outer in range(OUTER):
        clear_missing(U.at[INNER * outer], UY.at[outer], UCR.at[outer], D)
        clear_late(outer)

    def clear_vector(f, c):
        for side, j, s in ((-1, 0, 0), (1, nx + 1, 1)):
            @pl.when(jnp.logical_not(has[(side, 0)]))
            def _(j=j):
                for a in range(3):
                    MX[f, a, j] = zero

            @pl.when(jnp.logical_not(has[(0, side)]))
            def _(s=s):
                for a in range(3):
                    MYH[f, s, a] = zero8
        for c2, off in enumerate(DIAGONALS[:2]):
            @pl.when(jnp.logical_not(has[(-off[0], -off[1])]))
            def _(c2=c2):
                MCH[f, c2] = jnp.zeros((1, nz), F32)
        return c
    lax.fori_loop(0, nf, clear_vector, 0)

    def lookup(code, table_rows):
        out = [jnp.zeros(code.shape, F32) for _ in table_rows]
        for m in range(nmat):
            hit = code == m + 1
            out = [jnp.where(hit, mat[t, m], v) for t, v in zip(table_rows, out)]
        return out

    def look(j, part):
        code = XI[j, part, :]
        lam, shr, prm, sto, bio = lookup(code, (0, 1, 2, 3, 4))
        bio = 0.25 * bio
        LAM[j, part, :] = lam
        SHR[j, part, :] = shr
        PRM[j, part, :] = prm
        BIO[j, part, :] = bio
        STO[j, part, :] = sto
        STAB[j, part, :] = bio * bio / jnp.maximum(lam + 2.0 / 3.0 * shr, TINY)
    local[6].wait()
    for i in range(nx):
        look(D + i, slice(0, ny))
    wait_recv(codes_near)
    merge(XI, XIY, None)
    for i in range(nx):
        look(D + i, slice(ny, wide))
    for j in (D - 1, D + nx):
        look(j, slice(0, ny))

    def harmonic(one, two):
        return (2.0 * step_time) * one * two / jnp.maximum(one + two, TINY)

    def flow(j):
        prm = PRM[j]
        fzu = jnp.where(last_wide, 0.0, harmonic(prm, upz(prm)))
        fyu = harmonic(prm, upw(prm))
        FY[j], FZ[j] = fyu, fzu
        diag = STO[j] + STAB[j] + (FX[j] + FX[j + 1] + fyu + dnw(fyu) + fzu + dnz(fzu))
        DIAG[j] = diag
        PINV[j] = jnp.where(XI[j] > 0, 1.0 / jnp.maximum(diag, TINY), 0.0)

    def face(j):
        FX[j] = harmonic(PRM[j - 1], PRM[j])
    for j in range(D, D + nx + 1):
        face(j)
    for j in range(D, D + nx):
        flow(j)

    def rim():
        wait_recv(codes_far)
        merge_corners(XI, XIR)
        for j in (D - 1, D + nx):
            look(j, slice(ny, wide))
        for j in range(nx + 2 * D):
            if j < D - 1 or j > D + nx:
                look(j, slice(0, wide))
        for j in list(range(1, D + 1)) + list(range(D + nx, nx + 2 * D)):
            face(j)
        for j in list(range(1, D + 1)) + list(range(D + nx - 1, nx + 2 * D - 1)):
            flow(j)

    def stiff_face(t):
        SX[t] = 0.5 * (SHR[D + t - 2] + SHR[D + t - 1])

    def coefs(i):
        shr, lam = SHR[D + i], LAM[D + i]
        half = 0.5 * shr
        syu = 0.5 * (shr + upw(shr))
        syd = dnw(syu)
        szu = half + jnp.where(last_wide, 0.0, 0.5 * upz(shr))
        szd = half + jnp.where(first_wide, 0.0, 0.5 * dnz(shr))
        total = SX[i + 1] + SX[i + 2] + syu + syd + szu + szd
        if 0 <= i < nx:
            LAMY[slice(i, i + 1), :] = LAM[D + i, wide - 1:wide, :]
            SY[1, i], SY[0, i] = syu[:ny], syd[:ny]
            SZ[1, i] = jnp.where(last_lane, 0.0, szu[:ny])
            SZ[0, i] = jnp.where(first_lane, 0.0, szd[:ny])
            SSUM[i] = total[:ny]
        inside = XI[D + i] > 0
        hs = []
        for a, below in enumerate((LAM[D + i - 1], dnw(lam), jnp.where(first_wide, 0.0, dnz(lam)))):
            h = jnp.where(inside, 1.0 / jnp.maximum(total + below, TINY), 0.0)
            HB[a, i + 1] = h
            hs.append(h)
        KF[i + 1] = lam / (1.0 + lam * (hs[0] + hs[1] + hs[2]))

    def apply_pressure(F, j, rows):
        v = F[j]
        out = (DIAG[j] * v - FX[j + 1] * F[j + 1] - FX[j] * F[j - 1]
               - FY[j] * upw(v) - dnw(FY[j] * v)
               - FZ[j] * upz(v) - dnz(FZ[j] * v))
        return v[:rows], out[:rows]

    def apply_mech(f, emit, init, half=None, late=None):
        def below_y(corner):
            m = [MYH[f, 0, a] for a in range(3)]
            ahead = pltpu.roll(m[0], nx - 1, 0)
            if corner:
                ahead = jnp.where(rows8 == nx - 1, MCH[f, 1], ahead)
            z8 = jnp.where(lanes8 == nz - 1, 0.0, pltpu.roll(m[2], nz - 1, 1))
            LY[...] = LAMY[...] * (ahead - m[0] + MYS[f, 0, 1] - m[1] + z8 - m[2])

        def below_x():
            m = [MX[f, a, 0] for a in range(3)]
            return LAM[D - 1, 0:ny, :] * (MX[f, 0, 1] - m[0] + upy(m[1], MCH[f, 0]) - m[1]
                              + jnp.where(last_lane, 0.0, upz(m[2])) - m[2])

        below_y(late is None)
        edge = []
        if late is None:
            edge.append(below_x())

        def weigh(i):
            w = [MX[f, a, i + 1] for a in range(3)]
            return LAM[D + i, 0:ny, :] * (MX[f, 0, i + 2] - w[0] + upy(w[1], MYH[f, 1, 1, i:i + 1, :]) - w[1]
                                 + jnp.where(last_lane, 0.0, upz(w[2])) - w[2])

        def body(i, c):
            row = slice(i, i + 1)
            ws, outs, div = [], [], None
            for a in range(3):
                w, wx = MX[f, a, i + 1], MX[f, a, i + 2]
                wy, wz = upy(w, MYH[f, 1, a, row, :]), upz(w)
                out = (SSUM[i] * w - SX[i + 2, 0:ny, :] * wx - SX[i + 1, 0:ny, :] * MX[f, a, i]
                       - SY[1, i] * wy - SY[0, i] * dny(w, MYH[f, 0, a, row, :])
                       - SZ[1, i] * wz - SZ[0, i] * dnz(w))
                part = (wx, wy, jnp.where(last_lane, 0.0, wz))[a] - w
                div = part if div is None else div + part
                ws.append(w)
                outs.append(out)
            weighted = LAM[D + i, 0:ny, :] * div
            LW[i] = weighted
            before = edge[0] if i == 0 else weigh(i - 1) if i == nx - 1 or (i == 1 and late is not None) else LW[i - 1]
            below = (before, dny(weighted, LY[row, :]), jnp.where(first_lane, 0.0, dnz(weighted)))
            outs = [outs[a] + (below[a] - weighted) for a in range(3)]
            return emit(i, ws, outs, c)
        if late is not None:
            for i in range(1, nx - 1):
                init = body(i, init)
            late()
            below_y(True)
            edge.append(below_x())
            for i in (0, nx - 1):
                init = body(i, init)
            return init
        return loop(body, init, half=half)

    def block_solve(i, r, rows):
        part = slice(0, rows)
        scaled = [r[a] * HB[a, i + 1, part, :] for a in range(3)]
        tail = KF[i + 1, part, :] * (scaled[0] + scaled[1] + scaled[2])
        return [scaled[a] - HB[a, i + 1, part, :] * tail for a in range(3)]

    def dot3(a, b):
        return fold(a[0] * b[0] + a[1] * b[1] + a[2] * b[2])

    summed = []

    def all_sum(q, sums, meanwhile=None):
        row = jnp.zeros((1, 128), F32)
        for k, s in enumerate(sums):
            row = jnp.where(lane1 == k, jnp.sum(s, keepdims=True), row)
        RB[q, me] = row
        for d in sorted(range(1, ndev), key=lambda d: -min(d, ndev - d)):
            copy = pltpu.make_async_remote_copy(
                src_ref=RB.at[q, me], dst_ref=RB.at[q, me], send_sem=rsend.at[q],
                recv_sem=rrecv.at[q], device_id=peer(d), device_id_type=MESH)
            copy.start()
        every = RB.at[q, pl.ds(0, ndev - 1)]
        whole = pltpu.make_async_remote_copy(
            src_ref=every, dst_ref=every, send_sem=rsend.at[q], recv_sem=rrecv.at[q],
            device_id=peer(1), device_id_type=MESH)
        if meanwhile is not None:
            meanwhile()
        whole.wait_recv()
        summed.append(whole)
        parts = [RB[q, d] for d in range(ndev)]
        while len(parts) > 1:
            parts = [sum(parts[d + 1:d + 2], parts[d]) for d in range(0, len(parts), 2)]
        row = parts[0]
        return [row[:, k:k + 1] for k in range(len(sums))]

    def combine(t):
        n0, m0, m1, m2, m3, m4 = t
        n1 = m0 - n0
        n2 = m1 - n1
        l1, l2 = m1 / m0, m2 / m0
        d1 = m2 - l1 * m1
        e = m3 - l1 * m2
        l3 = jnp.where(d1 > 0, e / d1, 0.0)
        d2 = m4 - l2 * m2 - l3 * e
        y1 = n1 - l1 * n0
        y2 = n2 - l2 * n0 - l3 * y1
        c2 = jnp.where(d2 > 0, y2 / d2, 0.0)
        c1 = jnp.where(d1 > 0, y1 / d1, 0.0) - l3 * c2
        c0 = n0 / m0 - l1 * c1 - l2 * c2
        return c0, c1, c2

    zacc = jnp.zeros((8, 128), F32)
    wait_recv(p_near)
    merge(P0, P0Y, None)
    for i in range(nx):
        AP[i] = apply_pressure(P0, D + i, ny)[1]

    local[3].wait()
    local[4].wait()

    msent = []

    def retire(queue):
        if len(queue) == 2:
            wait_send(queue.pop(0))
    for outer in range(OUTER):
        base = 1 + INNER * outer

        u0 = U.at[INNER * outer]

        def p_start(i, acc):
            if outer > 0:
                m_change(i)
            own = slice(0, ny)
            rhs = (STO[D + i, own, :] * p_old[i] + step_time * fsource[i]
                   + STAB[D + i, own, :] * P0[D + i, own, :])
            if outer > 0:
                rhs = rhs - BIO[D + i, own, :] * DC[i]
            r = rhs - AP[i]
            u = r * PINV[D + i, own, :]
            u0[D + i, own, :] = u
            return acc + fold(r * u)
        if outer > 0:
            wait_send(made_p)
        n0 = loop(p_start, zacc)
        stage_corners(u0, UCS.at[outer])
        made_p = wide_field(u0, UY.at[outer], UCS.at[outer], UCR.at[outer], D, psend, precv)
        start(made_p)
        if outer > 0:
            loop(m_after, 0)
        if outer == 0:
            rim()
            for t in range(nx + 3):
                stiff_face(t)
            for i in range(-1, nx + 1):
                coefs(i)
            wait_recv(d_copy)
            wait_send(d_copy)

            def keep_ad(i, ws, outs, c):
                for a in range(3):
                    AD[a, i] = outs[a]
                    RX[0, a, i + 1, 0:ny, :] = bforce[a, i] - outs[a]
                return c
            local[5].wait()
            apply_mech(0, keep_ad, 0)
        else:
            wait_send(made_r)
        stage_load(outer)
        made_r = load_field(outer)
        start(made_r)
        sums = [n0]
        wait_recv(made_p[2:4])
        merge(u0, UY.at[outer], None)
        for k in range(INNER):
            sums = [jnp.sum(v, keepdims=True) for v in sums]
            F = U.at[INNER * outer + k]
            reach = 0 if k == INNER - 1 else D - 1 - k
            even, odd = zacc, zacc
            planes = list(range(D - reach, D + nx + reach))
            if k == 0:
                inner = planes[reach + 1:-reach - 1]
                planes = inner + [j for j in planes if j not in inner]
            for n, j in enumerate(planes):
                if k == 0 and n == len(inner):
                    wait_recv(made_p[:2] + made_p[4:])
                    merge_corners(u0, UCR.at[outer])
                own = D <= j < D + nx
                v, w = apply_pressure(F, j, wide if k < INNER - 1 else ny)
                if own:
                    WP[k, j - D] = w[:ny]
                    even = even + fold(v[:ny] * w[:ny])
                if k < INNER - 1:
                    u = w * PINV[j] - v
                    U[INNER * outer + k + 1, j] = u
                    if own:
                        odd = odd + fold(u[:ny] * w[:ny])
            sums += [even] if k == INNER - 1 else [even, odd]
            if k == INNER - 2:
                if outer > 0:
                    wait_send(made_v)
                stage_late(outer)
                made_v = late_field(outer)
                start(made_v)

        def arrivals():
            if outer == 0:
                wait_recv(p_far)
                merge_corners(P0, P0R)
                wait_send(p_near)
                wait_send(p_far)
            wait_recv(made_r)
            merge_load(outer)
            wait_recv(made_v)
            merge_late(outer)
        cs = combine(all_sum(2 * outer, sums, arrivals))

        for j in range(D - 2, D + nx + 1):
            v = P0[j]
            for k in range(INNER):
                v = v + cs[k] * U[INNER * outer + k, j]
            P0[j] = v

        n0 = zacc
        for i in range(-1, nx + 1):
            load = BIO[D + i] * P0[D + i]
            below = (BIO[D + i - 1] * P0[D + i - 1], dnw(load), jnp.where(first_wide, 0.0, dnz(load)))
            r = [RX[outer, a, i + 1] + (below[a] - load) for a in range(3)]
            u = block_solve(i, r, wide)
            if 0 <= i < nx:
                put_vector(base, i, [v[:ny] for v in u])
                for a in range(3):
                    MYH[base, 1, a, i:i + 1, :] = u[a][ny:ny + 1]
                    MYH[base, 0, a, i:i + 1, :] = u[a][wide - 1:wide]
                n0 = n0 + dot3([v[:ny] for v in r], [v[:ny] for v in u])
            else:
                for a in range(3):
                    MX[base, a, i + 1] = u[a][:ny]
                if i < 0:
                    MCH[base, 0] = u[1][ny:ny + 1]
                else:
                    MCH[base, 1] = u[0][wide - 1:wide]

        def send_planes(f, made):
            put_corners(f)
            start(made, True)

        def p_after(i, c):
            if outer == OUTER - 1:
                p_out[i] = P0[D + i, 0:ny, :]
            else:
                v = AP[i]
                for k in range(INNER):
                    v = v + cs[k] * WP[k, i]
                AP[i] = v
            return c
        loop(p_after, 0)
        sums = [n0]
        for k in range(INNER):
            sums = [jnp.sum(v, keepdims=True) for v in sums]
            late = None
            if k == INNER - 1:
                wait_recv(made[2:4])
                late = functools.partial(wait_recv, made[:2] + made[4:])
            elif k > 0:
                wait_recv(made)

            def m_step(i, v, w, c):
                if outer < OUTER - 1:
                    for a in range(3):
                        WM[k, a, i] = w[a]
                even = c[0] + dot3(v, w)
                if k == INNER - 1:
                    return (even,)
                z = block_solve(i, w, ny)
                u = [z[a] - v[a] for a in range(3)]
                put_vector(base + k + 1, i, u)
                return even, c[1] + dot3(u, w)
            half = None
            if k < INNER - 1:
                retire(msent)
                made = vector_field(base + k + 1)
                half = functools.partial(send_planes, base + k + 1, made)
            sums += apply_mech(base + k, m_step, (zacc,) * (1 if k == INNER - 1 else 2), half, late)
            if k < INNER - 1:
                start(made, False)
                msent.append(made)
        def changes():
            for k in range(INNER):
                for i in range(nx):
                    w = [MX[base + k, a, i + 1] for a in range(3)]
                    DK[k, i] = (MX[base + k, 0, i + 2] - w[0] + upy(w[1], MYH[base + k, 1, 1, i:i + 1, :]) - w[1]
                                + jnp.where(last_lane, 0.0, upz(w[2])) - w[2])
        cs = combine(all_sum(2 * outer + 1, sums, changes if outer < OUTER - 1 else None))

        def mixed(get, cs=cs, base=base):
            v = cs[0] * get(base)
            for k in range(1, INNER):
                v = v + cs[k] * get(base + k)
            return v

        def m_change(i, outer=outer, cs=cs):
            v = DC[i] if outer > 0 else None
            for k in range(INNER):
                part = cs[k] * DK[k, i]
                v = part if v is None else v + part
            DC[i] = v

        def m_after(i, c, cs=cs, mixed=mixed, outer=outer):
            for a in range(3):
                before = MX[0, a, i + 1] if outer == 0 else d_out[a, i]
                d_out[a, i] = before + mixed(lambda f, a=a: MX[f, a, i + 1])
            if outer < OUTER - 1:
                for a in range(3):
                    v = AD[a, i]
                    for k in range(INNER):
                        v = v + cs[k] * WM[k, a, i]
                    RX[outer + 1, a, i + 1, 0:ny, :] = bforce[a, i] - v
            return c
        if outer == OUTER - 1:
            loop(m_after, 0)

    for made in msent + [codes_near, codes_far, made_p, made_r, made_v]:
        wait_send(made)
    for copy in summed:
        copy.wait_send()


def on_device(dims, d_old, p_old, bforce, fsource, ids, materials):
    ngx, ngy, nx, ny, nz, nmat = dims
    nf = 1 + OUTER * INNER
    nq = 2 * OUTER

    def vm(*shape, dtype=F32):
        return pltpu.VMEM(shape, dtype)
    plane, strip = (ny, nz), (nx, nz)
    cell = (nx, ny, nz)
    ext = (nx + 2, ny, nz)
    broad = (ny + 8, nz)
    big = (nx + 2 * D, ny + 8, nz)
    edge = (2, nx, 8, nz)
    corner = (4, D - 1, 2 if D == 3 else 4, nz)
    dma = pltpu.SemaphoreType.DMA
    scratch = [
        pltpu.SMEM((5, nmat), F32), vm(*cell), vm(3, *cell), vm(*cell), vm(*cell, dtype=jnp.int32), dma((7,)),
        vm(*big, dtype=jnp.int32), vm(*edge, dtype=jnp.int32),
        vm(*corner, dtype=jnp.int32), vm(*corner, dtype=jnp.int32),
        vm(*big), vm(*big), vm(*big), vm(*big), vm(*big), vm(*big), vm(*strip),
        vm(nx + 3, *broad), vm(2, *cell), vm(2, *cell), vm(*cell),
        vm(*big), vm(*big), vm(*big), vm(*big), vm(*big),
        vm(3, nx + 2, *broad), vm(nx + 2, *broad),
        vm(*big), vm(*edge), vm(*corner), vm(*corner), vm(OUTER * INNER, *big), vm(OUTER, *edge), vm(OUTER, *corner), vm(OUTER, *corner),
        vm(OUTER, nx, 8, nz), vm(OUTER, 3, INNER - 1, 2, 2, nz), vm(OUTER, 3, INNER - 1, 2, 2, nz),
        vm(OUTER, 3, nx + 2, *broad), vm(OUTER, 2, 3, nx, 8, nz), vm(OUTER, 2, 3, 1, nz), vm(OUTER, 2, 3, 1, nz),
        vm(nf, 3, *ext), vm(nf, 2, 3, *strip), vm(nf, 2, 3, *strip), vm(nf, 2, 1, nz), vm(nf, 2, 1, nz),
        vm(INNER, *cell), vm(INNER, 3, *cell), vm(*cell), vm(3, *cell), vm(*cell), vm(INNER, *cell),
        vm(*strip), vm(*cell), vm(nq, ngx * ngy, 1, 128),
        dma((10,)), dma((10,)), dma((10,)), dma((10,)), dma((5,)), dma((5,)), dma((6,)), dma((6,)), dma((8,)), dma((8,)), dma((2, 6)), dma((2, 6)),
        dma((nq,)), dma((nq,)),
    ]
    block = pl.BlockSpec(memory_space=pltpu.VMEM)
    return pl.pallas_call(
        functools.partial(kernel, dims),
        out_shape=(pltpu.VMEM(d_old.shape, F32), pltpu.VMEM(p_old.shape, F32)),
        in_specs=[pl.BlockSpec(memory_space=pl.ANY)] * 6,
        out_specs=(block, block),
        scratch_shapes=scratch,
        compiler_params=pltpu.CompilerParams(
            collective_id=0, has_side_effects=True,
            vmem_limit_bytes=VMEM_BYTES - 4 * (d_old.size + p_old.size) - 131072),
        name="poro",
    )(materials, d_old, p_old, bforce, fsource, ids)


def solution(mesh):
    ngx, ngy = mesh.shape["gx"], mesh.shape["gy"]

    def body(d_old, p_old, bforce, fsource, ids, materials):
        dims = (ngx, ngy, *p_old.shape, materials.shape[1])
        return on_device(dims, d_old, p_old, bforce, fsource, ids, materials)

    return jax.shard_map(
        body,
        mesh=mesh,
        in_specs=(P(None, "gx", "gy", None), P("gx", "gy", None), P(None, "gx", "gy", None),
                  P("gx", "gy", None), P("gx", "gy", None), P()),
        out_specs=(P(None, "gx", "gy", None), P("gx", "gy", None)),
        check_vma=False,
    )
```

```python
import functools
import jax
import jax.numpy as jnp
from jax import lax
from jax.experimental import pallas as pl
from jax.experimental.pallas import tpu as pltpu
from jax.sharding import PartitionSpec as P

OUTER = 2
INNER = 3
step_time = 4.0
D = INNER
TINY = 1e-30
VMEM_BYTES = 67043328
DIAGONALS = ((1, -1), (-1, 1), (1, 1), (-1, -1))
MESH = pl.DeviceIdType.MESH
F32 = jnp.float32


def kernel(dims, *refs):
    ngx, ngy, nx, ny, nz, nmat = dims
    (mat_hbm, d_hbm, p_hbm, bf_hbm, fs_hbm, ids_hbm, d_out, p_out,
     mat, p_old, bforce, fsource, ids, lsem,
     XI, XIY, XIS, XIR, LAM, SHR, PRM, BIO, STO, STAB, LAMY,
     SX, SY, SZ, SSUM, FX, FY, FZ, DIAG, PINV, HB, KF,
     P0, P0Y, P0S, P0R, U, UY, UCS, UCR, VY, VCS, VCR, RX, RY, RCS, RCR, MX, MYS, MYH, MCS, MCH,
     WP, WM, AP, AD, DC, DK, LY, LW, RB,
     isend, irecv, zsend, zrecv, vsend, vrecv, wsend, wrecv, psend, precv, msend, mrecv, rsend, rrecv) = refs
    gx, gy = lax.axis_index("gx"), lax.axis_index("gy")
    local = [pltpu.make_async_copy(src, dst, lsem.at[n]) for n, (src, dst) in enumerate((
        (ids_hbm, ids), (p_hbm, P0.at[pl.ds(D, nx), pl.ds(0, ny)]), (d_hbm, MX.at[0, :, pl.ds(1, nx)]),
        (p_hbm, p_old), (fs_hbm, fsource), (bf_hbm, bforce), (mat_hbm, mat)))]
    for copy in local:
        copy.start()
    barrier = pltpu.get_barrier_semaphore()
    me, ndev = gx * ngy + gy, ngx * ngy

    def peer(d):
        t = lax.rem(me + d, ndev)
        return lax.div(t, ngy), lax.rem(t, ngy)
    has = {(-1, 0): gx > 0, (1, 0): gx < ngx - 1, (0, -1): gy > 0, (0, 1): gy < ngy - 1}
    for c in DIAGONALS:
        has[c] = jnp.logical_and(has[(c[0], 0)], has[(0, c[1])])

    rows = lax.broadcasted_iota(jnp.int32, (ny, nz), 0)
    lanes = lax.broadcasted_iota(jnp.int32, (ny, nz), 1)
    lanes8 = lax.broadcasted_iota(jnp.int32, (nx, nz), 1)
    rows8 = lax.broadcasted_iota(jnp.int32, (nx, nz), 0)
    lane1 = lax.broadcasted_iota(jnp.int32, (1, 128), 1)
    first_row, last_row = rows == 0, rows == ny - 1
    first_lane, last_lane = lanes == 0, lanes == nz - 1
    zero = jnp.zeros((ny, nz), F32)
    near = lax.broadcasted_iota(jnp.int32, (8, nz), 0) < 4
    wide = ny + 8
    first_wide = lax.broadcasted_iota(jnp.int32, (wide, nz), 1) == 0
    last_wide = lax.broadcasted_iota(jnp.int32, (wide, nz), 1) == nz - 1
    zero8 = jnp.zeros((nx, nz), F32)

    def upz(v):
        return pltpu.roll(v, nz - 1, 1)

    def dnz(v):
        return pltpu.roll(v, 1, 1)

    def upy(v, halo):
        return jnp.where(last_row, halo, pltpu.roll(v, ny - 1, 0))

    def dny(v, halo):
        return jnp.where(first_row, halo, pltpu.roll(v, 1, 0))

    def upw(v):
        return pltpu.roll(v, wide - 1, 0)

    def dnw(v):
        return pltpu.roll(v, 1, 0)

    def fold(v):
        out = None
        for i in range(0, ny, 8):
            for j in range(0, nz, 128):
                part = v[i:i + 8, j:j + 128]
                out = part if out is None else out + part
        return out

    def loop(body, init, low=0, high=nx, half=None):
        order = [low, high - 1] + list(range(low + 1, high - 1))
        for n, i in enumerate(order):
            init = body(i, init)
            if n == 1 and half is not None:
                half()
        return init

    def copies_of(pairs, send, recv):
        made = []
        for n, (src, dst, off) in enumerate(pairs):
            copy = pltpu.make_async_remote_copy(
                src_ref=src, dst_ref=dst, send_sem=send.at[n], recv_sem=recv.at[n],
                device_id=(gx + off[0], gy + off[1]), device_id_type=MESH)
            made.append((copy, off))
        return made

    def start(made, along=None):
        for copy, off in made:
            if along is not None and (off[0] != 0) != along:
                continue
            @pl.when(has[off])
            def _(copy=copy):
                copy.start()

    def wait_recv(made):
        for copy, off in made:
            @pl.when(has[(-off[0], -off[1])])
            def _(copy=copy):
                copy.wait_recv()

    def wait_send(made):
        for copy, off in made:
            @pl.when(has[off])
            def _(copy=copy):
                copy.wait_send()

    def wide_field(F, Y, CS, CR, depth, send, recv):
        pairs = [(F.at[pl.ds(D, depth), pl.ds(0, ny)], F.at[pl.ds(D + nx, depth), pl.ds(0, ny)], (-1, 0)),
                 (F.at[pl.ds(D + nx - depth, depth), pl.ds(0, ny)], F.at[pl.ds(D - depth, depth), pl.ds(0, ny)], (1, 0)),
                 (F.at[pl.ds(D, nx), pl.ds(0, 8)], Y.at[1], (0, -1)),
                 (F.at[pl.ds(D, nx), pl.ds(ny - 8, 8)], Y.at[0], (0, 1))]
        if CS is not None:
            pairs += [(CS.at[c], CR.at[c], off) for c, off in enumerate(DIAGONALS)]
        return copies_of(pairs, send, recv)

    def split_field(F, Y, CS, CR, depth, send, recv):
        far = depth - 1
        pairs = [(F.at[pl.ds(D, 1), pl.ds(0, ny)], F.at[pl.ds(D + nx, 1), pl.ds(0, ny)], (-1, 0)),
                 (F.at[pl.ds(D + nx - 1, 1), pl.ds(0, ny)], F.at[pl.ds(D - 1, 1), pl.ds(0, ny)], (1, 0)),
                 (F.at[pl.ds(D, nx), pl.ds(0, 8)], Y.at[1], (0, -1)),
                 (F.at[pl.ds(D, nx), pl.ds(ny - 8, 8)], Y.at[0], (0, 1)),
                 (F.at[pl.ds(D + 1, far), pl.ds(0, ny)], F.at[pl.ds(D + nx + 1, far), pl.ds(0, ny)], (-1, 0)),
                 (F.at[pl.ds(D + nx - depth, far), pl.ds(0, ny)], F.at[pl.ds(D - depth, far), pl.ds(0, ny)], (1, 0))]
        pairs += [(CS.at[c], CR.at[c], off) for c, off in enumerate(DIAGONALS)]
        made = copies_of(pairs, send, recv)
        return made[:4], made[4:]

    def stage_corners(F, CS):
        n, m = CS.shape[1:3]
        for c, (sx, sy) in enumerate(DIAGONALS):
            for t in range(n):
                CS[c, t] = F[D + (t if sx < 0 else nx - n + t), (0 if sy < 0 else ny - m):(m if sy < 0 else ny), :]

    def clear_missing(F, Y, CR, depth):
        none = jnp.zeros((wide, nz), F.dtype)
        for side, low in ((-1, D - depth), (1, D + nx)):
            @pl.when(jnp.logical_not(has[(side, 0)]))
            def _(low=low):
                for t in range(depth):
                    F[low + t] = none
        for side, s in ((-1, 0), (1, 1)):
            @pl.when(jnp.logical_not(has[(0, side)]))
            def _(s=s):
                for i in range(nx):
                    Y[s, i] = none[:8]
        if CR is not None:
            for c, off in enumerate(DIAGONALS):
                @pl.when(jnp.logical_not(has[(-off[0], -off[1])]))
                def _(c=c):
                    CR[c] = jnp.zeros(CR.shape[1:], F.dtype)

    def late_field(o):
        last = U.at[INNER * o + INNER - 1]
        pairs = [(last.at[pl.ds(D + nx - 2, 1), pl.ds(0, ny)], last.at[pl.ds(D - 2, 1), pl.ds(0, ny)], (1, 0)),
                 (last.at[pl.ds(D, nx), pl.ds(ny - 8, 8)], VY.at[o], (0, 1))]
        pairs += [(VCS.at[o, c], VCR.at[o, c], off) for c, off in enumerate(DIAGONALS[:3])]
        return copies_of(pairs, vsend, vrecv)

    def stage_late(o):
        for c, (sx, sy) in enumerate(DIAGONALS[:3]):
            for k in range(1, INNER):
                for t in range(2):
                    VCS[o, c, k - 1, t] = U[INNER * o + k, D + (t if sx < 0 else nx - 2 + t),
                                            (0 if sy < 0 else ny - 2):(2 if sy < 0 else ny), :]

    def merge_late(o):
        f = INNER * o + INNER - 1
        for i in range(nx):
            U[f, D + i, ny:, :] = jnp.where(near, U[f, D + i, ny:, :], VY[o, i])
        for c, (sx, sy) in enumerate(DIAGONALS[:3]):
            for k in range(1, INNER):
                for t in range(2):
                    low = ny if sy < 0 else wide - 2
                    U[INNER * o + k, (D + nx + t) if sx < 0 else (D - 2 + t), low:low + 2, :] = VCR[o, c, k - 1, t]

    def load_field(o):
        F = RX.at[o]
        pairs = [(F.at[:, pl.ds(1, 1), pl.ds(0, ny)], F.at[:, pl.ds(nx + 1, 1), pl.ds(0, ny)], (-1, 0)),
                 (F.at[:, pl.ds(nx, 1), pl.ds(0, ny)], F.at[:, pl.ds(0, 1), pl.ds(0, ny)], (1, 0)),
                 (F.at[:, pl.ds(1, nx), pl.ds(0, 8)], RY.at[o, 1], (0, -1)),
                 (F.at[:, pl.ds(1, nx), pl.ds(ny - 8, 8)], RY.at[o, 0], (0, 1)),
                 (RCS.at[o, 0], RCR.at[o, 0], DIAGONALS[0]), (RCS.at[o, 1], RCR.at[o, 1], DIAGONALS[1])]
        return copies_of(pairs, wsend, wrecv)

    def stage_load(o):
        for a in range(3):
            RCS[o, 0, a] = RX[o, a, nx, 0:1, :]
            RCS[o, 1, a] = RX[o, a, 1, ny - 1:ny, :]

    def merge_load(o):
        for a in range(3):
            for i in range(nx):
                RX[o, a, i + 1, ny:, :] = jnp.where(near, RY[o, 1, a, i], RY[o, 0, a, i])
            RX[o, a, 0, ny:ny + 1, :] = RCR[o, 0, a]
            RX[o, a, nx + 1, wide - 1:wide, :] = RCR[o, 1, a]

    def clear_late(o):
        none = jnp.zeros((wide, nz), F32)

        @pl.when(jnp.logical_not(has[(-1, 0)]))
        def _():
            U[INNER * o + INNER - 1, D - 2] = none
            for a in range(3):
                RX[o, a, 0] = none

        @pl.when(jnp.logical_not(has[(1, 0)]))
        def _():
            for a in range(3):
                RX[o, a, nx + 1] = none

        @pl.when(jnp.logical_not(has[(0, -1)]))
        def _():
            for i in range(nx):
                VY[o, i] = none[:8]
                for a in range(3):
                    RY[o, 0, a, i] = none[:8]

        @pl.when(jnp.logical_not(has[(0, 1)]))
        def _():
            for i in range(nx):
                for a in range(3):
                    RY[o, 1, a, i] = none[:8]
        for c, off in enumerate(DIAGONALS[:3]):
            @pl.when(jnp.logical_not(has[(-off[0], -off[1])]))
            def _(c=c):
                VCR[o, c] = jnp.zeros(VCR.shape[2:], F32)
                if c < 2:
                    RCR[o, c] = jnp.zeros(RCR.shape[2:], F32)

    def merge(F, Y, CR):
        for i in range(nx):
            F[D + i, ny:, :] = jnp.where(near, Y[1, i], Y[0, i])
        if CR is not None:
            merge_corners(F, CR)

    def merge_corners(F, CR):
        n, m = CR.shape[1:3]
        for c, (sx, sy) in enumerate(DIAGONALS):
            for t in range(n):
                low = ny if sy < 0 else wide - m
                F[(D + nx + t) if sx < 0 else (D - n + t), low:low + m, :] = CR[c, t]

    def vector_field(f):
        return copies_of(
            [(MX.at[f, :, 1], MX.at[f, :, nx + 1], (-1, 0)), (MX.at[f, :, nx], MX.at[f, :, 0], (1, 0)),
             (MYS.at[f, 0], MYH.at[f, 1], (0, -1)), (MYS.at[f, 1], MYH.at[f, 0], (0, 1)),
             (MCS.at[f, 0], MCH.at[f, 0], (1, -1)), (MCS.at[f, 1], MCH.at[f, 1], (-1, 1))],
            msend.at[f % 2], mrecv.at[f % 2])

    def put_vector(f, i, vs):
        for a in range(3):
            MX[f, a, i + 1] = vs[a]
            MYS[f, 0, a, slice(i, i + 1), :] = vs[a][0:1]
            MYS[f, 1, a, slice(i, i + 1), :] = vs[a][ny - 1:ny]

    def put_corners(f):
        MCS[f, 0] = MX[f, 1, nx, 0:1, :]
        MCS[f, 1] = MX[f, 0, 1, ny - 1:ny, :]

    nf = 1 + OUTER * INNER
    for d in range(1, ndev):
        pl.semaphore_signal(barrier, inc=1, device_id=peer(d), device_id_type=MESH)


    def stage_values(i, c):
        for side, y in ((0, 0), (1, ny - 1)):
            for a in range(3):
                MYS[0, side, a, i:i + 1, :] = MX[0, a, i + 1, y:y + 1, :]
        return c
    local[0].wait()
    for i in range(nx):
        XI[D + i, 0:ny, :] = ids[i] + 1
    stage_corners(XI, XIS)
    local[1].wait()
    stage_corners(P0, P0S)
    pl.semaphore_wait(barrier, ndev - 1)
    p_near, p_far = split_field(P0, P0Y, P0S, P0R, 2, zsend, zrecv)
    codes_near, codes_far = split_field(XI, XIY, XIS, XIR, D, isend, irecv)
    d_copy = vector_field(0)
    start(p_near)
    start(codes_near)
    start(codes_far)
    local[2].wait()
    loop(stage_values, 0)
    put_corners(0)
    start(d_copy)
    start(p_far)
    clear_missing(XI, XIY, XIR, D)
    clear_missing(P0, P0Y, P0R, 2)
    for outer in range(OUTER):
        clear_missing(U.at[INNER * outer], UY.at[outer], UCR.at[outer], D)
        clear_late(outer)

    def clear_vector(f, c):
        for side, j, s in ((-1, 0, 0), (1, nx + 1, 1)):
            @pl.when(jnp.logical_not(has[(side, 0)]))
            def _(j=j):
                for a in range(3):
                    MX[f, a, j] = zero

            @pl.when(jnp.logical_not(has[(0, side)]))
            def _(s=s):
                for a in range(3):
                    MYH[f, s, a] = zero8
        for c2, off in enumerate(DIAGONALS[:2]):
            @pl.when(jnp.logical_not(has[(-off[0], -off[1])]))
            def _(c2=c2):
                MCH[f, c2] = jnp.zeros((1, nz), F32)
        return c
    lax.fori_loop(0, nf, clear_vector, 0)

    def lookup(code, table_rows):
        out = [jnp.zeros(code.shape, F32) for _ in table_rows]
        for m in range(nmat):
            hit = code == m + 1
            out = [jnp.where(hit, mat[t, m], v) for t, v in zip(table_rows, out)]
        return out

    def look(j, part):
        code = XI[j, part, :]
        lam, shr, prm, sto, bio = lookup(code, (0, 1, 2, 3, 4))
        bio = 0.25 * bio
        LAM[j, part, :] = lam
        SHR[j, part, :] = shr
        PRM[j, part, :] = prm
        BIO[j, part, :] = bio
        STO[j, part, :] = sto
        STAB[j, part, :] = bio * bio / jnp.maximum(lam + 2.0 / 3.0 * shr, TINY)
    local[6].wait()
    for i in range(nx):
        look(D + i, slice(0, ny))
    wait_recv(codes_near[2:])
    merge(XI, XIY, None)
    for i in range(nx):
        look(D + i, slice(ny, wide))

    def harmonic(one, two):
        return (2.0 * step_time) * one * two / jnp.maximum(one + two, TINY)

    def flow(j):
        prm = PRM[j]
        fzu = jnp.where(last_wide, 0.0, harmonic(prm, upz(prm)))
        fyu = harmonic(prm, upw(prm))
        FY[j], FZ[j] = fyu, fzu
        diag = STO[j] + STAB[j] + (FX[j] + FX[j + 1] + fyu + dnw(fyu) + fzu + dnz(fzu))
        DIAG[j] = diag
        PINV[j] = jnp.where(XI[j] > 0, 1.0 / jnp.maximum(diag, TINY), 0.0)

    def face(j):
        FX[j] = harmonic(PRM[j - 1], PRM[j])
    for j in range(D + 1, D + nx):
        face(j)
    for j in range(D + 1, D + nx - 1):
        flow(j)
    wait_recv(codes_near[:2])
    for j in (D - 1, D + nx):
        look(j, slice(0, ny))
    for j in (D, D + nx):
        face(j)
    for j in (D, D + nx - 1):
        flow(j)

    def rim():
        wait_recv(codes_far)
        merge_corners(XI, XIR)
        for j in (D - 1, D + nx):
            look(j, slice(ny, wide))
        for j in range(nx + 2 * D):
            if j < D - 1 or j > D + nx:
                look(j, slice(0, wide))
        for j in list(range(1, D + 1)) + list(range(D + nx, nx + 2 * D)):
            face(j)
        for j in list(range(1, D + 1)) + list(range(D + nx - 1, nx + 2 * D - 1)):
            flow(j)

    def stiff_face(t):
        SX[t] = 0.5 * (SHR[D + t - 2] + SHR[D + t - 1])

    def coefs(i):
        shr, lam = SHR[D + i], LAM[D + i]
        half = 0.5 * shr
        syu = 0.5 * (shr + upw(shr))
        syd = dnw(syu)
        szu = half + jnp.where(last_wide, 0.0, 0.5 * upz(shr))
        szd = half + jnp.where(first_wide, 0.0, 0.5 * dnz(shr))
        total = SX[i + 1] + SX[i + 2] + syu + syd + szu + szd
        if 0 <= i < nx:
            LAMY[slice(i, i + 1), :] = LAM[D + i, wide - 1:wide, :]
            SY[1, i], SY[0, i] = syu[:ny], syd[:ny]
            SZ[1, i] = jnp.where(last_lane, 0.0, szu[:ny])
            SZ[0, i] = jnp.where(first_lane, 0.0, szd[:ny])
            SSUM[i] = total[:ny]
        inside = XI[D + i] > 0
        hs = []
        for a, below in enumerate((LAM[D + i - 1], dnw(lam), jnp.where(first_wide, 0.0, dnz(lam)))):
            h = jnp.where(inside, 1.0 / jnp.maximum(total + below, TINY), 0.0)
            HB[a, i + 1] = h
            hs.append(h)
        KF[i + 1] = lam / (1.0 + lam * (hs[0] + hs[1] + hs[2]))

    def apply_pressure(F, j, rows):
        v = F[j]
        out = (DIAG[j] * v - FX[j + 1] * F[j + 1] - FX[j] * F[j - 1]
               - FY[j] * upw(v) - dnw(FY[j] * v)
               - FZ[j] * upz(v) - dnz(FZ[j] * v))
        return v[:rows], out[:rows]

    def apply_mech(f, emit, init, half=None, late=None):
        def below_y(corner):
            m = [MYH[f, 0, a] for a in range(3)]
            ahead = pltpu.roll(m[0], nx - 1, 0)
            if corner:
                ahead = jnp.where(rows8 == nx - 1, MCH[f, 1], ahead)
            z8 = jnp.where(lanes8 == nz - 1, 0.0, pltpu.roll(m[2], nz - 1, 1))
            LY[...] = LAMY[...] * (ahead - m[0] + MYS[f, 0, 1] - m[1] + z8 - m[2])

        def below_x():
            m = [MX[f, a, 0] for a in range(3)]
            return LAM[D - 1, 0:ny, :] * (MX[f, 0, 1] - m[0] + upy(m[1], MCH[f, 0]) - m[1]
                              + jnp.where(last_lane, 0.0, upz(m[2])) - m[2])

        below_y(late is None)
        edge = []
        if late is None:
            edge.append(below_x())

        def weigh(i):
            w = [MX[f, a, i + 1] for a in range(3)]
            return LAM[D + i, 0:ny, :] * (MX[f, 0, i + 2] - w[0] + upy(w[1], MYH[f, 1, 1, i:i + 1, :]) - w[1]
                                 + jnp.where(last_lane, 0.0, upz(w[2])) - w[2])

        def body(i, c):
            row = slice(i, i + 1)
            ws, outs, div = [], [], None
            for a in range(3):
                w, wx = MX[f, a, i + 1], MX[f, a, i + 2]
                wy, wz = upy(w, MYH[f, 1, a, row, :]), upz(w)
                out = (SSUM[i] * w - SX[i + 2, 0:ny, :] * wx - SX[i + 1, 0:ny, :] * MX[f, a, i]
                       - SY[1, i] * wy - SY[0, i] * dny(w, MYH[f, 0, a, row, :])
                       - SZ[1, i] * wz - SZ[0, i] * dnz(w))
                part = (wx, wy, jnp.where(last_lane, 0.0, wz))[a] - w
                div = part if div is None else div + part
                ws.append(w)
                outs.append(out)
            weighted = LAM[D + i, 0:ny, :] * div
            LW[i] = weighted
            before = edge[0] if i == 0 else weigh(i - 1) if i == nx - 1 or (i == 1 and late is not None) else LW[i - 1]
            below = (before, dny(weighted, LY[row, :]), jnp.where(first_lane, 0.0, dnz(weighted)))
            outs = [outs[a] + (below[a] - weighted) for a in range(3)]
            return emit(i, ws, outs, c)
        if late is not None:
            for i in range(1, nx - 1):
                init = body(i, init)
            late()
            below_y(True)
            edge.append(below_x())
            for i in (0, nx - 1):
                init = body(i, init)
            return init
        return loop(body, init, half=half)

    def block_solve(i, r, rows):
        part = slice(0, rows)
        scaled = [r[a] * HB[a, i + 1, part, :] for a in range(3)]
        tail = KF[i + 1, part, :] * (scaled[0] + scaled[1] + scaled[2])
        return [scaled[a] - HB[a, i + 1, part, :] * tail for a in range(3)]

    def dot3(a, b):
        return fold(a[0] * b[0] + a[1] * b[1] + a[2] * b[2])

    summed = []

    def all_sum(q, sums, meanwhile=None):
        row = jnp.zeros((1, 128), F32)
        for k, s in enumerate(sums):
            row = jnp.where(lane1 == k, jnp.sum(s, keepdims=True), row)
        RB[q, me] = row
        for d in sorted(range(1, ndev), key=lambda d: -min(d, ndev - d)):
            copy = pltpu.make_async_remote_copy(
                src_ref=RB.at[q, me], dst_ref=RB.at[q, me], send_sem=rsend.at[q],
                recv_sem=rrecv.at[q], device_id=peer(d), device_id_type=MESH)
            copy.start()
        every = RB.at[q, pl.ds(0, ndev - 1)]
        whole = pltpu.make_async_remote_copy(
            src_ref=every, dst_ref=every, send_sem=rsend.at[q], recv_sem=rrecv.at[q],
            device_id=peer(1), device_id_type=MESH)
        if meanwhile is not None:
            meanwhile()
        whole.wait_recv()
        summed.append(whole)
        parts = [RB[q, d] for d in range(ndev)]
        while len(parts) > 1:
            parts = [sum(parts[d + 1:d + 2], parts[d]) for d in range(0, len(parts), 2)]
        row = parts[0]
        return [row[:, k:k + 1] for k in range(len(sums))]

    def combine(t):
        n0, m0, m1, m2, m3, m4 = t
        n1 = m0 - n0
        n2 = m1 - n1
        l1, l2 = m1 / m0, m2 / m0
        d1 = m2 - l1 * m1
        e = m3 - l1 * m2
        l3 = jnp.where(d1 > 0, e / d1, 0.0)
        d2 = m4 - l2 * m2 - l3 * e
        y1 = n1 - l1 * n0
        y2 = n2 - l2 * n0 - l3 * y1
        c2 = jnp.where(d2 > 0, y2 / d2, 0.0)
        c1 = jnp.where(d1 > 0, y1 / d1, 0.0) - l3 * c2
        c0 = n0 / m0 - l1 * c1 - l2 * c2
        return c0, c1, c2

    zacc = jnp.zeros((8, 128), F32)
    wait_recv(p_near)
    merge(P0, P0Y, None)
    for i in range(nx):
        AP[i] = apply_pressure(P0, D + i, ny)[1]

    local[3].wait()
    local[4].wait()

    msent = []

    def retire(queue):
        if len(queue) == 2:
            wait_send(queue.pop(0))
    for outer in range(OUTER):
        base = 1 + INNER * outer

        u0 = U.at[INNER * outer]

        def p_start(i, acc):
            if outer > 0:
                m_change(i)
            own = slice(0, ny)
            rhs = (STO[D + i, own, :] * p_old[i] + step_time * fsource[i]
                   + STAB[D + i, own, :] * P0[D + i, own, :])
            if outer > 0:
                rhs = rhs - BIO[D + i, own, :] * DC[i]
            r = rhs - AP[i]
            u = r * PINV[D + i, own, :]
            u0[D + i, own, :] = u
            return acc + fold(r * u)
        if outer > 0:
            wait_send(made_p)
        n0 = loop(p_start, zacc)
        stage_corners(u0, UCS.at[outer])
        made_p = wide_field(u0, UY.at[outer], UCS.at[outer], UCR.at[outer], D, psend, precv)
        start(made_p)
        if outer > 0:
            loop(m_after, 0)
        if outer == 0:
            rim()
            for t in range(nx + 3):
                stiff_face(t)
            for i in range(-1, nx + 1):
                coefs(i)
            wait_recv(d_copy)
            wait_send(d_copy)

            def keep_ad(i, ws, outs, c):
                for a in range(3):
                    AD[a, i] = outs[a]
                    RX[0, a, i + 1, 0:ny, :] = bforce[a, i] - outs[a]
                return c
            local[5].wait()
            apply_mech(0, keep_ad, 0)
        else:
            wait_send(made_r)
        stage_load(outer)
        made_r = load_field(outer)
        start(made_r)
        sums = [n0]
        wait_recv(made_p[2:4])
        merge(u0, UY.at[outer], None)
        for k in range(INNER):
            sums = [jnp.sum(v, keepdims=True) for v in sums]
            F = U.at[INNER * outer + k]
            reach = 0 if k == INNER - 1 else D - 1 - k
            even, odd = zacc, zacc
            planes = list(range(D - reach, D + nx + reach))
            if k == 0:
                inner = planes[reach + 1:-reach - 1]
                planes = inner + [j for j in planes if j not in inner]
            for n, j in enumerate(planes):
                if k == 0 and n == len(inner):
                    wait_recv(made_p[:2] + made_p[4:])
                    merge_corners(u0, UCR.at[outer])
                own = D <= j < D + nx
                v, w = apply_pressure(F, j, wide if k < INNER - 1 else ny)
                if own:
                    WP[k, j - D] = w[:ny]
                    even = even + fold(v[:ny] * w[:ny])
                if k < INNER - 1:
                    u = w * PINV[j] - v
                    U[INNER * outer + k + 1, j] = u
                    if own:
                        odd = odd + fold(u[:ny] * w[:ny])
            sums += [even] if k == INNER - 1 else [even, odd]
            if k == INNER - 2:
                if outer > 0:
                    wait_send(made_v)
                stage_late(outer)
                made_v = late_field(outer)
                start(made_v)

        def arrivals():
            if outer == 0:
                wait_recv(p_far)
                merge_corners(P0, P0R)
                wait_send(p_near)
                wait_send(p_far)
            wait_recv(made_r)
            merge_load(outer)
            wait_recv(made_v)
            merge_late(outer)
        cs = combine(all_sum(2 * outer, sums, arrivals))

        for j in range(D - 2, D + nx + 1):
            v = P0[j]
            for k in range(INNER):
                v = v + cs[k] * U[INNER * outer + k, j]
            P0[j] = v

        n0 = zacc
        for i in range(-1, nx + 1):
            load = BIO[D + i] * P0[D + i]
            below = (BIO[D + i - 1] * P0[D + i - 1], dnw(load), jnp.where(first_wide, 0.0, dnz(load)))
            r = [RX[outer, a, i + 1] + (below[a] - load) for a in range(3)]
            u = block_solve(i, r, wide)
            if 0 <= i < nx:
                put_vector(base, i, [v[:ny] for v in u])
                for a in range(3):
                    MYH[base, 1, a, i:i + 1, :] = u[a][ny:ny + 1]
                    MYH[base, 0, a, i:i + 1, :] = u[a][wide - 1:wide]
                n0 = n0 + dot3([v[:ny] for v in r], [v[:ny] for v in u])
            else:
                for a in range(3):
                    MX[base, a, i + 1] = u[a][:ny]
                if i < 0:
                    MCH[base, 0] = u[1][ny:ny + 1]
                else:
                    MCH[base, 1] = u[0][wide - 1:wide]

        def send_planes(f, made):
            put_corners(f)
            start(made, True)

        def p_after(i, c):
            if outer == OUTER - 1:
                p_out[i] = P0[D + i, 0:ny, :]
            else:
                v = AP[i]
                for k in range(INNER):
                    v = v + cs[k] * WP[k, i]
                AP[i] = v
            return c
        loop(p_after, 0)
        sums = [n0]
        for k in range(INNER):
            sums = [jnp.sum(v, keepdims=True) for v in sums]
            late = None
            if k == INNER - 1:
                wait_recv(made[2:4])
                late = functools.partial(wait_recv, made[:2] + made[4:])
            elif k > 0:
                wait_recv(made)

            def m_step(i, v, w, c):
                if outer < OUTER - 1:
                    for a in range(3):
                        WM[k, a, i] = w[a]
                even = c[0] + dot3(v, w)
                if k == INNER - 1:
                    return (even,)
                z = block_solve(i, w, ny)
                u = [z[a] - v[a] for a in range(3)]
                put_vector(base + k + 1, i, u)
                return even, c[1] + dot3(u, w)
            half = None
            if k < INNER - 1:
                retire(msent)
                made = vector_field(base + k + 1)
                half = functools.partial(send_planes, base + k + 1, made)
            sums += apply_mech(base + k, m_step, (zacc,) * (1 if k == INNER - 1 else 2), half, late)
            if k < INNER - 1:
                start(made, False)
                msent.append(made)
        def changes():
            for k in range(INNER):
                for i in range(nx):
                    w = [MX[base + k, a, i + 1] for a in range(3)]
                    DK[k, i] = (MX[base + k, 0, i + 2] - w[0] + upy(w[1], MYH[base + k, 1, 1, i:i + 1, :]) - w[1]
                                + jnp.where(last_lane, 0.0, upz(w[2])) - w[2])
        cs = combine(all_sum(2 * outer + 1, sums, changes if outer < OUTER - 1 else None))

        def mixed(get, cs=cs, base=base):
            v = cs[0] * get(base)
            for k in range(1, INNER):
                v = v + cs[k] * get(base + k)
            return v

        def m_change(i, outer=outer, cs=cs):
            v = DC[i] if outer > 0 else None
            for k in range(INNER):
                part = cs[k] * DK[k, i]
                v = part if v is None else v + part
            DC[i] = v

        def m_after(i, c, cs=cs, mixed=mixed, outer=outer):
            for a in range(3):
                before = MX[0, a, i + 1] if outer == 0 else d_out[a, i]
                d_out[a, i] = before + mixed(lambda f, a=a: MX[f, a, i + 1])
            if outer < OUTER - 1:
                for a in range(3):
                    v = AD[a, i]
                    for k in range(INNER):
                        v = v + cs[k] * WM[k, a, i]
                    RX[outer + 1, a, i + 1, 0:ny, :] = bforce[a, i] - v
            return c
        if outer == OUTER - 1:
            loop(m_after, 0)

    for made in msent + [codes_near, codes_far, made_p, made_r, made_v]:
        wait_send(made)
    for copy in summed:
        copy.wait_send()


def on_device(dims, d_old, p_old, bforce, fsource, ids, materials):
    ngx, ngy, nx, ny, nz, nmat = dims
    nf = 1 + OUTER * INNER
    nq = 2 * OUTER

    def vm(*shape, dtype=F32):
        return pltpu.VMEM(shape, dtype)
    plane, strip = (ny, nz), (nx, nz)
    cell = (nx, ny, nz)
    ext = (nx + 2, ny, nz)
    broad = (ny + 8, nz)
    big = (nx + 2 * D, ny + 8, nz)
    edge = (2, nx, 8, nz)
    corner = (4, D - 1, 2 if D == 3 else 4, nz)
    dma = pltpu.SemaphoreType.DMA
    scratch = [
        pltpu.SMEM((5, nmat), F32), vm(*cell), vm(3, *cell), vm(*cell), vm(*cell, dtype=jnp.int32), dma((7,)),
        vm(*big, dtype=jnp.int32), vm(*edge, dtype=jnp.int32),
        vm(*corner, dtype=jnp.int32), vm(*corner, dtype=jnp.int32),
        vm(*big), vm(*big), vm(*big), vm(*big), vm(*big), vm(*big), vm(*strip),
        vm(nx + 3, *broad), vm(2, *cell), vm(2, *cell), vm(*cell),
        vm(*big), vm(*big), vm(*big), vm(*big), vm(*big),
        vm(3, nx + 2, *broad), vm(nx + 2, *broad),
        vm(*big), vm(*edge), vm(*corner), vm(*corner), vm(OUTER * INNER, *big), vm(OUTER, *edge), vm(OUTER, *corner), vm(OUTER, *corner),
        vm(OUTER, nx, 8, nz), vm(OUTER, 3, INNER - 1, 2, 2, nz), vm(OUTER, 3, INNER - 1, 2, 2, nz),
        vm(OUTER, 3, nx + 2, *broad), vm(OUTER, 2, 3, nx, 8, nz), vm(OUTER, 2, 3, 1, nz), vm(OUTER, 2, 3, 1, nz),
        vm(nf, 3, *ext), vm(nf, 2, 3, *strip), vm(nf, 2, 3, *strip), vm(nf, 2, 1, nz), vm(nf, 2, 1, nz),
        vm(INNER, *cell), vm(INNER, 3, *cell), vm(*cell), vm(3, *cell), vm(*cell), vm(INNER, *cell),
        vm(*strip), vm(*cell), vm(nq, ngx * ngy, 1, 128),
        dma((10,)), dma((10,)), dma((10,)), dma((10,)), dma((5,)), dma((5,)), dma((6,)), dma((6,)), dma((8,)), dma((8,)), dma((2, 6)), dma((2, 6)),
        dma((nq,)), dma((nq,)),
    ]
    block = pl.BlockSpec(memory_space=pltpu.VMEM)
    return pl.pallas_call(
        functools.partial(kernel, dims),
        out_shape=(pltpu.VMEM(d_old.shape, F32), pltpu.VMEM(p_old.shape, F32)),
        in_specs=[pl.BlockSpec(memory_space=pl.ANY)] * 6,
        out_specs=(block, block),
        scratch_shapes=scratch,
        compiler_params=pltpu.CompilerParams(
            collective_id=0, has_side_effects=True,
            vmem_limit_bytes=VMEM_BYTES - 4 * (d_old.size + p_old.size) - 131072),
        name="poro",
    )(materials, d_old, p_old, bforce, fsource, ids)


def solution(mesh):
    ngx, ngy = mesh.shape["gx"], mesh.shape["gy"]

    def body(d_old, p_old, bforce, fsource, ids, materials):
        dims = (ngx, ngy, *p_old.shape, materials.shape[1])
        return on_device(dims, d_old, p_old, bforce, fsource, ids, materials)

    return jax.shard_map(
        body,
        mesh=mesh,
        in_specs=(P(None, "gx", "gy", None), P("gx", "gy", None), P(None, "gx", "gy", None),
                  P("gx", "gy", None), P("gx", "gy", None), P()),
        out_specs=(P(None, "gx", "gy", None), P("gx", "gy", None)),
        check_vma=False,
    )
```
